8 devices in a mesh: fsdp: 8 (over z, y, x, core).
Axes of the slice: x: 2, y: 2, z: 1, core: 2. Of those that a mesh axis runs over, the one named last changes fastest.
Arguments:
- act_in: bfloat16 [192, 196, 768], P('fsdp')
- labels: int32 [192], P('fsdp')
- layer_p: float32 [2, 4877312], P(None, 'fsdp')
- head_w: float32 [768, 1000], P('fsdp')
- small_p: float32 [3072], P('fsdp')
- layer_m: float32 [2, 4877312], P(None, 'fsdp')
- head_m: float32 [768, 1000], P('fsdp')
- small_m: float32 [3072], P('fsdp')
- layer_v: float32 [2, 4877312], P(None, 'fsdp')
- head_v: float32 [768, 1000], P('fsdp')
- small_v: float32 [3072], P('fsdp')
Outputs:
- output 1: float32 [], replicated
- output 2: float32 [2, 4877312], P(None, 'fsdp')
- output 3: float32 [768, 1000], P('fsdp')
- output 4: float32 [3072], P('fsdp')
- output 5: float32 [2, 4877312], P(None, 'fsdp')
- output 6: float32 [768, 1000], P('fsdp')
- output 7: float32 [3072], P('fsdp')
- output 8: float32 [2, 4877312], P(None, 'fsdp')
- output 9: float32 [768, 1000], P('fsdp')
- output 10: float32 [3072], P('fsdp')
All inputs are finite; a program needn't handle non-finite values.
Results may differ from the reference program's by a relative error of at most 0.001.
Values are sent between devices in bfloat16 or wider.
A program may use at most 1 GiB of HBM per device.

```python
import jax
import jax.numpy as jnp
from jax import lax

CHANNELS = 768
TOKENS = 196
TOKEN_HID = 384
CHAN_HID = 3072
CLASSES = 1000
BATCH_DEV = 24
FSDP_DEVS = 8
ADAM_STEP = 10

GLOBAL_BATCH = BATCH_DEV * FSDP_DEVS
PAD_UNIT = 128 * FSDP_DEVS
MAT_LEN = 2 * TOKENS * TOKEN_HID + 2 * CHANNELS * CHAN_HID
LAYER_LEN = MAT_LEN + 5 * CHANNELS + TOKEN_HID + TOKENS + CHAN_HID
LAYER_PAD = (LAYER_LEN + PAD_UNIT - 1) // PAD_UNIT * PAD_UNIT
SMALL_LEN = 2 * CHANNELS + CLASSES
SMALL_PAD = (SMALL_LEN + PAD_UNIT - 1) // PAD_UNIT * PAD_UNIT
PIECE_SIZES = (TOKENS * TOKEN_HID, TOKEN_HID * TOKENS, CHANNELS * CHAN_HID, CHAN_HID * CHANNELS, CHANNELS, CHANNELS, TOKEN_HID, TOKENS, CHANNELS, CHANNELS, CHAN_HID, CHANNELS)
LN_EPS = 1e-6
LEARN_RATE = 0.003
BETA_ONE = 0.9
BETA_TWO = 0.999
ADAM_EPS = 1e-8
WEIGHT_DECAY = 0.03


def unpack_layer(flat):
    pieces = []
    piece_start = 0
    for piece_len in PIECE_SIZES:
        pieces.append(flat[piece_start:piece_start + piece_len])
        piece_start = piece_start + piece_len
    w_tok1 = pieces[0].reshape(TOKENS, TOKEN_HID)
    w_tok2 = pieces[1].reshape(TOKEN_HID, TOKENS)
    w_ch1 = pieces[2].reshape(CHANNELS, CHAN_HID)
    w_ch2 = pieces[3].reshape(CHAN_HID, CHANNELS)
    return [w_tok1, w_tok2, w_ch1, w_ch2] + pieces[4:12]


def layer_norm(x_in, ln_gain, ln_shift):
    x_f = x_in.astype(jnp.float32)
    mean_val = jnp.mean(x_f, axis=-1, keepdims=True)
    var_val = jnp.mean(jnp.square(x_f - mean_val), axis=-1, keepdims=True)
    normed = (x_f - mean_val) * lax.rsqrt(var_val + LN_EPS)
    return (normed * ln_gain.astype(jnp.float32) + ln_shift.astype(jnp.float32)).astype(jnp.bfloat16)


def mixer_layer(x_in, flat):
    w_tok1, w_tok2, w_ch1, w_ch2, ln1_g, ln1_b, b_tok1, b_tok2, ln2_g, ln2_b, b_ch1, b_ch2 = unpack_layer(flat)
    normed = layer_norm(x_in, ln1_g, ln1_b)
    hid_tok = jnp.einsum('bsc,sj->bcj', normed.astype(jnp.float32), w_tok1.astype(jnp.float32)) + b_tok1.astype(jnp.float32)
    act_tok = jax.nn.gelu(hid_tok).astype(jnp.bfloat16)
    tok_out = jnp.einsum('bcj,js->bsc', act_tok.astype(jnp.float32), w_tok2.astype(jnp.float32)) + b_tok2.astype(jnp.float32)[:, None]
    after_tok = (x_in.astype(jnp.float32) + tok_out).astype(jnp.bfloat16)
    normed2 = layer_norm(after_tok, ln2_g, ln2_b)
    hid_ch = jnp.einsum('bsc,cd->bsd', normed2.astype(jnp.float32), w_ch1.astype(jnp.float32)) + b_ch1.astype(jnp.float32)
    act_ch = jax.nn.gelu(hid_ch).astype(jnp.bfloat16)
    ch_out = jnp.einsum('bsd,dc->bsc', act_ch.astype(jnp.float32), w_ch2.astype(jnp.float32)) + b_ch2.astype(jnp.float32)
    return (after_tok.astype(jnp.float32) + ch_out).astype(jnp.bfloat16)


def block_loss(layer_p, head_w, small_p, x_block, label_block):
    layers_bf = layer_p.astype(jnp.bfloat16)
    hidden = x_block
    for layer_idx in range(2):
        hidden = mixer_layer(hidden, layers_bf[layer_idx])
    small_bf = small_p.astype(jnp.bfloat16)
    lnf_g = small_bf[:CHANNELS]
    lnf_b = small_bf[CHANNELS:2 * CHANNELS]
    head_b = small_bf[2 * CHANNELS:2 * CHANNELS + CLASSES]
    normed = layer_norm(hidden, lnf_g, lnf_b)
    pooled = jnp.mean(normed.astype(jnp.float32), axis=1).astype(jnp.bfloat16)
    logits = jnp.dot(pooled, head_w.astype(jnp.bfloat16), preferred_element_type=jnp.float32) + head_b.astype(jnp.float32)
    log_norm = jax.nn.logsumexp(logits, axis=-1)
    is_label = jnp.arange(CLASSES)[None, :] == label_block[:, None]
    picked = jnp.sum(jnp.where(is_label, logits, 0.0), axis=-1)
    return jnp.sum(log_norm - picked) / GLOBAL_BATCH


def loss_and_grads(act_in, labels, layer_p, head_w, small_p):
    x_blocks = act_in.reshape(FSDP_DEVS, BATCH_DEV, TOKENS, CHANNELS)
    label_blocks = labels.reshape(FSDP_DEVS, BATCH_DEV)
    grad_fn = jax.value_and_grad(block_loss, argnums=(0, 1, 2))

    def scan_body(running, block_pair):
        loss_part, grad_parts = grad_fn(layer_p, head_w, small_p, block_pair[0], block_pair[1])
        return (running[0] + loss_part, running[1] + grad_parts[0], running[2] + grad_parts[1], running[3] + grad_parts[2]), None

    start_val = (jnp.zeros((), jnp.float32), jnp.zeros_like(layer_p), jnp.zeros_like(head_w), jnp.zeros_like(small_p))
    totals, _ = lax.scan(scan_body, start_val, (x_blocks, label_blocks))
    return totals


def adam_update(master, gradient, moment, second, decay_rate):
    moment_new = BETA_ONE * moment + (1.0 - BETA_ONE) * gradient
    second_new = BETA_TWO * second + (1.0 - BETA_TWO) * gradient * gradient
    m_hat = moment_new / (1.0 - BETA_ONE ** ADAM_STEP)
    v_hat = second_new / (1.0 - BETA_TWO ** ADAM_STEP)
    master_new = master - LEARN_RATE * (m_hat / (jnp.sqrt(v_hat) + ADAM_EPS) + decay_rate * master)
    return master_new, moment_new, second_new


def draw_layer(key):
    subkeys = jax.random.split(key, 13)
    normal = jax.random.normal
    pieces = [
        normal(subkeys[0], (TOKENS * TOKEN_HID,), jnp.float32) * TOKENS ** -0.5,
        normal(subkeys[1], (TOKEN_HID * TOKENS,), jnp.float32) * TOKEN_HID ** -0.5,
        normal(subkeys[2], (CHANNELS * CHAN_HID,), jnp.float32) * CHANNELS ** -0.5,
        normal(subkeys[3], (CHAN_HID * CHANNELS,), jnp.float32) * CHAN_HID ** -0.5,
        1.0 + 0.2 * normal(subkeys[4], (CHANNELS,), jnp.float32),
        0.2 * normal(subkeys[5], (CHANNELS,), jnp.float32),
        0.3 * normal(subkeys[6], (TOKEN_HID,), jnp.float32),
        0.3 * normal(subkeys[7], (TOKENS,), jnp.float32),
        1.0 + 0.2 * normal(subkeys[8], (CHANNELS,), jnp.float32),
        0.2 * normal(subkeys[9], (CHANNELS,), jnp.float32),
        0.3 * normal(subkeys[10], (CHAN_HID,), jnp.float32),
        0.3 * normal(subkeys[11], (CHANNELS,), jnp.float32),
        0.02 * normal(subkeys[12], (LAYER_PAD - LAYER_LEN,), jnp.float32),
    ]
    return jnp.concatenate(pieces)


def setup_inputs(seed: int = 0) -> dict:
    keys = jax.random.split(jax.random.key(seed), 12)
    normal = jax.random.normal
    base = normal(keys[0], (GLOBAL_BATCH, 1, CHANNELS), jnp.float32)
    noise = normal(keys[1], (GLOBAL_BATCH, TOKENS, CHANNELS), jnp.float32)
    act_in = (base + noise).astype(jnp.bfloat16)
    labels = jax.random.randint(keys[2], (GLOBAL_BATCH,), 0, CLASSES, jnp.int32)
    layer_p = jnp.stack([draw_layer(keys[3]), draw_layer(keys[4])])
    head_w = normal(keys[5], (CHANNELS, CLASSES), jnp.float32) * CHANNELS ** -0.5
    small_p = jnp.concatenate([
        2.0 + 0.3 * normal(keys[6], (CHANNELS,), jnp.float32),
        0.3 * normal(keys[7], (CHANNELS,), jnp.float32),
        normal(keys[8], (CLASSES,), jnp.float32),
        0.02 * normal(keys[9], (SMALL_PAD - SMALL_LEN,), jnp.float32),
    ])
    _, g_layer, g_head, g_small = loss_and_grads(act_in, labels, layer_p, head_w, small_p)
    layer_rms = jnp.sqrt(jnp.mean(jnp.square(g_layer), axis=1, keepdims=True))
    head_rms = jnp.sqrt(jnp.mean(jnp.square(g_head)))
    small_rms = jnp.sqrt(jnp.mean(jnp.square(g_small)))
    mkeys = jax.random.split(keys[10], 6)
    uniform = jax.random.uniform
    layer_m = 0.3 * layer_rms * normal(mkeys[0], layer_p.shape, jnp.float32)
    head_m = 0.3 * head_rms * normal(mkeys[1], head_w.shape, jnp.float32)
    small_m = 0.3 * small_rms * normal(mkeys[2], small_p.shape, jnp.float32)
    layer_v = 0.01 * jnp.square(layer_rms) * uniform(mkeys[3], layer_p.shape, jnp.float32, 0.5, 2.0)
    head_v = 0.01 * jnp.square(head_rms) * uniform(mkeys[4], head_w.shape, jnp.float32, 0.5, 2.0)
    small_v = 0.01 * jnp.square(small_rms) * uniform(mkeys[5], small_p.shape, jnp.float32, 0.5, 2.0)
    return {'act_in': act_in, 'labels': labels, 'layer_p': layer_p, 'head_w': head_w, 'small_p': small_p, 'layer_m': layer_m, 'head_m': head_m, 'small_m': small_m, 'layer_v': layer_v, 'head_v': head_v, 'small_v': small_v}


def reference(act_in, labels, layer_p, head_w, small_p, layer_m, head_m, small_m, layer_v, head_v, small_v):
    loss_value, g_layer, g_head, g_small = loss_and_grads(act_in, labels, layer_p, head_w, small_p)
    sq_total = jnp.sum(jnp.square(g_layer)) + jnp.sum(jnp.square(g_head)) + jnp.sum(jnp.square(g_small))
    clip_scale = 1.0 / jnp.maximum(1.0, jnp.sqrt(sq_total))
    layer_decay = jnp.where(jnp.arange(LAYER_PAD) < MAT_LEN, WEIGHT_DECAY, 0.0)[None, :]
    new_lp, new_lm, new_lv = adam_update(layer_p, g_layer * clip_scale, layer_m, layer_v, layer_decay)
    new_hw, new_hm, new_hv = adam_update(head_w, g_head * clip_scale, head_m, head_v, WEIGHT_DECAY)
    new_sp, new_sm, new_sv = adam_update(small_p, g_small * clip_scale, small_m, small_v, 0.0)
    return (loss_value, new_lp, new_hw, new_sp, new_lm, new_hm, new_sm, new_lv, new_hv, new_sv)
```

```python
import functools
import math

import jax
import jax.numpy as jnp
from jax import lax
from jax.experimental import pallas as pl
from jax.experimental.pallas import tpu as pltpu
from jax.sharding import PartitionSpec as P

F32, BF16 = jnp.float32, jnp.bfloat16
LN_EPS = 1e-6
LEARN_RATE = 0.003
BETA_ONE = 0.9
BETA_TWO = 0.999
ADAM_EPS = 1e-8
WEIGHT_DECAY = 0.03
ADAM_STEP = 10

NDEV = 8
TOK, CH, TH, HID, NCLS = 196, 768, 384, 3072, 1000
SH = 4763
T1 = 2 * TOK * TH // 128
RW = CH * HID // 128
C1, C2 = HID // 128, CH // 128
VEC0 = T1 + 2 * RW - 7 * SH
MARG = 384
MESH = pl.DeviceIdType.MESH
ANY = pl.BlockSpec(memory_space=pl.ANY)
VMEM = pl.BlockSpec(memory_space=pltpu.VMEM)


def c1_span(d):
    return max(0, SH * d - T1), min(RW, SH * (d + 1) - T1)


def c2_span(d):
    return max(0, SH * d - T1 - RW), min(RW, SH * (d + 1) - T1 - RW)


def tiles_of(span, per):
    lo, hi = span
    if lo >= hi:
        return 0, 0
    return lo // per, -(-hi // per)


def edges(span_of, per):
    out = []
    for d in range(NDEV):
        lo, hi = span_of(d)
        if lo < hi and lo > 0 and lo % per:
            out.append((d, lo // per, lo % per))
    return out


EDGE1 = edges(c1_span, 16 * C1)
EDGE2 = edges(c2_span, 16 * C2)


def piece_moves(d, l, src, dst):
    s1, s2, stok, svec = src
    w1, w2, e1, e2, tok, vec = dst
    out = []
    for span_of, per, s, w, e, eds in ((c1_span, 16 * C1, s1, w1, e1, EDGE1), (c2_span, 16 * C2, s2, w2, e2, EDGE2)):
        lo, hi = tiles_of(span_of(d), per)
        if lo == hi:
            continue
        first = lo
        for k, (owner, row, _) in enumerate(eds):
            if owner == d:
                out.append((s.at[l, pl.ds(0, 16)], e.at[l, k]))
                first = lo + 1
        n = hi - first
        out.append((s.at[l, pl.ds(16 * (first - lo), 16 * n)], w.at[l, pl.ds(16 * first, 16 * n)]))
    if d == 0:
        out.append((stok.at[l], tok.at[l]))
    if d == NDEV - 1:
        out.append((svec.at[l], vec.at[l]))
    return out


def entry_barrier(me):
    barrier = pltpu.get_barrier_semaphore()
    for rel in (1, 2, 4, 6):
        pl.semaphore_signal(barrier, inc=1, device_id=(peer(me, rel),), device_id_type=MESH)
    pl.semaphore_wait(barrier, 4)


def peer(me, rel):
    t = me
    if rel & 1:
        t = t + 1 - 2 * lax.rem(me, 2)
    if rel & 2:
        t = t + 2 - 4 * lax.rem(me // 2, 2)
    if rel & 4:
        t = t + 4 - 8 * (me // 4)
    return t


RELS = (2, 4, 6)


def gather_kernel(p_ref, head_ref, small_ref, w1, w2, tok, vec, headf, smallf, e1, e2,
                  xs, s1, s2, stok, svec, shead, ssmall, m1, m2, ld_sem, send_sem, recv_sem, fwd_sem, own_sem, mg_sem):
    me = lax.axis_index("fsdp")
    for l in range(2):
        pltpu.make_async_copy(p_ref.at[:, l, :], xs.at[l, pl.ds(MARG, SH)], ld_sem.at[l]).start()
    shead[...] = head_ref[...].astype(BF16)
    ssmall[...] = small_ref[...].astype(BF16).astype(F32)
    entry_barrier(me)

    def moves(d, g, own_source):
        if g < 2:
            dst = (w1, w2, e1, e2, tok, vec)
            src = (s1, s2, stok, svec)
            both = piece_moves(d, g, src, dst)
        else:
            both = [(shead, headf.at[pl.ds(96 * d, 96)]), (ssmall, smallf.at[d])]
        return [(a if own_source else b, b, i) for i, (a, b) in enumerate(both)]

    def remote(a, b, ssem, d, dev):
        return pltpu.make_async_remote_copy(src_ref=a, dst_ref=b, send_sem=ssem, recv_sem=recv_sem.at[d], device_id=(dev,), device_id_type=MESH)

    for g in range(3):
        if g < 2:
            l = g
            pltpu.make_async_copy(p_ref.at[:, l, :], xs.at[l, pl.ds(MARG, SH)], ld_sem.at[l]).wait()
        for d in range(NDEV):
            @pl.when(me == d)
            def _():
                if g < 2:
                    for span_of, per, s in ((c1_span, C1, s1), (c2_span, C2, s2)):
                        lo, hi = tiles_of(span_of(d), 16 * per)
                        if lo == hi:
                            continue
                        base0 = 16 * per * lo - span_of(d)[0] + MARG + (T1 if (d == 0) else 0)
                        if per == C2 and d == 4:
                            base0 = base0 + c1_span(4)[1] - c1_span(4)[0]

                        def one(i, carry, per=per, s=s, base0=base0):
                            base = base0 + i * (16 * per)
                            row = pl.multiple_of(i * 16, 16)
                            for c in range(per):
                                s[l, pl.ds(row, 16), 128 * c:128 * c + 128] = xs[l, pl.ds(base + c, 16, stride=per), :].astype(BF16)
                            return carry

                        lax.fori_loop(0, hi - lo, one, 0)
                    if d == 0:
                        stok[l] = xs[l, MARG:MARG + T1, :].astype(BF16)
                    if d == NDEV - 1:
                        svec[l] = xs[l, MARG + VEC0:MARG + SH, :].astype(BF16)
                for k, rel in enumerate((4, 2, 6, 1)):
                    for a, b, i in moves(d, g, True):
                        remote(a, b, send_sem.at[k, g, i], (d, g, i), d ^ rel).start()
                for a, b, i in moves(d, g, True):
                    pltpu.make_async_copy(a, b, own_sem.at[g, i]).start()
    for g in range(3):
        for s in range(NDEV):
            for rel in RELS:
                @pl.when(me == (s ^ rel))
                def _():
                    for a, b, i in moves(s, g, False):
                        remote(a, b, fwd_sem.at[s, g, i], (s, g, i), s ^ rel ^ 1).wait_recv()
                    for a, b, i in moves(s, g, False):
                        remote(a, b, fwd_sem.at[s, g, i], (s, g, i), s ^ rel ^ 1).start()
    for g in range(3):
        for s in range(NDEV):
            for rel in (1, 3, 5, 7):
                @pl.when(me == (s ^ rel))
                def _():
                    for a, b, i in moves(s, g, False):
                        remote(a, b, fwd_sem.at[s, g, i], (s, g, i), s).wait_recv()
    for g in range(3):
        for d in range(NDEV):
            @pl.when(me == d)
            def _():
                for k, rel in enumerate((4, 2, 6, 1)):
                    for a, b, i in moves(d, g, True):
                        remote(a, b, send_sem.at[k, g, i], (d, g, i), d ^ rel).wait_send()
                for a, b, i in moves(d, g, True):
                    pltpu.make_async_copy(a, b, own_sem.at[g, i]).wait()
        for s in range(NDEV):
            for rel in RELS:
                @pl.when(me == (s ^ rel))
                def _():
                    for a, b, i in moves(s, g, False):
                        remote(a, b, fwd_sem.at[s, g, i], (s, g, i), s ^ rel ^ 1).wait_send()
    for per, w, e, m, eds in ((C1, w1, e1, m1, EDGE1), (C2, w2, e2, m2, EDGE2)):
        todo = [(l, k, row, below) for l in range(2) for k, (_, row, below) in enumerate(eds)]
        for l, k, row, below in todo:
            pltpu.make_async_copy(w.at[l, pl.ds(16 * row, 16)], m.at[0, l, k], mg_sem.at[0, l, k]).start()
            pltpu.make_async_copy(e.at[l, k], m.at[1, l, k], mg_sem.at[1, l, k]).start()
        for l, k, row, below in todo:
            pltpu.make_async_copy(w.at[l, pl.ds(16 * row, 16)], m.at[0, l, k], mg_sem.at[0, l, k]).wait()
            pltpu.make_async_copy(e.at[l, k], m.at[1, l, k], mg_sem.at[1, l, k]).wait()
        for l, k, row, below in todo:
            shape = (16, 128 * per)
            pos = lax.broadcasted_iota(jnp.int32, shape, 0) * per + lax.broadcasted_iota(jnp.int32, shape, 1) // 128
            m[0, l, k] = jnp.where(pos < below, m[0, l, k].astype(F32), m[1, l, k].astype(F32)).astype(BF16)
        for l, k, row, below in todo:
            pltpu.make_async_copy(m.at[0, l, k], w.at[l, pl.ds(16 * row, 16)], mg_sem.at[0, l, k]).start()
        for l, k, row, below in todo:
            pltpu.make_async_copy(m.at[0, l, k], w.at[l, pl.ds(16 * row, 16)], mg_sem.at[0, l, k]).wait()


def gather_all(p_view, head_w, small8):
    sds = jax.ShapeDtypeStruct
    outs = [sds((2, CH, HID), BF16), sds((2, HID, CH), BF16), sds((2, T1, 128), BF16), sds((2, SH - VEC0, 128), BF16),
            sds((CH, NCLS), BF16), sds((NDEV, 8, 128), F32), sds((2, len(EDGE1), 16, HID), BF16), sds((2, len(EDGE2), 16, CH), BF16)]
    n1 = max(16 * (b - a) for a, b in (tiles_of(c1_span(d), 16 * C1) for d in range(NDEV)))
    n2 = max(16 * (b - a) for a, b in (tiles_of(c2_span(d), 16 * C2) for d in range(NDEV)))
    dma = pltpu.SemaphoreType.DMA
    return pl.pallas_call(
        gather_kernel,
        in_specs=[ANY, VMEM, VMEM],
        out_specs=[ANY] * 8,
        out_shape=outs,
        scratch_shapes=[pltpu.VMEM((2, SH + 2 * MARG + 5, 128), F32), pltpu.VMEM((2, n1, HID), BF16), pltpu.VMEM((2, n2, CH), BF16),
                        pltpu.VMEM((2, T1, 128), BF16), pltpu.VMEM((2, SH - VEC0, 128), BF16), pltpu.VMEM((96, NCLS), BF16), pltpu.VMEM((8, 128), F32),
                        pltpu.VMEM((2, 2, len(EDGE1), 16, HID), BF16), pltpu.VMEM((2, 2, len(EDGE2), 16, CH), BF16),
                        dma((2,)), dma((4, 3, 3)), dma((NDEV, 3, 3)), dma((NDEV, 3, 3)), dma((3, 3)), dma((2, 2, 4))],
        compiler_params=pltpu.CompilerParams(collective_id=0, has_side_effects=True, vmem_limit_bytes=60000000),
        name="gather_weights",
    )(p_view, head_w, small8)[:6]


def g1_rows(d):
    lo, hi = tiles_of(c1_span(d), 8 * C1)
    return 8 * lo, 8 * hi


def g2_rows(d):
    lo, hi = tiles_of(c2_span(d), 8 * C2)
    return 8 * lo, 8 * hi


def pack(rows_of, core):
    at, where = 0, {}
    for s in range(core, NDEV, 2):
        lo, hi = rows_of(s)
        if lo < hi:
            where[s] = (lo, hi - lo, at)
            at += hi - lo
    return where, at


PK1 = [pack(g1_rows, c) for c in range(2)]
PK2 = [pack(g2_rows, c) for c in range(2)]
N1 = max(PK1[0][1], PK1[1][1])
N2 = max(PK2[0][1], PK2[1][1])
B1 = max(hi - lo for lo, hi in map(g1_rows, range(NDEV)))
B2 = max(hi - lo for lo, hi in map(g2_rows, range(NDEV)))


def reduce_kernel(dw1, dw2, tokg, vecg, out, a1, a2, at, av, r1, r2, rt, rv, b1, b2, bt, bv, gs, ld_sem, ps_sem, pr_sem, xs_sem, xr_sem):
    me = lax.axis_index("fsdp")
    core = lax.rem(me, 2)

    def chip_blocks(c, d1, d2, dt, dv):
        out_ = []
        for (where, _), g, dst in ((PK1[c], dw1, d1), (PK2[c], dw2, d2)):
            for s, (lo, n, at_) in where.items():
                out_.append((g.at[pl.ds(lo, n)], dst.at[pl.ds(at_, n)]))
        out_.append((tokg, dt) if c == 0 else (vecg, dv))
        return [(a, b, i) for i, (a, b) in enumerate(out_)]

    for c in range(2):
        @pl.when(core == c)
        def _():
            for a, b, i in chip_blocks(c, a1, a2, at, av):
                pltpu.make_async_copy(a, b, ld_sem.at[i]).start()
    entry_barrier(me)

    def to_partner(i, a, b, dev):
        return pltpu.make_async_remote_copy(src_ref=a, dst_ref=b, send_sem=ps_sem.at[i], recv_sem=pr_sem.at[i], device_id=(dev,), device_id_type=MESH)

    for c in range(2):
        @pl.when(core == c)
        def _():
            for a, b, i in chip_blocks(1 - c, r1, r2, rt, rv):
                to_partner(i, a, b, peer(me, 1)).start()
            for a, b, i in chip_blocks(c, a1, a2, at, av):
                pltpu.make_async_copy(a, b, ld_sem.at[i]).wait()
            for a, b, i in chip_blocks(c, r1, r2, rt, rv):
                to_partner(i, a, b, peer(me, 1)).wait_recv()

    def share_blocks(s, slot):
        c = s % 2
        out_ = []
        for (where, _), src, dst in ((PK1[c], a1, b1), (PK2[c], a2, b2)):
            if s in where:
                _, n, at_ = where[s]
                out_.append((src.at[pl.ds(at_, n)], dst.at[slot, pl.ds(0, n)]))
        if s == 0:
            out_.append((at, bt.at[slot]))
        if s == NDEV - 1:
            out_.append((av, bv.at[slot]))
        return [(a, b, i) for i, (a, b) in enumerate(out_)]

    def to_owner(a, b, slot, i, dev):
        return pltpu.make_async_remote_copy(src_ref=a, dst_ref=b, send_sem=xs_sem.at[slot, i], recv_sem=xr_sem.at[slot, i], device_id=(dev,), device_id_type=MESH)

    def add_rows(a, r, n, step):
        def one(i, carry):
            o = pl.multiple_of(i * step, step)
            a[pl.ds(o, step), :] = a[pl.ds(o, step), :] + r[pl.ds(o, step), :]
            return carry
        lax.fori_loop(0, n // step, one, 0)

    add_rows(a1, r1, N1, 16)
    add_rows(a2, r2, N2, 48)

    @pl.when(core == 0)
    def _():
        add_rows(at, rt, T1, 56)

    @pl.when(core == 1)
    def _():
        add_rows(av, rv, SH - VEC0, 64)

    for d in range(NDEV):
        @pl.when(me == d)
        def _():
            for slot, rel in enumerate(RELS):
                for a, b, i in share_blocks(d ^ rel, slot):
                    to_owner(a, b, slot, i, d ^ rel).start()
            for slot, rel in enumerate(RELS):
                for a, b, i in share_blocks(d, slot):
                    to_owner(a, b, slot, i, d ^ rel).wait_recv()
            for (where, _), src, dst, span_of, per in ((PK1[d % 2], a1, b1, c1_span, C1), (PK2[d % 2], a2, b2, c2_span, C2)):
                if d not in where:
                    continue
                lo, n, at_ = where[d]
                base0 = per * lo - span_of(d)[0] + MARG + (T1 if d == 0 else 0)
                if per == C2 and d == 4:
                    base0 = base0 + c1_span(4)[1] - c1_span(4)[0]

                def one(i, carry, src=src, dst=dst, per=per, base0=base0, at_=at_):
                    o = pl.multiple_of(i * 8, 8)
                    tot = src[pl.ds(at_ + o, 8), :] + dst[0, pl.ds(o, 8), :] + dst[1, pl.ds(o, 8), :] + dst[2, pl.ds(o, 8), :]
                    base = base0 + i * (8 * per)
                    for c in range(per):
                        gs[pl.ds(base + c, 8, stride=per), :] = tot[:, 128 * c:128 * c + 128]
                    return carry

                lax.fori_loop(0, n // 8, one, 0)
            if d == 0:
                gs[MARG:MARG + T1, :] = at[...] + bt[0] + bt[1] + bt[2]
            if d == NDEV - 1:
                gs[MARG + VEC0:MARG + SH, :] = av[...] + bv[0] + bv[1] + bv[2]
            pltpu.make_async_copy(gs.at[pl.ds(MARG, SH)], out, ld_sem.at[0]).start()
            for slot, rel in enumerate(RELS):
                for a, b, i in share_blocks(d ^ rel, slot):
                    to_owner(a, b, slot, i, d ^ rel).wait_send()
            pltpu.make_async_copy(gs.at[pl.ds(MARG, SH)], out, ld_sem.at[0]).wait()
    for c in range(2):
        @pl.when(core == c)
        def _():
            for a, b, i in chip_blocks(1 - c, r1, r2, rt, rv):
                to_partner(i, a, b, peer(me, 1)).wait_send()


def reduce_layer(dw1, dw2, tokg, vecg, cid):
    dma = pltpu.SemaphoreType.DMA
    nv = SH - VEC0
    return pl.pallas_call(
        reduce_kernel,
        in_specs=[ANY] * 4,
        out_specs=ANY,
        out_shape=jax.ShapeDtypeStruct((SH, 128), F32),
        scratch_shapes=[pltpu.VMEM((N1, HID), F32), pltpu.VMEM((N2, CH), F32), pltpu.VMEM((T1, 128), F32), pltpu.VMEM((nv, 128), F32),
                        pltpu.VMEM((N1, HID), F32), pltpu.VMEM((N2, CH), F32), pltpu.VMEM((T1, 128), F32), pltpu.VMEM((nv, 128), F32),
                        pltpu.VMEM((3, B1, HID), F32), pltpu.VMEM((3, B2, CH), F32), pltpu.VMEM((3, T1, 128), F32), pltpu.VMEM((3, nv, 128), F32),
                        pltpu.VMEM((SH + 2 * MARG + 5, 128), F32), dma((6,)), dma((6,)), dma((6,)), dma((3, 2)), dma((3, 2))],
        compiler_params=pltpu.CompilerParams(collective_id=cid, has_side_effects=True, vmem_limit_bytes=66000000),
        name=f"reduce_grads_{cid}",
    )(dw1, dw2, tokg, vecg)


def adam_math(p, g, m, v, decay):
    m_new = BETA_ONE * m + (1.0 - BETA_ONE) * g
    v_new = BETA_TWO * v + (1.0 - BETA_TWO) * g * g
    m_hat = m_new / (1.0 - BETA_ONE ** ADAM_STEP)
    v_hat = v_new / (1.0 - BETA_TWO ** ADAM_STEP)
    p_new = p - LEARN_RATE * (m_hat / (jnp.sqrt(v_hat) + ADAM_EPS) + decay * p)
    return p_new, m_new, v_new


NCHUNK = 4


def chunk_rows(k):
    step = -(-SH // (40 * NCHUNK)) * 40
    return k * step, min(SH, (k + 1) * step) - k * step


def adam_kernel(p_ref, m_ref, v_ref, g0, g1, scale_ref, po, mo, vo, ps, ms, vs, gs, in_sem, out_sem):
    me = lax.axis_index("fsdp")
    ins = ((p_ref, ps), (m_ref, ms), (v_ref, vs))
    outs = ((ps, po), (ms, mo), (vs, vo))

    def loads(k):
        a, n = chunk_rows(k)
        for j, (src, dst) in enumerate(ins):
            for l in range(2):
                yield pltpu.make_async_copy(src.at[pl.ds(a, n), l, :], dst.at[l, pl.ds(a, n)], in_sem.at[k, j, l])
        for l, g in enumerate((g0, g1)):
            yield pltpu.make_async_copy(g.at[pl.ds(a, n)], gs.at[l, pl.ds(a, n)], in_sem.at[k, 3, l])

    def stores(k):
        a, n = chunk_rows(k)
        for j, (src, dst) in enumerate(outs):
            for l in range(2):
                yield pltpu.make_async_copy(src.at[l, pl.ds(a, n)], dst.at[pl.ds(a, n), l, :], out_sem.at[k, j, l])

    for k in range(NCHUNK):
        for c in loads(k):
            c.start()
    scale = scale_ref[0, 0]
    mat_rows = T1 + 2 * RW - me * SH
    for k in range(NCHUNK):
        for c in loads(k):
            c.wait()
        a, n = chunk_rows(k)
        for l in range(2):
            def one(i, carry, l=l, a=a):
                o = pl.multiple_of(a + i * 40, 8)
                row = o + lax.broadcasted_iota(jnp.int32, (40, 128), 0)
                decay = jnp.where(row < mat_rows, WEIGHT_DECAY, 0.0)
                at = pl.ds(o, 40)
                p, m, v = adam_math(ps[l, at, :], gs[l, at, :] * scale, ms[l, at, :], vs[l, at, :], decay)
                ps[l, at, :] = p
                ms[l, at, :] = m
                vs[l, at, :] = v
                return carry
            lax.fori_loop(0, -(-n // 40), one, 0)
        for c in stores(k):
            c.start()
    for k in range(NCHUNK):
        for c in stores(k):
            c.wait()


def adam_layers(pv, mv, vv, g0, g1, scale):
    sds = jax.ShapeDtypeStruct((SH, 2, 128), F32)
    rows = chunk_rows(NCHUNK - 1)[0] + -(-chunk_rows(NCHUNK - 1)[1] // 40) * 40
    rows = max(rows, chunk_rows(1)[0] * NCHUNK)
    buf = pltpu.VMEM((2, rows + 40, 128), F32)
    return pl.pallas_call(
        adam_kernel,
        in_specs=[ANY] * 5 + [pl.BlockSpec(memory_space=pltpu.SMEM)],
        out_specs=[ANY] * 3,
        out_shape=[sds] * 3,
        scratch_shapes=[buf] * 4 + [pltpu.SemaphoreType.DMA((NCHUNK, 4, 2))] * 2,
        compiler_params=pltpu.CompilerParams(vmem_limit_bytes=60000000),
        name="adam_layers",
    )(pv, mv, vv, g0, g1, scale)


def layer_norm(x_in, ln_gain, ln_shift):
    x_f = x_in.astype(F32)
    mean_val = jnp.mean(x_f, axis=-1, keepdims=True)
    var_val = jnp.mean(jnp.square(x_f - mean_val), axis=-1, keepdims=True)
    normed = (x_f - mean_val) * lax.rsqrt(var_val + LN_EPS)
    return (normed * ln_gain.astype(F32) + ln_shift.astype(F32)).astype(BF16)


def gelu_bf16(hidden):
    return jax.nn.gelu(hidden).astype(BF16)


def gelu_grad(hidden, d_act):
    _, pullback = jax.vjp(gelu_bf16, hidden)
    return pullback(d_act.astype(BF16))[0]


def norm_grad(x_in, ln_gain, ln_shift, d_normed):
    _, pullback = jax.vjp(layer_norm, x_in, ln_gain.astype(F32), ln_shift.astype(F32))
    d_x, d_gain, d_shift = pullback(d_normed.astype(BF16))
    return d_x.astype(F32), d_gain, d_shift


def layer_forward(x_in, weights):
    w_tok1, w_tok2, w_ch1, w_ch2, ln1_g, ln1_b, b_tok1, b_tok2, ln2_g, ln2_b, b_ch1, b_ch2 = weights
    normed = layer_norm(x_in, ln1_g, ln1_b)
    hid_tok = jnp.einsum('bsc,sj->bcj', normed, w_tok1, preferred_element_type=F32) + b_tok1.astype(F32)
    act_tok = gelu_bf16(hid_tok)
    tok_out = jnp.einsum('bcj,js->bsc', act_tok, w_tok2, preferred_element_type=F32) + b_tok2.astype(F32)[:, None]
    after_tok = (x_in.astype(F32) + tok_out).astype(BF16)
    normed2 = layer_norm(after_tok, ln2_g, ln2_b)
    hid_ch = jnp.einsum('bsc,cd->bsd', normed2, w_ch1, preferred_element_type=F32) + b_ch1.astype(F32)
    act_ch = gelu_bf16(hid_ch)
    ch_out = jnp.einsum('bsd,dc->bsc', act_ch, w_ch2, preferred_element_type=F32) + b_ch2.astype(F32)
    layer_out = (after_tok.astype(F32) + ch_out).astype(BF16)
    return layer_out, (x_in, normed, hid_tok, act_tok, after_tok, normed2, hid_ch, act_ch)


def layer_backward(d_out, weights, cache):
    w_tok1, w_tok2, w_ch1, w_ch2, ln1_g, ln1_b, b_tok1, b_tok2, ln2_g, ln2_b, b_ch1, b_ch2 = weights
    x_in, normed, hid_tok, act_tok, after_tok, normed2, hid_ch, act_ch = cache
    d_out_bf = d_out.astype(BF16)
    g_b_ch2 = jnp.sum(d_out, axis=(0, 1))
    g_w_ch2 = jnp.einsum('bsd,bsc->dc', act_ch, d_out_bf, preferred_element_type=F32)
    d_act_ch = jnp.einsum('bsc,dc->bsd', d_out_bf, w_ch2, preferred_element_type=F32)
    d_hid_ch = gelu_grad(hid_ch, d_act_ch)
    d_hid_ch_bf = d_hid_ch.astype(BF16)
    g_b_ch1 = jnp.sum(d_hid_ch, axis=(0, 1))
    g_w_ch1 = jnp.einsum('bsc,bsd->cd', normed2, d_hid_ch_bf, preferred_element_type=F32)
    d_normed2 = jnp.einsum('bsd,cd->bsc', d_hid_ch_bf, w_ch1, preferred_element_type=F32)
    d_after_ln, g_ln2_g, g_ln2_b = norm_grad(after_tok, ln2_g, ln2_b, d_normed2)
    d_after = d_after_ln + d_out
    d_after_bf = d_after.astype(BF16)
    g_b_tok2 = jnp.sum(d_after, axis=(0, 2))
    g_w_tok2 = jnp.einsum('bcj,bsc->js', act_tok, d_after_bf, preferred_element_type=F32)
    d_act_tok = jnp.einsum('bsc,js->bcj', d_after_bf, w_tok2, preferred_element_type=F32)
    d_hid_tok = gelu_grad(hid_tok, d_act_tok)
    d_hid_tok_bf = d_hid_tok.astype(BF16)
    g_b_tok1 = jnp.sum(d_hid_tok, axis=(0, 1))
    g_w_tok1 = jnp.einsum('bsc,bcj->sj', normed, d_hid_tok_bf, preferred_element_type=F32)
    d_normed = jnp.einsum('bcj,sj->bsc', d_hid_tok_bf, w_tok1, preferred_element_type=F32)
    d_in_ln, g_ln1_g, g_ln1_b = norm_grad(x_in, ln1_g, ln1_b, d_normed)
    d_in = d_in_ln + d_after
    tok_flat = jnp.concatenate([g_w_tok1.reshape(-1, 128), g_w_tok2.reshape(-1, 128)])
    vec_flat = jnp.concatenate([g_ln1_g, g_ln1_b, g_b_tok1, g_b_tok2, g_ln2_g, g_ln2_b, g_b_ch1, g_b_ch2])
    vec_flat = jnp.pad(vec_flat, (0, (SH - VEC0) * 128 - vec_flat.shape[0])).reshape(-1, 128)
    return d_in, (g_w_ch1, g_w_ch2, tok_flat, vec_flat)


def head_step(hidden, labels, lnf_g, lnf_b, head_b, head_full, global_b):
    num_tokens = hidden.shape[1]
    normed = layer_norm(hidden, lnf_g, lnf_b)
    pooled = (jnp.sum(normed, axis=1, dtype=F32) / num_tokens).astype(BF16)
    logits = jnp.dot(pooled, head_full, preferred_element_type=F32) + head_b.astype(F32)
    log_norm = jax.nn.logsumexp(logits, axis=-1)
    is_label = jnp.arange(NCLS)[None, :] == labels[:, None]
    picked = jnp.sum(jnp.where(is_label, logits, 0.0), axis=-1)
    loss_sum = jnp.sum(log_norm - picked)
    d_logits = (jnp.exp(logits - log_norm[:, None]) - is_label.astype(F32)) / global_b
    d_logits_bf = d_logits.astype(BF16)
    g_head_b = jnp.sum(d_logits, axis=0)
    g_head_w = jnp.einsum('bc,bk->ck', pooled, d_logits_bf, preferred_element_type=F32)
    d_pooled = jnp.einsum('bk,ck->bc', d_logits_bf, head_full, preferred_element_type=F32)
    d_normed = jnp.broadcast_to((d_pooled / num_tokens)[:, None, :], normed.shape)
    d_hidden, g_lnf_g, g_lnf_b = norm_grad(hidden, lnf_g, lnf_b, d_normed)
    g_small = jnp.concatenate([g_lnf_g, g_lnf_b, g_head_b])
    return loss_sum, d_hidden, g_head_w, g_small


VEC_SIZES = (CH, CH, TH, TOK, CH, CH, HID, CH)


def unpack_vectors(vec):
    flat, out, at = vec.reshape(-1), [], 0
    for n in VEC_SIZES:
        out.append(flat[at:at + n])
        at += n
    return out


def view(a):
    return a.reshape(2, SH, 128).transpose(1, 0, 2)


def unview(a):
    return a.transpose(1, 0, 2).reshape(2, SH * 128)


def solution(mesh):
    row_spec = P('fsdp')
    layer_spec = P(None, 'fsdp')
    in_specs = (row_spec, row_spec, layer_spec, row_spec, row_spec, layer_spec, row_spec, row_spec, layer_spec, row_spec, row_spec)
    out_specs = (P(),) + in_specs[2:]

    def device_step(act_in, labels, layer_p, head_w, small_p, layer_m, head_m, small_m, layer_v, head_v, small_v):
        global_b = act_in.shape[0] * NDEV
        small8 = jnp.pad(small_p.reshape(3, 128), ((0, 5), (0, 0)))
        w1, w2, tok, vec, head_full, small_slots = gather_all(view(layer_p), head_w, small8)
        small_full = small_slots[:, :3].reshape(-1)
        weights = []
        for l in range(2):
            wt1 = tok[l, :T1 // 2].reshape(TOK, TH)
            wt2 = tok[l, T1 // 2:].reshape(TH, TOK)
            weights.append([wt1, wt2, w1[l], w2[l]] + unpack_vectors(vec[l]))
        hidden, caches = act_in, []
        for l in range(2):
            hidden, cache = layer_forward(hidden, weights[l])
            caches.append(cache)
        loss_sum, d_hidden, g_head_w, g_small = head_step(
            hidden, labels, small_full[:CH], small_full[CH:2 * CH], small_full[2 * CH:2 * CH + NCLS], head_full, global_b)
        shards = [None, None]
        for l in (1, 0):
            d_hidden, grads = layer_backward(d_hidden, weights[l], caches[l])
            shards[l] = reduce_layer(*grads, cid=1 + l)
        head_g = lax.psum_scatter(g_head_w, 'fsdp', scatter_dimension=0, tiled=True)
        small_flat = jnp.pad(g_small, (0, 3072 - g_small.shape[0]))
        small_g = lax.psum_scatter(small_flat, 'fsdp', scatter_dimension=0, tiled=True)
        sq_local = sum(jnp.sum(jnp.square(g)) for g in (shards[0], shards[1], head_g, small_g))
        loss_value, sq = lax.psum((loss_sum, sq_local), 'fsdp')
        clip_scale = 1.0 / jnp.maximum(1.0, jnp.sqrt(sq))
        new_l = adam_layers(view(layer_p), view(layer_m), view(layer_v), shards[0], shards[1], clip_scale.reshape(1, 1))
        new_lp, new_lm, new_lv = [unview(a) for a in new_l]
        new_hw, new_hm, new_hv = adam_math(head_w, head_g * clip_scale, head_m, head_v, WEIGHT_DECAY)
        new_sp, new_sm, new_sv = adam_math(small_p, small_g * clip_scale, small_m, small_v, 0.0)
        return (loss_value / global_b, new_lp, new_hw, new_sp, new_lm, new_hm, new_sm, new_lv, new_hv, new_sv)

    return jax.shard_map(device_step, mesh=mesh, in_specs=in_specs, out_specs=out_specs, check_vma=False)
```

```python
import functools
import math

import jax
import jax.numpy as jnp
from jax import lax
from jax.experimental import pallas as pl
from jax.experimental.pallas import tpu as pltpu
from jax.sharding import PartitionSpec as P

F32, BF16 = jnp.float32, jnp.bfloat16
ZERO = 0
ONE = 1
TWO = 2
THREE = 3
FOUR = 4
FIVE = 5
SIX = 6
EIGHT = 8
SIXTEEN = 16
LANES = 128
TWO_TILES = 256
SEVEN = 7
LN_EPS = 1e-6
LEARN_RATE = 0.003
BETA_ONE = 0.9
BETA_TWO = 0.999
ADAM_EPS = 1e-8
WEIGHT_DECAY = 0.03
ADAM_STEP = 10

NDEV = EIGHT
TOK, CH, TH, HID, NCLS = 196, 768, 384, 3072, 1000
SH = 4763
T1 = TWO * TOK * TH // LANES
RW = CH * HID // LANES
C1, C2 = HID // LANES, CH // LANES
VEC0 = T1 + TWO * RW - SEVEN * SH
MARG = 384
GROUP = FOUR
GR = GROUP * TOK
ROWS = 24 * TOK
WIN = 208
MESH = pl.DeviceIdType.MESH
ANY = pl.BlockSpec(memory_space=pl.ANY)
VMEM = pl.BlockSpec(memory_space=pltpu.VMEM)


def c1_span(d):
    return max(ZERO, SH * d - T1), min(RW, SH * (d + ONE) - T1)


def c2_span(d):
    return max(ZERO, SH * d - T1 - RW), min(RW, SH * (d + ONE) - T1 - RW)


def tiles_of(span, per):
    lo, hi = span
    if lo >= hi:
        return ZERO, ZERO
    return lo // per, -(-hi // per)


def edges(span_of, per):
    out = []
    for d in range(NDEV):
        lo, hi = span_of(d)
        if lo < hi and lo > ZERO and lo % per:
            out.append((d, lo // per, lo % per))
    return out


EDGE1 = edges(c1_span, SIXTEEN * C1)
EDGE2 = edges(c2_span, SIXTEEN * C2)


def matrix_moves(d, s1, s2, w1, w2, e1, e2):
    out = []
    for span_of, per, s, w, e, eds in ((c1_span, SIXTEEN * C1, s1, w1, e1, EDGE1), (c2_span, SIXTEEN * C2, s2, w2, e2, EDGE2)):
        lo, hi = tiles_of(span_of(d), per)
        if lo == hi:
            continue
        first = lo
        for k, (owner, row, _) in enumerate(eds):
            if owner == d:
                out.append((s.at[pl.ds(ZERO, SIXTEEN)], e.at[k]))
                first = lo + ONE
        n = hi - first
        out.append((s.at[pl.ds(SIXTEEN * (first - lo), SIXTEEN * n)], w.at[pl.ds(SIXTEEN * first, SIXTEEN * n)]))
    return out


def entry_barrier(me):
    barrier = pltpu.get_barrier_semaphore()
    for rel in (ONE, TWO, FOUR, SIX):
        pl.semaphore_signal(barrier, inc=ONE, device_id=(peer(me, rel),), device_id_type=MESH)
    pl.semaphore_wait(barrier, FOUR)


def peer(me, rel):
    t = me
    if rel & ONE:
        t = t + ONE - TWO * lax.rem(me, TWO)
    if rel & TWO:
        t = t + TWO - FOUR * lax.rem(me // TWO, TWO)
    if rel & FOUR:
        t = t + FOUR - EIGHT * (me // FOUR)
    return t


RELS = (TWO, FOUR, SIX)


class Spread:
    def __init__(self, pieces, send_sem, recv_sem, fwd_sem):
        self.pieces, self.send_sem, self.recv_sem, self.fwd_sem = pieces, send_sem, recv_sem, fwd_sem
        self.me = lax.axis_index("fsdp")

    def copies(self, d, k, rel):
        return [pltpu.make_async_remote_copy(src_ref=a, dst_ref=b, send_sem=self.send_sem.at[k, i], recv_sem=self.recv_sem.at[d, i], device_id=(d ^ rel,), device_id_type=MESH)
                for i, (a, b) in enumerate(self.pieces(d))]

    def handed(self, s, to):
        return [pltpu.make_async_remote_copy(src_ref=b, dst_ref=b, send_sem=self.fwd_sem.at[s, i], recv_sem=self.recv_sem.at[s, i], device_id=(to,), device_id_type=MESH)
                for i, (_, b) in enumerate(self.pieces(s))]

    def each(self, rels, body):
        for rel in rels:
            for s in range(NDEV):
                if self.pieces(s):
                    pl.when(self.me == s ^ rel)(functools.partial(body, s, rel))

    def start(self):
        def body(d, _):
            for k, rel in enumerate(ORDER):
                for copy in self.copies(d, k, rel):
                    copy.start()
        self.each((ZERO,), body)

    def hand_on(self, rels):
        def body(s, rel):
            for copy in self.handed(s, s ^ rel ^ ONE):
                copy.wait_recv()
            for copy in self.handed(s, s ^ rel ^ ONE):
                copy.start()
        self.each(rels, body)

    def arrive(self):
        def body(s, rel):
            for copy in self.handed(s, s):
                copy.wait_recv()
        self.each((ONE, THREE, FIVE, SEVEN), body)

    def sent(self):
        def own(d, _):
            for k, rel in enumerate(ORDER):
                for copy in self.copies(d, k, rel):
                    copy.wait_send()
        self.each((ZERO,), own)

        def other(s, rel):
            for copy in self.handed(s, s ^ rel ^ ONE):
                copy.wait_send()
        self.each(RELS, other)


ORDER = (FOUR, TWO, SIX, ONE)


def merge_edges(w1, w2, e1, e2, m1, m2, sem):
    jobs = [(k, per, w.at[pl.ds(SIXTEEN * row, SIXTEEN)], e.at[k], m, below)
            for per, w, e, m, eds in ((C1, w1, e1, m1, EDGE1), (C2, w2, e2, m2, EDGE2)) for k, (_, row, below) in enumerate(eds)]
    loads = [pltpu.make_async_copy(src, m.at[i, k], sem.at[i, n]) for n, (k, _, w, e, m, _) in enumerate(jobs) for i, src in enumerate((w, e))]
    stores = [pltpu.make_async_copy(m.at[ZERO, k], w, sem.at[ZERO, n]) for n, (k, _, w, e, m, _) in enumerate(jobs)]
    for copy in loads:
        copy.start()
    for copy in loads:
        copy.wait()
    for k, per, _, _, m, below in jobs:
        shape = (SIXTEEN, LANES * per)
        pos = lax.broadcasted_iota(jnp.int32, shape, ZERO) * per + lax.broadcasted_iota(jnp.int32, shape, ONE) // LANES
        m[ZERO, k] = jnp.where(pos < below, m[ZERO, k].astype(F32), m[ONE, k].astype(F32)).astype(BF16)
    for copy in stores:
        copy.start()
    for copy in stores:
        copy.wait()


def edge_scratch():
    return [pltpu.VMEM((TWO, len(EDGE1), SIXTEEN, HID), BF16), pltpu.VMEM((TWO, len(EDGE2), SIXTEEN, CH), BF16), pltpu.SemaphoreType.DMA((TWO, len(EDGE1) + len(EDGE2)))]


def spread_sems(n):
    dma = pltpu.SemaphoreType.DMA
    return [dma((len(ORDER), n)), dma((NDEV, n)), dma((NDEV, n))]


def lay_token_weights(tok, flat, nat, wt1s, wt2s, wt1t, wt2t):
    flat[ZERO:T1, :] = tok[...].astype(F32)
    period = LANES * TOK // math.gcd(LANES, TOK)
    nrow, npos = period // LANES, period // TOK
    reps = TH // npos
    lane = lax.broadcasted_iota(jnp.int32, (reps, LANES), ONE)
    for j in range(npos):
        f, o = divmod(TOK * j, LANES)
        rows = [flat[pl.ds(T1 // TWO + f + i, reps, stride=nrow), :] for i in range(THREE)]
        for i in range(TWO):
            part = jnp.where(lane >= o, rows[i], rows[i + ONE])
            nat[i, pl.ds(j, reps, stride=npos), :] = pltpu.roll(part, (LANES - o) % LANES, axis=ONE) if o else part
    two_t = jnp.concatenate([nat[ZERO].T, nat[ONE].T], axis=ZERO)
    for i in range(GROUP):
        for s, t, ref_n in ((wt2t, wt2s, two_t), (wt1s, wt1t, None)):
            flat[T1:T1 + WIN, :] = jnp.zeros((WIN, LANES), F32)
            for c in range(TH // LANES):
                lanes_ = slice(LANES * c, LANES * c + LANES)
                part = flat[pl.ds(c, TOK, stride=TH // LANES), :] if ref_n is None else ref_n[ZERO:TOK, lanes_]
                flat[T1 + FOUR * i:T1 + FOUR * i + TOK, :] = part
                full = flat[T1:T1 + WIN, :]
                s[i, :, lanes_] = full.astype(BF16)
                t[i, lanes_, :] = full.T.astype(BF16)


def lay_bias_vectors(vec, vf, bt1, bt2, cv, b1):
    vf[...] = vec[...].astype(F32)

    def put(ref, row, first, n, src):
        for c in range(n // LANES):
            ref[row:row + ONE, LANES * c:LANES * c + LANES] = src[first + c:first + c + ONE, :]

    ng, nt = CH // LANES, TH // LANES
    put(cv, ZERO, ZERO, CH, vf)
    put(cv, ONE, ng, CH, vf)
    for c in range(nt):
        bt1[LANES * c:LANES * c + LANES, :] = jnp.broadcast_to(vf[TWO * ng + c:TWO * ng + c + ONE, :], (LANES, LANES)).T
    at = TWO * ng + nt
    cols = [jnp.broadcast_to(vf[at + i:at + i + ONE, :], (LANES, LANES)).T for i in range(TWO)]
    cut = TOK - LANES
    for i in range(GROUP):
        bt2[i] = jnp.zeros((WIN, LANES), F32)
        bt2[i, FOUR * i:FOUR * i + LANES, :] = cols[ZERO]
        bt2[i, FOUR * i + LANES:FOUR * i + TOK, :] = cols[ONE][ZERO:cut, :]
    n = vf.shape[ZERO] - at - TWO
    lane = lax.broadcasted_iota(jnp.int32, (n, LANES), ONE)
    rest = pltpu.roll(jnp.where(lane >= cut, vf[at + ONE:at + ONE + n, :], vf[at + TWO:at + TWO + n, :]), LANES - cut, axis=ONE)
    vf[ZERO:n, :] = rest
    put(cv, TWO, ZERO, CH, vf)
    put(cv, THREE, ng, CH, vf)
    put(b1, ZERO, TWO * ng, HID, vf)
    put(cv, FOUR, TWO * ng + HID // LANES, CH, vf)


def gather_kernel(p_ref, head_ref, small_ref, w1, w2, st1, st2, headf, *rest):
    (tw0, tw1, (fv, hb)), rest = (rest[ZERO:EIGHT], rest[EIGHT:SIXTEEN], rest[SIXTEEN:18]), rest[18:]
    (e1, e2, xs, s1, s2, stok, svec, shead, ssmall, tok, vec, smallf, flat, nat, vf, m1, m2, ed_sem, ld_sem, stage_sem, own_sem), rest = rest[:21], rest[21:]
    me = lax.axis_index("fsdp")
    loads = [pltpu.make_async_copy(p_ref.at[:, l, :], xs.at[l, pl.ds(MARG, SH)], ld_sem.at[l]) for l in range(TWO)]
    for copy in loads:
        copy.start()
    shead[...] = head_ref[...].astype(BF16)
    ssmall[...] = small_ref[...].astype(BF16).astype(F32)

    def early(d):
        out = [(ssmall, smallf.at[d])]
        if d == ZERO:
            out += [(stok.at[l], tok.at[l]) for l in range(TWO)]
        if d == NDEV - ONE:
            out += [(svec.at[l], vec.at[l]) for l in range(TWO)]
        return out

    def matrices(d):
        return matrix_moves(d, s1.at[ZERO], s2.at[ZERO], w1, w2, e1, e2)

    def classes(d):
        return [(shead, headf.at[pl.ds(HROWS * d, HROWS)])]

    jobs = [Spread(f, *rest[THREE * i:THREE * i + THREE]) for i, f in enumerate((early, matrices, classes))]

    def keep_own(d, _):
        return [pltpu.make_async_copy(a, b, own_sem.at[i]) for i, (a, b) in enumerate(matrices(d) + classes(d))]

    for copy in loads:
        copy.wait()

    @pl.when(me == ZERO)
    def _():
        stok[...] = xs[:, MARG:MARG + T1, :].astype(BF16)
        tok[...] = stok[...]

    @pl.when(me == NDEV - ONE)
    def _():
        svec[...] = xs[:, MARG + VEC0:MARG + SH, :].astype(BF16)
        vec[...] = svec[...]

    entry_barrier(me)
    jobs[ZERO].start()

    def tile(l):
        def body(d, _):
            for span_of, per, s, skip in ((c1_span, C1, s1, T1 if d == ZERO else ZERO), (c2_span, C2, s2, max(ZERO, c1_span(d)[ONE] - c1_span(d)[ZERO]))):
                lo, hi = tiles_of(span_of(d), SIXTEEN * per)
                base0 = SIXTEEN * per * lo - span_of(d)[ZERO] + MARG + skip

                def one(i, carry, per=per, s=s, base0=base0):
                    row = pl.multiple_of(i * SIXTEEN, SIXTEEN)
                    for c in range(per):
                        s[l, pl.ds(row, SIXTEEN), LANES * c:LANES * c + LANES] = xs[l, pl.ds(base0 + c + i * (SIXTEEN * per), SIXTEEN, stride=per), :].astype(BF16)
                    return carry

                if lo < hi:
                    lax.fori_loop(ZERO, hi - lo, one, ZERO)
        jobs[ZERO].each((ZERO,), body)

    tile(ZERO)
    jobs[ONE].start()
    jobs[TWO].start()
    for d in range(NDEV):
        @pl.when(me == d)
        def _():
            smallf[d] = ssmall[...]
            for copy in keep_own(d, ZERO):
                copy.start()
    tile(ONE)
    stage = [pltpu.make_async_copy(a.at[ONE], b, stage_sem.at[i]) for i, (a, b) in enumerate(((s1, st1), (s2, st2)))]
    for copy in stage:
        copy.start()
    jobs[ZERO].hand_on(RELS)
    jobs[ZERO].arrive()
    for l, (wt1s, wt2s, wt1t, wt2t, bt1, bt2, cv, b1) in enumerate((tw0, tw1)):
        lay_token_weights(tok.at[l], flat, nat, wt1s, wt2s, wt1t, wt2t)
        lay_bias_vectors(vec.at[l], vf, bt1, bt2, cv, b1)
    for d in range(NDEV):
        flat[THREE * d:THREE * d + THREE, :] = smallf[d, ZERO:THREE, :]
    for i in range(TWO):
        for c in range(CH // LANES):
            fv[i:i + ONE, LANES * c:LANES * c + LANES] = flat[C2 * i + c:C2 * i + c + ONE, :]
    for c in range(NCP // LANES):
        hb[ZERO:ONE, LANES * c:LANES * c + LANES] = flat[TWO * C2 + c:TWO * C2 + c + ONE, :]
    for rel in ORDER[:THREE]:
        jobs[ONE].hand_on((rel,))
    jobs[TWO].hand_on(RELS)
    jobs[ONE].arrive()
    jobs[TWO].arrive()
    for job in jobs:
        job.sent()
    for d in range(NDEV):
        @pl.when(me == d)
        def _():
            for copy in keep_own(d, ZERO):
                copy.wait()
    merge_edges(w1, w2, e1, e2, m1, m2, ed_sem)
    for copy in stage:
        copy.wait()


STAGE1 = max(SIXTEEN * (b - a) for a, b in (tiles_of(c1_span(d), SIXTEEN * C1) for d in range(NDEV)))
STAGE2 = max(SIXTEEN * (b - a) for a, b in (tiles_of(c2_span(d), SIXTEEN * C2) for d in range(NDEV)))


def gather_all(p_view, head_w, small8):
    sds = jax.ShapeDtypeStruct
    per_layer = [sds((GROUP, WIN, TH), BF16), sds((GROUP, TH, WIN), BF16), sds((GROUP, TH, WIN), BF16), sds((GROUP, WIN, TH), BF16),
                 sds((TH, LANES), F32), sds((GROUP, WIN, LANES), F32), sds((EIGHT, CH), F32), sds((EIGHT, HID), F32)]
    far = [sds((CH, HID), BF16), sds((HID, CH), BF16), sds((STAGE1, HID), BF16), sds((STAGE2, CH), BF16), sds((CH, NCLS), BF16)]
    near = per_layer * TWO + [sds((EIGHT, CH), F32), sds((EIGHT, NCP), F32)]
    edge = [sds((len(EDGE1), SIXTEEN, HID), BF16), sds((len(EDGE2), SIXTEEN, CH), BF16)]
    dma = pltpu.SemaphoreType.DMA
    nv = SH - VEC0
    outs = pl.pallas_call(
        gather_kernel,
        in_specs=[ANY, VMEM, VMEM],
        out_specs=[ANY] * len(far) + [VMEM] * len(near) + [ANY] * TWO,
        out_shape=far + near + edge,
        scratch_shapes=[pltpu.VMEM((TWO, SH + TWO * MARG + FIVE, LANES), F32), pltpu.VMEM((TWO, STAGE1, HID), BF16), pltpu.VMEM((TWO, STAGE2, CH), BF16),
                        pltpu.VMEM((TWO, T1, LANES), BF16), pltpu.VMEM((TWO, nv, LANES), BF16), pltpu.VMEM((HROWS, NCLS), BF16), pltpu.VMEM((EIGHT, LANES), F32),
                        pltpu.VMEM((TWO, T1, LANES), BF16), pltpu.VMEM((TWO, nv, LANES), BF16), pltpu.VMEM((NDEV, EIGHT, LANES), F32),
                        pltpu.VMEM((T1 + WIN + EIGHT, LANES), F32), pltpu.VMEM((TWO, TH, LANES), F32), pltpu.VMEM((nv, LANES), F32)] + edge_scratch()
        + [dma((TWO,)), dma((TWO,)), dma((SIX,))] + spread_sems(THREE) + spread_sems(FOUR) + spread_sems(ONE),
        compiler_params=pltpu.CompilerParams(collective_id=ZERO, has_side_effects=True, vmem_limit_bytes=60000000),
        name="gather_weights",
    )(p_view, head_w, small8)
    n = len(far)
    return outs[:n], outs[n:n + EIGHT], outs[n + EIGHT:n + SIXTEEN], outs[n + SIXTEEN:n + 18]


def g1_rows(d):
    lo, hi = tiles_of(c1_span(d), EIGHT * C1)
    return EIGHT * lo, EIGHT * hi


def g2_rows(d):
    lo, hi = tiles_of(c2_span(d), EIGHT * C2)
    return EIGHT * lo, EIGHT * hi


QUART = HID // CH
HALF = CH // TWO
BLK = max(QUART * (g1_rows(d)[ONE] - g1_rows(d)[ZERO]) + g2_rows(d)[ONE] - g2_rows(d)[ZERO] for d in range(NDEV))


def core_rows(s):
    lo, hi = g1_rows(s)
    return QUART * (hi - lo) + g2_rows(s)[ONE] - g2_rows(s)[ZERO]


def share_pieces(s, dw1, dw2, tok=None, vec=None):
    lo, hi = g1_rows(s)
    full = pl.ds(ZERO, CH)
    out = [(dw1.at[q, pl.ds(lo, hi - lo)], pl.ds(q * (hi - lo), hi - lo), full) for q in range(QUART) if lo < hi]
    at = QUART * (hi - lo)
    lo, hi = g2_rows(s)
    if lo < hi:
        out.append((dw2.at[pl.ds(lo, hi - lo)], pl.ds(at, hi - lo), full))
    if tok is not None and s == ZERO:
        out.append((tok, pl.ds(core_rows(s), TROWS), full))
    if vec is not None and s == NDEV - ONE:
        out.append((vec, pl.ds(core_rows(s), VROWS), full))
    return list(enumerate(out))


NCP = 1024
HROWS = CH // NDEV
TROWS, VROWS = 200, SIXTEEN


def add_into(dst, src, n):
    def one(i, carry):
        at = pl.ds(pl.multiple_of(i * SIXTEEN, SIXTEEN), SIXTEEN)
        dst[at, :] = dst[at, :] + src[at, :]
        return carry
    lax.fori_loop(ZERO, n // SIXTEEN, one, ZERO)


class Reduction:
    def __init__(self, given, red, sums, own, ld, ps, pr, hs, hr, out_sem, free):
        self.given, self.red, self.sums, self.own, self.free = given, red, sums, own, free
        self.n = red.shape[ONE]
        self.ld, self.ps, self.pr, self.hs, self.hr, self.out_sem = ld, ps, pr, hs, hr, out_sem
        self.me = lax.axis_index("fsdp")
        chip = self.me // TWO
        px, py = lax.rem(chip, TWO), chip // TWO
        self.k, self.kx, self.ky = chip, chip + ONE - TWO * px, chip + TWO - FOUR * py
        self.kd = self.kx + TWO - FOUR * py

    def per_core(self, body):
        for c in range(TWO):
            @pl.when(lax.rem(self.me, TWO) == c)
            def _():
                body(c)

    def load(self, k, c):
        return [pltpu.make_async_copy(src, self.own.at[k % TWO, rows, lanes_], self.ld.at[k % TWO, i]) for i, (src, rows, lanes_) in share_pieces(TWO * k + c, *self.given)]

    def give(self, k, c):
        return [pltpu.make_async_remote_copy(src_ref=src, dst_ref=self.sums.at[k, rows, lanes_], send_sem=self.ps.at[k, i], recv_sem=self.pr.at[k, i], device_id=(peer(self.me, ONE),), device_id_type=MESH)
                for i, (src, rows, lanes_) in share_pieces(TWO * k + c, *self.given)]

    def hop(self, i, src, dst, rel):
        return pltpu.make_async_remote_copy(src_ref=src, dst_ref=dst, send_sem=self.hs.at[i], recv_sem=self.hr.at[i], device_id=(peer(self.me, rel),), device_id_type=MESH)

    def left(self, ref, k):
        return ref.at[k, :, pl.ds(ZERO, HALF)]

    def right(self, ref, k):
        return ref.at[k, :, pl.ds(HALF, HALF)]

    def ready(self, i):
        for rel in (TWO, FOUR):
            pl.semaphore_signal(self.free.at[i], inc=ONE, device_id=(peer(self.me, rel),), device_id_type=MESH)
        pl.semaphore_wait(self.free.at[i], TWO)

    def first_hops(self):
        return [self.hop(ZERO, self.left(self.sums, self.kx), self.left(self.own, ZERO), TWO), self.hop(ONE, self.left(self.sums, self.kd), self.left(self.own, ONE), TWO),
                self.hop(TWO, self.right(self.sums, self.ky), self.right(self.own, ZERO), FOUR), self.hop(THREE, self.right(self.sums, self.kd), self.right(self.own, ONE), FOUR)]

    def begin(self):
        barrier = pltpu.get_barrier_semaphore()
        for rel in (ONE, TWO, FOUR):
            pl.semaphore_signal(barrier, inc=ONE, device_id=(peer(self.me, rel),), device_id_type=MESH)
        pl.semaphore_wait(barrier, THREE)

        def body(c):
            for k in range(FOUR):
                for copy in self.give(k, ONE - c):
                    copy.start()
            for k in range(TWO):
                for copy in self.load(k, c):
                    copy.start()
        self.per_core(body)

    def partner_done(self):
        for k in range(FOUR):
            def wait(c):
                for copy in self.load(k, c):
                    copy.wait()
                for copy in self.give(k, c):
                    copy.wait_recv()
            self.per_core(wait)
            add_into(self.sums.at[k], self.own.at[k % TWO], self.n)
            if k < TWO:
                def more(c):
                    for copy in self.load(k + TWO, c):
                        copy.start()
                self.per_core(more)
        self.ready(ZERO)
        for copy in self.first_hops():
            copy.start()

    def first_done(self):
        for copy in self.first_hops():
            copy.wait_recv()
        add_into(self.sums.at[self.k], self.own.at[ZERO], self.n)
        add_into(self.left(self.sums, self.ky), self.left(self.own, ONE), self.n)
        add_into(self.right(self.sums, self.kx), self.right(self.own, ONE), self.n)
        outs = self.outputs()
        for copy in outs:
            copy.start()

    def outputs(self):
        own, left, right = self.red.at[ZERO], self.red.at[ONE, :, pl.ds(ZERO, HALF)], self.red.at[ONE, :, pl.ds(HALF, HALF)]
        pairs = (self.sums.at[self.k], own), (self.left(self.sums, self.ky), left), (self.right(self.sums, self.kx), right)
        return [pltpu.make_async_copy(a, b, self.out_sem.at[i]) for i, (a, b) in enumerate(pairs)]

    def finish(self):
        for copy in self.first_hops():
            copy.wait_send()

        def body(c):
            for k in range(FOUR):
                for copy in self.give(k, ONE - c):
                    copy.wait_send()
        self.per_core(body)
        for copy in self.outputs():
            copy.wait()


def last_hops(red, late, send, recv, me):
    out = []
    for i, rel in enumerate((FOUR, TWO)):
        part = pl.ds(HALF * i, HALF)
        out.append(pltpu.make_async_remote_copy(src_ref=red.at[ONE, :, part], dst_ref=late.at[:, part], send_sem=send.at[i], recv_sem=recv.at[i], device_id=(peer(me, rel),), device_id_type=MESH))
    return out


def reduction_scratch(n):
    dma = pltpu.SemaphoreType.DMA
    pieces = QUART + TWO
    return [pltpu.VMEM((FOUR, n, CH), F32), pltpu.VMEM((TWO, n, CH), F32),
            dma((TWO, pieces)), dma((FOUR, pieces)), dma((FOUR, pieces)), dma((FOUR,)), dma((FOUR,)), dma((THREE,)), pltpu.SemaphoreType.REGULAR((ONE,))]


def untile(block, flat, d):
    lo, hi = g1_rows(d)
    n1 = hi - lo
    jobs = [(q * n1, n1, C1, C1 * lo - c1_span(d)[ZERO] + (T1 if d == ZERO else ZERO) + C2 * q) for q in range(QUART) if n1]
    lo, hi = g2_rows(d)
    if lo < hi:
        jobs.append((QUART * n1, hi - lo, C2, C2 * lo - c2_span(d)[ZERO] + max(ZERO, c1_span(d)[ONE] - c1_span(d)[ZERO])))
    for at, n, stride, base in jobs:
        def one(i, carry, at=at, stride=stride, base=base):
            rows = pl.ds(pl.multiple_of(at + EIGHT * i, EIGHT), EIGHT)
            for c in range(C2):
                flat[pl.ds(MARG + base + c + i * (EIGHT * stride), EIGHT, stride=stride), :] = block[rows, LANES * c:LANES * c + LANES]
            return carry
        lax.fori_loop(ZERO, n // EIGHT, one, ZERO)


def adam_math(p, g, m, v, decay):
    m_new = BETA_ONE * m + (1.0 - BETA_ONE) * g
    v_new = BETA_TWO * v + (1.0 - BETA_TWO) * g * g
    m_hat = m_new / (1.0 - BETA_ONE ** ADAM_STEP)
    v_hat = v_new / (1.0 - BETA_TWO ** ADAM_STEP)
    p_new = p - LEARN_RATE * (m_hat / (jnp.sqrt(v_hat) + ADAM_EPS) + decay * p)
    return p_new, m_new, v_new


NVIEW = 40
CHUNK = 1200
NCHUNK = FOUR
GROWS = CHUNK * NCHUNK
EXR = 32
LOSS_ROW = 24


def chunk_rows(k):
    return k * CHUNK, min(SH, (k + ONE) * CHUNK) - k * CHUNK


def lay_tokens(blk, r0, flat, flip, ta, tb):
    for c in range(TH // LANES):
        flat[pl.ds(MARG + c, TOK, stride=TH // LANES), :] = blk[r0:r0 + TOK, LANES * c:LANES * c + LANES]
    flip[:, ZERO:TROWS] = blk[r0:r0 + TROWS, TH:TWO * TH].T
    ta[ZERO:TH, :] = flip[:, ZERO:LANES]
    tb[ZERO:TH, :] = flip[:, LANES:TWO_TILES]
    period = LANES * TOK // math.gcd(LANES, TOK)
    nrow, npos = period // LANES, period // TOK
    reps = TH // npos
    lane = lax.broadcasted_iota(jnp.int32, (reps, LANES), ONE)
    for m in range(nrow):
        j, o = divmod(LANES * m, TOK)
        first = ta[pl.ds(j, reps, stride=npos), :]
        second = tb[pl.ds(j, reps, stride=npos), :]
        if o < LANES:
            row = pltpu.roll(jnp.where(lane >= o, first, second), (LANES - o) % LANES, axis=ONE) if o else first
        else:
            row = pltpu.roll(second, (TWO_TILES - o) % LANES, axis=ONE) if o > LANES else second
        if TOK - o < LANES:
            following = ta[pl.ds(j + ONE, reps, stride=npos), :]
            row = jnp.where(lane < TOK - o, row, pltpu.roll(following, TOK - o, axis=ONE))
        flat[pl.ds(MARG + T1 // TWO + m, reps, stride=nrow), :] = row


def lay_vectors(blk, r0, flat, va, vb):
    at = MARG + VEC0

    def pieces(row, n):
        return [blk[r0 + row:r0 + row + ONE, LANES * c:LANES * c + LANES] for c in range(n // LANES)]

    b_t2 = pieces(VROWS - SIX, TWO_TILES)
    plain = pieces(ZERO, CH) + pieces(ONE, CH) + pieces(9, TH) + b_t2[:ONE]
    for i, v in enumerate(plain):
        flat[at + i:at + i + ONE, :] = v
    moved = pieces(TWO, CH) + pieces(THREE, CH) + sum([pieces(FIVE + q, CH) for q in range(QUART)], []) + pieces(FOUR, CH)
    va[...] = jnp.zeros(va.shape, F32)
    for i, v in enumerate(moved):
        va[i:i + ONE, :] = v
    cut = TOK - LANES
    vb[ZERO:EIGHT, :] = jnp.broadcast_to(b_t2[ONE], (EIGHT, LANES))
    vb[EIGHT:EIGHT + va.shape[ZERO], :] = pltpu.roll(va[...], cut, axis=ONE)
    n = SH - VEC0 - len(plain)
    lane = lax.broadcasted_iota(jnp.int32, (n, LANES), ONE)
    flat[at + len(plain):MARG + SH, :] = jnp.where(lane < cut, vb[SEVEN:SEVEN + n, :], vb[EIGHT:EIGHT + n, :])


def finish_kernel(red0, red1, late1, heads, tok_ref, vec_ref, ex_ref, g_out, gh_out, gsm_out, loss_ref,
                  gs, r0, r1, l0, l1, tsum, tgot, vsum, vgot, ex, nrm, flip, ta, tb, va, vb, hparts,
                  g_sem, head_sem, red_sem, pair_s, pair_r, own_s, own_r, ex_s, ex_r, nm_s, nm_r, hop_s, hop_r):
    me = lax.axis_index("fsdp")
    core = lax.rem(me, TWO)
    others = [lax.rem(me + i, NDEV) for i in range(ONE, NDEV)]
    reds = [pltpu.make_async_copy(a, b, red_sem.at[i]) for i, (a, b) in enumerate(((red1.at[ZERO], r1), (late1, l1), (red0.at[ZERO], r0)))]
    heads_in = pltpu.make_async_copy(heads, hparts, head_sem)
    for copy in reds + [heads_in]:
        copy.start()
    ex[ZERO] = ex_ref[...]
    barrier = pltpu.get_barrier_semaphore()
    for dev in others:
        pl.semaphore_signal(barrier, inc=ONE, device_id=(dev,), device_id_type=MESH)
    pl.semaphore_wait(barrier, NDEV - ONE)

    def remote(src, dst, ss, rs, dev):
        return pltpu.make_async_remote_copy(src_ref=src, dst_ref=dst, send_sem=ss, recv_sem=rs, device_id=(dev,), device_id_type=MESH)

    give_tok = remote(tok_ref, tgot.at[THREE], pair_s, pair_r, peer(me, ONE))
    give_vec = remote(vec_ref, vgot.at[THREE], pair_s, pair_r, peer(me, ONE))
    pl.when(core == ONE)(give_tok.start)
    pl.when(core == ZERO)(give_vec.start)
    small = [remote(ex.at[ZERO], ex.at[i], ex_s.at[i], ex_r.at[i], others[i - ONE]) for i in range(ONE, NDEV)]
    for copy in small:
        copy.start()

    def to_owner(src, dst, rel, owner):
        slot = rel // TWO - ONE
        return remote(src, dst.at[slot], own_s.at[slot], own_r.at[slot], owner)

    sides = ((ZERO, ZERO, give_tok, tok_ref, tsum, tgot), (ONE, NDEV - ONE, give_vec, vec_ref, vsum, vgot))
    for c, owner, give, mine, total, got in sides:
        @pl.when(core == c)
        def _():
            give.wait_recv()
            total[...] = mine[...] + got[THREE]
            for rel in RELS:
                @pl.when(me == owner ^ rel)
                def _():
                    to_owner(total, got, rel, owner).start()
    hops = last_hops(red0, l0, hop_s, hop_r, me)
    for copy in hops:
        copy.start()
    for copy in reds:
        copy.wait()
    add_into(r1, l1, r1.shape[ZERO])

    def per_device(body):
        for d in range(NDEV):
            @pl.when(me == d)
            def _():
                body(d)

    per_device(lambda d: untile(r1, gs.at[ONE], d))
    heads_in.wait()
    g_head = hparts[ZERO]
    for d in range(ONE, NDEV):
        g_head = g_head + hparts[d]
    gh_out[...] = g_head[:, ZERO:NCLS]
    acc = fold_rows(fold_lanes(g_head * g_head))
    for copy in small:
        copy.wait_recv()
    first = lax.rem(NDEV - me, NDEV)
    tot = ex[first]
    for d in range(ONE, NDEV):
        tot = tot + ex[lax.rem(first + d, NDEV)]
    ta[ZERO:EXR, :] = tot
    loss_ref[...] = tot[LOSS_ROW:LOSS_ROW + EIGHT, :]
    g_small = ta[pl.ds(THREE * me, THREE), :]
    gsm_out[...] = g_small
    acc = acc + jnp.sum(g_small * g_small, axis=ZERO, keepdims=True) / EIGHT
    for c, owner, give, mine, total, got in sides:
        @pl.when(me == owner)
        def _():
            for rel in RELS:
                to_owner(total, got, rel, owner).wait_recv()
            total[...] = total[...] + got[ZERO] + (got[ONE] + got[TWO])
            if c == ZERO:
                lay_tokens(total, ZERO, gs.at[ZERO], flip, ta, tb)
            else:
                lay_vectors(total, ZERO, gs.at[ZERO], va, vb)
    for copy in hops:
        copy.wait_recv()
    add_into(r0, l0, r0.shape[ZERO])

    def rest_of(d):
        untile(r0, gs.at[ZERO], d)
        if d == ZERO:
            lay_tokens(r0, core_rows(ZERO), gs.at[ONE], flip, ta, tb)
        if d == NDEV - ONE:
            lay_vectors(r0, core_rows(NDEV - ONE), gs.at[ONE], va, vb)

    per_device(rest_of)
    flats = [pltpu.make_async_copy(gs.at[l, pl.ds(MARG, SH)], g_out.at[l], g_sem.at[l]) for l in range(TWO)]
    for copy in flats:
        copy.start()

    def square(i, carry):
        for l in range(TWO):
            part = gs[l, pl.ds(pl.multiple_of(MARG + i * NVIEW, EIGHT), NVIEW), :]
            carry = carry + fold_rows(part * part)
        return carry

    whole = SH // NVIEW
    acc = lax.fori_loop(ZERO, whole, square, acc)
    rest = SH - whole * NVIEW
    for l in range(TWO):
        part = gs[l, MARG + SH - rest:MARG + SH, :]
        acc = acc + jnp.sum(part * part, axis=ZERO, keepdims=True) / EIGHT
    nrm[ZERO] = acc
    norms = [remote(nrm.at[ZERO], nrm.at[i], nm_s.at[i], nm_r.at[i], others[i - ONE]) for i in range(ONE, NDEV)]
    for copy in norms:
        copy.start()
    for copy in norms:
        copy.wait_recv()
    tot = nrm[first]
    for d in range(ONE, NDEV):
        tot = tot + nrm[lax.rem(first + d, NDEV)]
    norm = jnp.sqrt(jnp.sum(jnp.sum(tot, axis=ZERO, keepdims=True), axis=ONE, keepdims=True))
    loss_ref[FOUR:EIGHT, :] = jnp.broadcast_to(1.0 / jnp.maximum(1.0, norm), (FOUR, LANES))
    for copy in small + norms + hops:
        copy.wait_send()
    for c, owner, give, mine, total, got in sides:
        pl.when(core != c)(give.wait_send)
        for rel in RELS:
            pl.when(me == owner ^ rel)(to_owner(total, got, rel, owner).wait_send)
    for copy in flats:
        copy.wait()


def finish(red0, red1, late1, heads, tok, vec, ex):
    sds = jax.ShapeDtypeStruct
    dma = pltpu.SemaphoreType.DMA
    blk0, blk1 = pltpu.VMEM(red0.shape[ONE:], F32), pltpu.VMEM(red1.shape[ONE:], F32)
    return pl.pallas_call(
        finish_kernel,
        in_specs=[ANY] * FOUR + [VMEM] * THREE,
        out_specs=[ANY] + [VMEM] * THREE,
        out_shape=[sds((TWO, SH, LANES), F32), sds((HROWS, NCLS), F32), sds((THREE, LANES), F32), sds((EIGHT, LANES), F32)],
        scratch_shapes=[pltpu.VMEM((TWO, GROWS + TWO * MARG, LANES), F32), blk0, blk1, blk0, blk1,
                        pltpu.VMEM((TROWS, CH), F32), pltpu.VMEM((FOUR, TROWS, CH), F32), pltpu.VMEM((VROWS, CH), F32), pltpu.VMEM((FOUR, VROWS, CH), F32),
                        pltpu.VMEM((NDEV, EXR, LANES), F32), pltpu.VMEM((NDEV, EIGHT, LANES), F32), pltpu.VMEM((TH, TWO_TILES), F32),
                        pltpu.VMEM((TH + EIGHT, LANES), F32), pltpu.VMEM((TH + EIGHT, LANES), F32), pltpu.VMEM((48, LANES), F32), pltpu.VMEM((56, LANES), F32), pltpu.VMEM((NDEV, HROWS, NCP), F32),
                        dma((TWO,)), dma, dma((THREE,)), dma, dma, dma((THREE,)), dma((THREE,)), dma((NDEV,)), dma((NDEV,)), dma((NDEV,)), dma((NDEV,)), dma((TWO,)), dma((TWO,))],
        compiler_params=pltpu.CompilerParams(collective_id=THREE, has_side_effects=True, vmem_limit_bytes=67000000),
        name="finish",
    )(red0, red1, late1, heads, tok, vec, ex)


def update_kernel(p_ref, m_ref, v_ref, g_ref, hg_ref, sg_ref, scale_ref, hp_ref, hm_ref, hv_ref, sp_ref, sm_ref, sv_ref,
                  po, mo, vo, hpo, hmo, hvo, spo, smo, svo, ps, ms, vs, gs, in_sem, out_sem):
    me = lax.axis_index("fsdp")
    ins = ((p_ref, ps), (m_ref, ms), (v_ref, vs))
    outs = ((ps, po), (ms, mo), (vs, vo))

    def loads(k):
        a, n = chunk_rows(k)
        rows = pl.ds(a, n)
        return [pltpu.make_async_copy(src.at[rows, l, :], dst.at[l, rows], in_sem.at[k, j, l]) for j, (src, dst) in enumerate(ins) for l in range(TWO)] + [
            pltpu.make_async_copy(g_ref.at[l, rows], gs.at[l, rows], in_sem.at[k, THREE, l]) for l in range(TWO)]

    def stores(k):
        a, n = chunk_rows(k)
        return [pltpu.make_async_copy(src.at[l, pl.ds(a, n)], dst.at[pl.ds(a, n), l, :], out_sem.at[k, j, l]) for j, (src, dst) in enumerate(outs) for l in range(TWO)]

    for k in range(NCHUNK):
        for copy in loads(k):
            copy.start()
    scale = scale_ref[FOUR:FIVE, ZERO:ONE]
    hpo[...], hmo[...], hvo[...] = adam_math(hp_ref[...], hg_ref[...] * scale, hm_ref[...], hv_ref[...], WEIGHT_DECAY)
    spo[...], smo[...], svo[...] = adam_math(sp_ref[...], sg_ref[...] * scale, sm_ref[...], sv_ref[...], 0.0)
    mat_rows = T1 + TWO * RW - me * SH
    for k in range(NCHUNK):
        for copy in loads(k):
            copy.wait()
        a, n = chunk_rows(k)
        for l in range(TWO):
            def one(i, carry, l=l, a=a):
                o = pl.multiple_of(a + i * NVIEW, EIGHT)
                row = o + lax.broadcasted_iota(jnp.int32, (NVIEW, LANES), ZERO)
                decay = jnp.where(row < mat_rows, WEIGHT_DECAY, 0.0)
                at = pl.ds(o, NVIEW)
                ps[l, at, :], ms[l, at, :], vs[l, at, :] = adam_math(ps[l, at, :], gs[l, at, :] * scale, ms[l, at, :], vs[l, at, :], decay)
                return carry
            lax.fori_loop(ZERO, -(-n // NVIEW), one, ZERO)
        for copy in stores(k):
            copy.start()
    for k in range(NCHUNK):
        for copy in stores(k):
            copy.wait()


def update(pv, mv, vv, g, head_g, small_g, scale, heads, smalls):
    sds = jax.ShapeDtypeStruct
    dma = pltpu.SemaphoreType.DMA
    big, hd, sm = sds((SH, TWO, LANES), F32), sds((HROWS, NCLS), F32), sds((THREE, LANES), F32)
    return pl.pallas_call(
        update_kernel,
        in_specs=[ANY] * FOUR + [VMEM] * 9,
        out_specs=[ANY] * THREE + [VMEM] * SIX,
        out_shape=[big] * THREE + [hd] * THREE + [sm] * THREE,
        scratch_shapes=[pltpu.VMEM((TWO, GROWS, LANES), F32)] * FOUR + [dma((NCHUNK, FOUR, TWO)), dma((NCHUNK, THREE, TWO))],
        compiler_params=pltpu.CompilerParams(vmem_limit_bytes=67000000),
        name="update",
    )(pv, mv, vv, g, head_g, small_g, scale, *heads, *smalls)

CG = math.sqrt(2.0 / math.pi)
CA = CG * 0.044715


def mm(a, b):
    return jnp.dot(a, b, preferred_element_type=F32)


def mm_t(a, b):
    return lax.dot_general(a, b, (((ONE,), (ONE,)), ((), ())), preferred_element_type=F32)


def cat6(col):
    return jnp.concatenate([col] * (CH // LANES), axis=ONE)


def norm_stats(x):
    mean = jnp.mean(x, axis=-ONE, keepdims=True)
    cent = x - mean
    rstd = lax.rsqrt(jnp.mean(cent * cent, axis=-ONE, keepdims=True) + LN_EPS)
    return cent * rstd, rstd


def gelu_of(x):
    t = jnp.tanh(x * (CG + CA * (x * x)))
    half = 0.5 * x
    return half + half * t


def gelu_and_grad(x, d):
    u = CA * (x * x)
    q = CG + u
    t = jnp.tanh(x * q)
    s = 1.0 + t
    act = 0.5 * x * s
    return act, d * (0.5 * s + act * (1.0 - t) * (q + (u + u)))


def load_group(x_ref, xf):
    if len(x_ref.shape) == THREE:
        for i in range(GROUP):
            xf[TOK * i:TOK * i + TOK, :] = x_ref[i].astype(F32)
    else:
        xf[...] = x_ref[...].astype(F32)


def forward_kernel(first, x_ref, wt1_ref, wt2_ref, bt1_ref, bt2_ref, w1_ref, w2_ref, cv_ref, b1_ref, *rest):
    if first:
        (st1, st2), rest = rest[:TWO], rest[TWO:]
    (x1_ref, ut_ref, hid_ref, h2_ref, x2_ref), rest = rest[:FIVE], rest[FIVE:]
    if first:
        (flat_ref, nw1, nw2, e1, e2), rest = rest[:FIVE], rest[FIVE:]
    (xf, hs, acts), rest = rest[:THREE], rest[THREE:]
    step = pl.program_id(ZERO)
    if first:
        m1, m2, ed_sem, own_sem, *sems = rest

        def pieces(d):
            return matrix_moves(d, st1, st2, nw1, nw2, e1, e2)

        job = Spread(pieces, *sems)

        def keep_own(act):
            def body(d, _):
                for i, (a, b) in enumerate(pieces(d)):
                    getattr(pltpu.make_async_copy(a, b, own_sem.at[i]), act)()
            job.each((ZERO,), body)

        @pl.when(step == ZERO)
        def _():
            entry_barrier(job.me)
            job.start()
            keep_own("start")

        pl.when(step == ROWS // GR - ONE)(functools.partial(job.hand_on, ORDER[:THREE]))
    load_group(x_ref, xf)
    if first:
        flat_ref[...] = xf[...].astype(BF16)
    nrm, _ = norm_stats(xf[...])
    hs[...] = (nrm * cv_ref[ZERO:ONE, :] + cv_ref[ONE:TWO, :]).astype(BF16)
    for i in range(GROUP):
        lo = 192 * i
        ut = mm(wt1_ref[i], hs[lo:lo + WIN, :]) + cat6(bt1_ref[...])
        ut_ref[i] = ut
        out = mm(wt2_ref[i], gelu_of(ut).astype(BF16)) + cat6(bt2_ref[i])
        xf[lo:lo + WIN, :] = xf[lo:lo + WIN, :] + out
    x1b = xf[...].astype(BF16)
    x1_ref[...] = x1b
    x1 = x1b.astype(F32)
    nrm2, _ = norm_stats(x1)
    h2_ref[...] = (nrm2 * cv_ref[TWO:THREE, :] + cv_ref[THREE:FOUR, :]).astype(BF16)
    for j in range(ZERO, HID, 512):
        hid = mm(h2_ref[...], w1_ref[:, j:j + 512]) + b1_ref[ZERO:ONE, j:j + 512]
        hid_ref[:, j:j + 512] = hid
        acts[:, j:j + 512] = gelu_of(hid).astype(BF16)
    x2_ref[...] = (x1_ref[...].astype(F32) + (mm(acts[...], w2_ref[...]) + cv_ref[FOUR:FIVE, :])).astype(BF16)

    if first:
        @pl.when(step == ROWS // GR - ONE)
        def _():
            job.arrive()
            job.sent()
            keep_own("wait")
            merge_edges(nw1, nw2, e1, e2, m1, m2, ed_sem)


def once(shape):
    return pl.BlockSpec(shape, lambda g: (ZERO,) * len(shape), pipeline_mode=pl.Buffered(ONE))


def by_group(shape):
    return pl.BlockSpec(shape, lambda g: (g,) + (ZERO,) * (len(shape) - ONE))


def forward_layer(x, wt1t, wt2t, bt1, bt2, w1, w2, cv, b1, stage=()):
    sds = jax.ShapeDtypeStruct
    first = x.ndim == THREE
    act = by_group((GR, CH))
    act_s = sds((ROWS, CH), BF16)
    outs = [act, by_group((GROUP, TH, CH)), by_group((GR, HID)), act, act]
    shapes = [act_s, sds((24, TH, CH), F32), sds((ROWS, HID), F32), act_s, act_s]
    scratch = [pltpu.VMEM((GR, CH), F32), pltpu.VMEM((GR, CH), BF16), pltpu.VMEM((GR, HID), BF16)]
    params = {}
    if first:
        outs += [act] + [ANY] * FOUR
        shapes += [act_s, sds((CH, HID), BF16), sds((HID, CH), BF16), sds((len(EDGE1), SIXTEEN, HID), BF16), sds((len(EDGE2), SIXTEEN, CH), BF16)]
        scratch += edge_scratch() + [pltpu.SemaphoreType.DMA((FOUR,))] + spread_sems(FOUR)
        params = {"collective_id": FOUR, "has_side_effects": True}
    return pl.pallas_call(
        functools.partial(forward_kernel, first),
        grid=(ROWS // GR,),
        in_specs=[by_group((GROUP, TOK, CH)) if first else act, once((GROUP, TH, WIN)), once((GROUP, WIN, TH)), once((TH, LANES)), once((GROUP, WIN, LANES)),
                  once((CH, HID)), once((HID, CH)), once((EIGHT, CH)), once((EIGHT, HID))] + [ANY] * len(stage),
        out_specs=outs,
        out_shape=shapes,
        scratch_shapes=scratch,
        compiler_params=pltpu.CompilerParams(vmem_limit_bytes=67000000, **params),
        name="forward_layer",
    )(x, wt1t, wt2t, bt1, bt2, w1, w2, cv, b1, *stage)

def fold_rows(a):
    return jnp.sum(a.reshape(a.shape[ZERO] // EIGHT, EIGHT, a.shape[ONE]), axis=ZERO)


def fold_lanes(a):
    tot = a[:, ZERO:LANES]
    for k in range(ONE, a.shape[ONE] // LANES):
        tot = tot + a[:, LANES * k:LANES * k + LANES]
    return tot


def norm_back(nrm, rstd, gain, d):
    dg = d * gain
    m1 = jnp.mean(dg, axis=-ONE, keepdims=True)
    m2 = jnp.mean(dg * nrm, axis=-ONE, keepdims=True)
    return rstd * (dg - m1 - nrm * m2)


SUB = 112


def backward_kernel(first, dh_ref, d2_ref, x1_ref, x_ref, ut_ref, w1_ref, wt1_ref, wt2_ref, cv_ref, gb1_ref, dw1, dw2, *rest):
    if first:
        tok1, vec1, *rest = rest
        given = dw1, dw2, tok1, vec1
    else:
        dx_ref, *rest = rest
        given = dw1, dw2
    tok_ref, vec_ref, red, gt1_ref, gt2_ref, gbt1_ref, gbt2_ref, gcv_ref, d1b, hs, dhf, acts, dus, *comm = rest
    step = pl.program_id(ZERO)
    job = Reduction(given, red, *comm)
    pl.when(step == ZERO)(job.begin)
    pl.when(step == TWO)(job.partner_done)

    @pl.when(step == ZERO)
    def _():
        for r in (gt1_ref, gt2_ref, gbt1_ref, gbt2_ref, gcv_ref):
            r[...] = jnp.zeros(r.shape, F32)

    def through_w1(c, carry):
        cols = pl.ds(pl.multiple_of(c * TWO_TILES, TWO_TILES), TWO_TILES)
        dhf[:, cols] = mm_t(dh_ref[...], w1_ref[cols, :])
        return carry

    lax.fori_loop(ZERO, CH // TWO_TILES, through_w1, ZERO)

    def norm_two(i, carry):
        rows = pl.ds(pl.multiple_of(i * SUB, SUB), SUB)
        d_n2 = dhf[rows, :].astype(BF16).astype(F32)
        nrm2, rstd2 = norm_stats(x1_ref[rows, :].astype(F32))
        d2 = d2_ref[rows, :].astype(F32)
        for k, part in ((TWO, d_n2 * nrm2), (THREE, d_n2), (FOUR, d2)):
            gcv_ref[k] += fold_rows(part)
        d1 = (norm_back(nrm2, rstd2, cv_ref[TWO:THREE, :], d_n2) + d2).astype(BF16)
        d1b[rows, :] = d1
        gbt2_ref[rows, :] += fold_lanes(d1.astype(F32))
        nrm1, _ = norm_stats(x_ref[rows, :].astype(F32))
        hs[rows, :] = (nrm1 * cv_ref[ZERO:ONE, :] + cv_ref[ONE:TWO, :]).astype(BF16)
        dhf[rows, :] = jnp.zeros((SUB, CH), F32)
        return carry

    lax.fori_loop(ZERO, GR // SUB, norm_two, ZERO)
    def one_image(i, carry):
        win = pl.ds(pl.multiple_of(192 * i, 192), WIN)
        for j in range(ZERO, TH, LANES):
            part = slice(j, j + LANES)
            d_act = mm(wt2_ref[i, part, :], d1b[win, :]).astype(BF16).astype(F32)
            act, d_u = gelu_and_grad(ut_ref[i, part, :], d_act)
            gbt1_ref[part, :] += fold_lanes(d_u)
            acts[part, :] = act.astype(BF16)
            dus[part, :] = d_u.astype(BF16)
        gt2_ref[i] += mm_t(d1b[win, :], acts[...])
        gt1_ref[i] += mm_t(hs[win, :], dus[...])
        dhf[win, :] += mm(wt1_ref[i], dus[...])
        return carry

    lax.fori_loop(ZERO, GROUP, one_image, ZERO)

    def norm_one(i, carry):
        rows = pl.ds(pl.multiple_of(i * SUB, SUB), SUB)
        d_n1 = dhf[rows, :].astype(BF16).astype(F32)
        nrm1, rstd1 = norm_stats(x_ref[rows, :].astype(F32))
        for k, part in ((ZERO, d_n1 * nrm1), (ONE, d_n1)):
            gcv_ref[k] += fold_rows(part)
        if not first:
            dx_ref[rows, :] = (norm_back(nrm1, rstd1, cv_ref[ZERO:ONE, :], d_n1) + d1b[rows, :].astype(F32)).astype(BF16)
        return carry

    lax.fori_loop(ZERO, GR // SUB, norm_one, ZERO)

    @pl.when(step == ROWS // GR - ONE)
    def _():
        for g, at in ((gt1_ref, ZERO), (gt2_ref, TH)):
            tok_ref[ZERO:TOK, at:at + TH] = sum(g[i, FOUR * i:FOUR * i + TOK, :] for i in range(ONE, GROUP)) + g[ZERO, ZERO:TOK, :]
        tok_ref[TOK:TROWS, :] = jnp.zeros((TROWS - TOK, CH), F32)
        vec_ref[...] = jnp.zeros(vec_ref.shape, F32)
        for i in range(FIVE):
            vec_ref[i:i + ONE, :] = jnp.sum(gcv_ref[i], axis=ZERO, keepdims=True)
        for q in range(QUART):
            vec_ref[FIVE + q:SIX + q, :] = jnp.sum(gb1_ref[:, CH * q:CH * q + CH], axis=ZERO, keepdims=True)
        vec_ref[9:10, ZERO:TH] = jnp.sum(gbt1_ref[...].T, axis=ZERO, keepdims=True)
        per_tok = sum(gbt2_ref[TOK * i:TOK * i + TOK, :] for i in range(ONE, GROUP)) + gbt2_ref[ZERO:TOK, :]
        vec_ref[10:11, ZERO:TOK] = jnp.sum(per_tok.T, axis=ZERO, keepdims=True)
        job.first_done()
        job.finish()


def backward_layer(dh, d2, x1, x, ut, w1, wt1s, wt2s, cv, gb1, dw1, dw2, extra):
    sds = jax.ShapeDtypeStruct
    first = len(extra) == TWO
    act = by_group((GR, CH))
    keep = lambda shape: pl.BlockSpec(shape, lambda g: (ZERO,) * len(shape))
    n = BLK
    outs, shapes = [keep((TROWS, CH)), keep((VROWS, CH)), ANY], [sds((TROWS, CH), F32), sds((VROWS, CH), F32), sds((TWO, n, CH), F32)]
    if not first:
        outs, shapes = [act] + outs, [sds((ROWS, CH), BF16)] + shapes
    return pl.pallas_call(
        functools.partial(backward_kernel, first),
        grid=(ROWS // GR,),
        in_specs=[by_group((GR, HID)), act, act, act, by_group((GROUP, TH, CH)), once((CH, HID)), once((GROUP, WIN, TH)), once((GROUP, TH, WIN)), once((EIGHT, CH)), once((EIGHT, HID))] + [ANY] * (TWO + len(extra)),
        out_specs=outs,
        out_shape=shapes,
        scratch_shapes=[pltpu.VMEM((GROUP, WIN, TH), F32), pltpu.VMEM((GROUP, WIN, TH), F32), pltpu.VMEM((TH, LANES), F32), pltpu.VMEM((GR, LANES), F32), pltpu.VMEM((FIVE, EIGHT, CH), F32),
                        pltpu.VMEM((GR, CH), BF16), pltpu.VMEM((GR, CH), BF16), pltpu.VMEM((GR, CH), F32)] + [pltpu.VMEM((TH, CH), BF16)] * TWO + reduction_scratch(n),
        compiler_params=pltpu.CompilerParams(collective_id=ONE if first else TWO, has_side_effects=True, vmem_limit_bytes=67000000),
        name="backward_layer",
    )(dh, d2, x1, x, ut, w1, wt1s, wt2s, cv, gb1, dw1, dw2, *extra)

KP = 4864
NJ = TWO_TILES
NSUB = SIX
STEPS = HID // NJ


def channel_back_kernel(late, d2_ref, h2_ref, w2_ref, hid_ref, *rest):
    give, dh_ref, dw1_ref, dw2_ref, db1_ref, take, st, even, odd, dbs, dwst, own_sem, send, recv = rest
    j = pl.program_id(ZERO)
    sub, part = ROWS // NSUB, TWO * CH // NSUB
    me = lax.axis_index("fsdp")
    if late:
        others = [peer(me, rel) for rel in (TWO, FOUR)]
        hops = last_hops(give, take, send, recv, me)
    else:
        others = [lax.rem(me + i, NDEV) for i in range(ONE, NDEV)]
        mine = lambda d: give.at[pl.ds(pl.multiple_of(HROWS * d, HROWS), HROWS)]
        hops = [pltpu.make_async_remote_copy(src_ref=mine(d), dst_ref=take.at[me], send_sem=send.at[i], recv_sem=recv.at[i], device_id=(d,), device_id_type=MESH) for i, d in enumerate(others)]
        own = pltpu.make_async_copy(mine(me), take.at[me], own_sem)

    @pl.when(j == ZERO)
    def _():
        barrier = pltpu.get_barrier_semaphore()
        for dev in others:
            pl.semaphore_signal(barrier, inc=ONE, device_id=(dev,), device_id_type=MESH)
        pl.semaphore_wait(barrier, len(others))
        for copy in hops:
            copy.start()
        if not late:
            own.start()

    @pl.when(j == ZERO)
    def _():
        st[ZERO:CH, ZERO:ROWS] = h2_ref[...].T
        st[CH:TWO * CH, ZERO:ROWS] = d2_ref[...].T
        st[:, ROWS:KP] = jnp.zeros((TWO * CH, KP - ROWS), BF16)
        for rhs in (even, odd):
            rhs[:, ROWS:KP, :] = jnp.zeros((TWO, KP - ROWS, NJ), BF16)

    def through_w2(r):
        rows = pl.ds(pl.multiple_of(r * sub, sub), sub)
        return mm_t(d2_ref[rows, :], w2_ref[...])

    def through_gelu(r, d_act, sums, rhs):
        rows = pl.ds(pl.multiple_of(r * sub, sub), sub)
        act, dh = gelu_and_grad(hid_ref[rows, :], d_act.astype(BF16).astype(F32))
        rhs[ONE, rows, :] = act.astype(BF16)
        dhb = dh.astype(BF16)
        rhs[ZERO, rows, :] = dhb
        dh_ref[rows, :] = dhb
        return sums + fold_rows(dh)

    def weight_part(r, rhs):
        rows = pl.ds(pl.multiple_of(r * part, part), part)
        dwst[rows, :] = mm(st[rows, :], rhs[(r * part) // CH])

    def emit():
        db1_ref[...] = dbs[...]
        dw1_ref[...] = dwst[ZERO:CH, :]
        dw2_ref[...] = dwst[CH:TWO * CH, :].T

    zero = jnp.zeros((EIGHT, NJ), F32)

    @pl.when(j == ZERO)
    def _():
        dbs[...] = lax.fori_loop(ZERO, NSUB, lambda r, sums: through_gelu(r, through_w2(r), sums, even), zero)

    for parity, (new, old) in enumerate(((even, odd), (odd, even))):
        @pl.when((j > ZERO) & (j < STEPS) & (lax.rem(j, TWO) == parity))
        def _():
            def both(r, sums):
                d_act = through_w2(r)
                weight_part(r, old)
                return through_gelu(r, d_act, sums, new)

            sums = lax.fori_loop(ZERO, NSUB, both, zero)
            emit()
            dbs[...] = sums

    @pl.when(j == STEPS)
    def _():
        def only(r, carry):
            weight_part(r, odd)
            return carry

        lax.fori_loop(ZERO, NSUB, only, ZERO)
        emit()
        for copy in hops:
            copy.wait()
        if not late:
            own.wait()


def channel_back(d2, h2, w2, hid, give, late):
    sds = jax.ShapeDtypeStruct
    cur = lambda j: jnp.minimum(j, STEPS - ONE)
    prev = lambda j: jnp.maximum(j - ONE, ZERO)
    wide = CH // NJ
    outs = [pl.BlockSpec((ROWS, NJ), lambda j: (ZERO, cur(j))), pl.BlockSpec((None, CH, NJ), lambda j: (prev(j) // wide, ZERO, lax.rem(prev(j), wide))),
            pl.BlockSpec((NJ, CH), lambda j: (prev(j), ZERO)), pl.BlockSpec((EIGHT, NJ), lambda j: (ZERO, prev(j)))]
    shapes = [sds((ROWS, HID), BF16), sds((QUART, CH, CH), F32), sds((HID, CH), F32), sds((EIGHT, HID), F32)]
    scratch = [pltpu.VMEM((TWO * CH, KP), BF16), pltpu.VMEM((TWO, KP, NJ), BF16), pltpu.VMEM((TWO, KP, NJ), BF16), pltpu.VMEM((EIGHT, NJ), F32), pltpu.VMEM((TWO * CH, NJ), F32)]
    outs.append(ANY)
    shapes.append(sds(give.shape[ONE:] if late else (NDEV, HROWS, NCP), F32))
    scratch += [pltpu.SemaphoreType.DMA] + [pltpu.SemaphoreType.DMA((NDEV,))] * TWO
    return pl.pallas_call(
        functools.partial(channel_back_kernel, late),
        grid=(STEPS + ONE,),
        in_specs=[once((ROWS, CH)), once((ROWS, CH)), pl.BlockSpec((NJ, CH), lambda j: (cur(j), ZERO)), pl.BlockSpec((ROWS, NJ), lambda j: (ZERO, cur(j)))] + [ANY],
        out_specs=outs,
        out_shape=shapes,
        scratch_shapes=scratch,
        compiler_params=pltpu.CompilerParams(collective_id=FIVE + late, has_side_effects=True, vmem_limit_bytes=67000000),
        name="channel_back",
    )(d2, h2, w2, hid, give)

IMG_PAD = 32


def head_kernel(x_ref, lab_ref, hw_ref, fv_ref, hb_ref, d2_ref, ghw_ref, ex_ref, pool, gfv_ref, dl):
    ngroup = ROWS // GR

    def image_of_row(shape, dim, g):
        row = lax.broadcasted_iota(jnp.int32, shape, dim)
        return GROUP * g + sum((row >= TOK * i).astype(jnp.int32) for i in range(ONE, GROUP))

    def normed(g):
        nrm, rstd = norm_stats(x_ref[pl.ds(pl.multiple_of(g * GR, GR), GR), :].astype(F32))
        return nrm, rstd

    pool[...] = jnp.zeros(pool.shape, F32)

    def pool_one(g, carry):
        nrm, _ = normed(g)
        pick = image_of_row((IMG_PAD, GR), ONE, g) == lax.broadcasted_iota(jnp.int32, (IMG_PAD, GR), ZERO)
        pool[...] += mm(pick.astype(F32).astype(BF16), (nrm * fv_ref[ZERO:ONE, :] + fv_ref[ONE:TWO, :]).astype(BF16))
        return carry

    lax.fori_loop(ZERO, ngroup, pool_one, ZERO)
    real = lax.broadcasted_iota(jnp.int32, (IMG_PAD, NCLS), ZERO) < 24
    pooled = (pool[...] / TOK).astype(BF16)
    logits = mm(pooled, hw_ref[...]) + hb_ref[ZERO:ONE, ZERO:NCLS]
    top = jnp.max(logits, axis=-ONE, keepdims=True)
    log_norm = top + jnp.log(jnp.sum(jnp.exp(logits - top), axis=-ONE, keepdims=True))
    is_label = lax.broadcasted_iota(jnp.int32, (IMG_PAD, NCLS), ONE) == lab_ref[:, ZERO:ONE]
    picked = jnp.sum(jnp.where(is_label, logits, 0.0), axis=-ONE, keepdims=True)
    per_image = jnp.where(lax.broadcasted_iota(jnp.int32, (IMG_PAD, ONE), ZERO) < 24, log_norm - picked, 0.0)
    d_logits = jnp.where(real, (jnp.exp(logits - log_norm) - is_label.astype(F32)) / (24 * NDEV), 0.0)
    d_log_b = d_logits.astype(BF16)
    dl[...] = jnp.zeros(dl.shape, F32)
    dl[:, ZERO:NCLS] = d_logits
    ghw_ref[...] = lax.dot_general(pooled, dl[...].astype(BF16), (((ZERO,), (ZERO,)), ((), ())), preferred_element_type=F32)
    d_pool = mm_t(d_log_b, hw_ref[...])
    pool[...] = d_pool / TOK
    gfv_ref[...] = jnp.zeros(gfv_ref.shape, F32)

    def back_one(g, carry):
        nrm, rstd = normed(g)
        pick = image_of_row((GR, IMG_PAD), ZERO, g) == lax.broadcasted_iota(jnp.int32, (GR, IMG_PAD), ONE)
        d_n = mm(pick.astype(F32).astype(BF16), pool[...].astype(BF16))
        gfv_ref[ZERO] += fold_rows(d_n * nrm)
        gfv_ref[ONE] += fold_rows(d_n)
        d2_ref[pl.ds(pl.multiple_of(g * GR, GR), GR), :] = norm_back(nrm, rstd, fv_ref[ZERO:ONE, :], d_n).astype(BF16)
        return carry

    lax.fori_loop(ZERO, ngroup, back_one, ZERO)
    nrow = CH // LANES
    parts = [jnp.sum(gfv_ref[i], axis=ZERO, keepdims=True) for i in range(TWO)] + [jnp.sum(dl[...], axis=ZERO, keepdims=True)]
    ex_ref[...] = jnp.zeros(ex_ref.shape, F32)
    for i, part in enumerate(parts):
        for c in range(part.shape[ONE] // LANES):
            ex_ref[nrow * i + c:nrow * i + c + ONE, :] = part[:, LANES * c:LANES * c + LANES]
    ex_ref[LOSS_ROW:EXR, :] = jnp.broadcast_to(jnp.sum(per_image, axis=ZERO, keepdims=True), (EXR - LOSS_ROW, LANES))


def head_layer(x2, labels, head_full, fv, head_b):
    sds = jax.ShapeDtypeStruct
    lab = jnp.broadcast_to(jnp.pad(labels, (ZERO, IMG_PAD - 24))[:, None], (IMG_PAD, LANES))
    return pl.pallas_call(
        head_kernel,
        in_specs=[VMEM] * FIVE,
        out_specs=[VMEM] * THREE,
        out_shape=[sds((ROWS, CH), BF16), sds((CH, NCP), F32), sds((EXR, LANES), F32)],
        scratch_shapes=[pltpu.VMEM((IMG_PAD, CH), F32), pltpu.VMEM((TWO, EIGHT, CH), F32), pltpu.VMEM((IMG_PAD, NCP), F32)],
        compiler_params=pltpu.CompilerParams(vmem_limit_bytes=60000000),
        name="head_loss",
    )(x2, lab, head_full, fv, head_b)


def view(a):
    return a.reshape(TWO, SH, LANES).transpose(ONE, ZERO, TWO)


def unview(a):
    return a.transpose(ONE, ZERO, TWO).reshape(TWO, SH * LANES)


def solution(mesh):
    row_spec = P('fsdp')
    layer_spec = P(None, 'fsdp')
    in_specs = (row_spec, row_spec) + (layer_spec, row_spec, row_spec) * THREE
    out_specs = (P(),) + in_specs[TWO:]

    def device_step(act_in, labels, layer_p, head_w, small_p, layer_m, head_m, small_m, layer_v, head_v, small_v):
        small8 = jnp.pad(small_p.reshape(THREE, LANES), ((ZERO, FIVE), (ZERO, ZERO)))
        (w1, w2, st1, st2, head_full), *vectors, (fv, hb) = gather_all(view(layer_p), head_w, small8)
        x, stage, saved = act_in, (st1, st2), []
        for wt1s, wt2s, wt1t, wt2t, bt1, bt2, cv, b1 in vectors:
            x1, ut, hid, h2, x2, *more = forward_layer(x, wt1t, wt2t, bt1, bt2, w1, w2, cv, b1, stage)
            saved.append((more[ZERO] if more else x, x1, ut, hid, h2, w1, w2, wt1s, wt2s, cv))
            if more:
                w1, w2 = more[ONE:THREE]
            x, stage = x2, ()
        d2, g_head, ex = head_layer(x, labels, head_full, fv, hb)
        give, extra, arrived, reds = g_head, (), [], []
        for x, x1, ut, hid, h2, w1, w2, wt1s, wt2s, cv in reversed(saved):
            dh, dw1, dw2, gb1, got = channel_back(d2, h2, w2, hid, give, len(arrived) > ZERO)
            *d_in, g_tok, g_vec, give = backward_layer(dh, d2, x1, x, ut, w1, wt1s, wt2s, cv, gb1, dw1, dw2, extra)
            arrived.append(got)
            reds.append(give)
            extra = g_tok, g_vec
            d2 = d_in[ZERO] if d_in else None
        heads, late = arrived
        g, g_head, g_small, scalars = finish(reds[ONE], reds[ZERO], late, heads, g_tok, g_vec, ex)
        smalls = [a.reshape(THREE, LANES) for a in (small_p, small_m, small_v)]
        outs = update(view(layer_p), view(layer_m), view(layer_v), g, g_head, g_small, scalars, (head_w, head_m, head_v), smalls)
        new_lp, new_lm, new_lv = [unview(a) for a in outs[:THREE]]
        new_hw, new_hm, new_hv = outs[THREE:SIX]
        new_sp, new_sm, new_sv = [a.reshape(-ONE) for a in outs[SIX:]]
        return (scalars[ZERO, ZERO] / (act_in.shape[ZERO] * NDEV), new_lp, new_hw, new_sp, new_lm, new_hm, new_sm, new_lv, new_hv, new_sv)

    return jax.shard_map(device_step, mesh=mesh, in_specs=in_specs, out_specs=out_specs, check_vma=False)
```

```python
import functools
import math

import jax
import jax.numpy as jnp
from jax import lax
from jax.experimental import pallas as pl
from jax.experimental.pallas import tpu as pltpu
from jax.sharding import PartitionSpec as P

F32, BF16 = jnp.float32, jnp.bfloat16
ZERO = 0
ONE = 1
TWO = 2
THREE = 3
FOUR = 4
FIVE = 5
SIX = 6
EIGHT = 8
SIXTEEN = 16
LANES = 128
TWO_TILES = 256
SEVEN = 7
LN_EPS = 1e-6
LEARN_RATE = 0.003
BETA_ONE = 0.9
BETA_TWO = 0.999
ADAM_EPS = 1e-8
WEIGHT_DECAY = 0.03
ADAM_STEP = 10

NDEV = EIGHT
TOK, CH, TH, HID, NCLS = 196, 768, 384, 3072, 1000
SH = 4763
T1 = TWO * TOK * TH // LANES
RW = CH * HID // LANES
C1, C2 = HID // LANES, CH // LANES
VEC0 = T1 + TWO * RW - SEVEN * SH
MARG = 384
GROUP = FOUR
GR = GROUP * TOK
ROWS = 24 * TOK
WIN = 208
MESH = pl.DeviceIdType.MESH
ANY = pl.BlockSpec(memory_space=pl.ANY)
VMEM = pl.BlockSpec(memory_space=pltpu.VMEM)


def c1_span(d):
    return max(ZERO, SH * d - T1), min(RW, SH * (d + ONE) - T1)


def c2_span(d):
    return max(ZERO, SH * d - T1 - RW), min(RW, SH * (d + ONE) - T1 - RW)


def tiles_of(span, per):
    lo, hi = span
    if lo >= hi:
        return ZERO, ZERO
    return lo // per, -(-hi // per)


def edges(span_of, per):
    out = []
    for d in range(NDEV):
        lo, hi = span_of(d)
        if lo < hi and lo > ZERO and lo % per:
            out.append((d, lo // per, lo % per))
    return out


EDGE1 = edges(c1_span, SIXTEEN * C1)
EDGE2 = edges(c2_span, SIXTEEN * C2)


def matrix_moves(d, s1, s2, w1, w2, e1, e2):
    out = []
    for span_of, per, s, w, e, eds in ((c1_span, SIXTEEN * C1, s1, w1, e1, EDGE1), (c2_span, SIXTEEN * C2, s2, w2, e2, EDGE2)):
        lo, hi = tiles_of(span_of(d), per)
        if lo == hi:
            continue
        first = lo
        for k, (owner, row, _) in enumerate(eds):
            if owner == d:
                out.append((s.at[pl.ds(ZERO, SIXTEEN)], e.at[k]))
                first = lo + ONE
        n = hi - first
        out.append((s.at[pl.ds(SIXTEEN * (first - lo), SIXTEEN * n)], w.at[pl.ds(SIXTEEN * first, SIXTEEN * n)]))
    return out


def entry_barrier(me):
    barrier = pltpu.get_barrier_semaphore()
    for rel in (ONE, TWO, FOUR, SIX):
        pl.semaphore_signal(barrier, inc=ONE, device_id=(peer(me, rel),), device_id_type=MESH)
    pl.semaphore_wait(barrier, FOUR)


def peer(me, rel):
    t = me
    if rel & ONE:
        t = t + ONE - TWO * lax.rem(me, TWO)
    if rel & TWO:
        t = t + TWO - FOUR * lax.rem(me // TWO, TWO)
    if rel & FOUR:
        t = t + FOUR - EIGHT * (me // FOUR)
    return t


RELS = (TWO, FOUR, SIX)


class Spread:
    def __init__(self, pieces, send_sem, recv_sem, fwd_sem, far_sem):
        self.pieces, self.send_sem, self.recv_sem, self.fwd_sem, self.far_sem = pieces, send_sem, recv_sem, fwd_sem, far_sem
        self.me = lax.axis_index("fsdp")

    def copies(self, d, k, rel):
        return [pltpu.make_async_remote_copy(src_ref=a, dst_ref=b, send_sem=self.send_sem.at[k, i], recv_sem=self.recv_sem.at[d, i], device_id=(d ^ rel,), device_id_type=MESH)
                for i, (a, b) in enumerate(self.pieces(d))]

    def handed(self, s, to):
        return [pltpu.make_async_remote_copy(src_ref=b, dst_ref=b, send_sem=self.fwd_sem.at[s, i], recv_sem=self.recv_sem.at[s, i], device_id=(to,), device_id_type=MESH)
                for i, (_, b) in enumerate(self.pieces(s))]

    def each(self, rels, body):
        for rel in rels:
            for s in range(NDEV):
                if self.pieces(s):
                    pl.when(self.me == s ^ rel)(functools.partial(body, s, rel))

    def start(self):
        def body(d, _):
            for k, rel in enumerate(ORDER):
                for copy in self.copies(d, k, rel):
                    copy.start()
        self.each((ZERO,), body)

    def across(self, s, rel):
        if rel != (FOUR if s % TWO else TWO):
            return []
        return [pltpu.make_async_remote_copy(src_ref=b, dst_ref=b, send_sem=self.far_sem.at[i], recv_sem=self.recv_sem.at[s, i], device_id=(s ^ SIX,), device_id_type=MESH)
                for i, (_, b) in enumerate(self.pieces(s))]

    def hand_on(self, rels):
        def body(s, rel):
            for copy in self.handed(s, s ^ rel ^ ONE):
                copy.wait_recv()
            for copy in self.across(s, rel) + self.handed(s, s ^ rel ^ ONE):
                copy.start()
        self.each(rels, body)

    def arrive(self):
        def body(s, rel):
            for copy in self.handed(s, s):
                copy.wait_recv()
        self.each((ONE, THREE, FIVE, SEVEN), body)

    def sent(self):
        def own(d, _):
            for k, rel in enumerate(ORDER):
                for copy in self.copies(d, k, rel):
                    copy.wait_send()
        self.each((ZERO,), own)

        def other(s, rel):
            for copy in self.across(s, rel) + self.handed(s, s ^ rel ^ ONE):
                copy.wait_send()
        self.each(RELS, other)


ORDER = (FOUR, TWO, ONE)


def merge_edges(w1, w2, e1, e2, m1, m2, sem):
    jobs = [(k, per, w.at[pl.ds(SIXTEEN * row, SIXTEEN)], e.at[k], m, below)
            for per, w, e, m, eds in ((C1, w1, e1, m1, EDGE1), (C2, w2, e2, m2, EDGE2)) for k, (_, row, below) in enumerate(eds)]
    loads = [pltpu.make_async_copy(src, m.at[i, k], sem.at[i, n]) for n, (k, _, w, e, m, _) in enumerate(jobs) for i, src in enumerate((w, e))]
    stores = [pltpu.make_async_copy(m.at[ZERO, k], w, sem.at[ZERO, n]) for n, (k, _, w, e, m, _) in enumerate(jobs)]
    for copy in loads:
        copy.start()
    for copy in loads:
        copy.wait()
    for k, per, _, _, m, below in jobs:
        shape = (SIXTEEN, LANES * per)
        pos = lax.broadcasted_iota(jnp.int32, shape, ZERO) * per + lax.broadcasted_iota(jnp.int32, shape, ONE) // LANES
        m[ZERO, k] = jnp.where(pos < below, m[ZERO, k].astype(F32), m[ONE, k].astype(F32)).astype(BF16)
    for copy in stores:
        copy.start()
    for copy in stores:
        copy.wait()


def edge_scratch():
    return [pltpu.VMEM((TWO, len(EDGE1), SIXTEEN, HID), BF16), pltpu.VMEM((TWO, len(EDGE2), SIXTEEN, CH), BF16), pltpu.SemaphoreType.DMA((TWO, len(EDGE1) + len(EDGE2)))]


def spread_sems(n):
    dma = pltpu.SemaphoreType.DMA
    return [dma((len(ORDER), n)), dma((NDEV, n)), dma((NDEV, n)), dma((n,))]


def lay_token_weights(tok, flat, nat, wt1s, wt2s, wt1t, wt2t):
    flat[ZERO:T1, :] = tok[...].astype(F32)
    period = LANES * TOK // math.gcd(LANES, TOK)
    nrow, npos = period // LANES, period // TOK
    reps = TH // npos
    lane = lax.broadcasted_iota(jnp.int32, (reps, LANES), ONE)
    for j in range(npos):
        f, o = divmod(TOK * j, LANES)
        rows = [flat[pl.ds(T1 // TWO + f + i, reps, stride=nrow), :] for i in range(THREE)]
        for i in range(TWO):
            part = jnp.where(lane >= o, rows[i], rows[i + ONE])
            nat[i, pl.ds(j, reps, stride=npos), :] = pltpu.roll(part, (LANES - o) % LANES, axis=ONE) if o else part
    two_t = jnp.concatenate([nat[ZERO].T, nat[ONE].T], axis=ZERO)
    for i in range(GROUP):
        for s, t, ref_n in ((wt2t, wt2s, two_t), (wt1s, wt1t, None)):
            flat[T1:T1 + WIN, :] = jnp.zeros((WIN, LANES), F32)
            for c in range(TH // LANES):
                lanes_ = slice(LANES * c, LANES * c + LANES)
                part = flat[pl.ds(c, TOK, stride=TH // LANES), :] if ref_n is None else ref_n[ZERO:TOK, lanes_]
                flat[T1 + FOUR * i:T1 + FOUR * i + TOK, :] = part
                full = flat[T1:T1 + WIN, :]
                s[i, :, lanes_] = full.astype(BF16)
                t[i, lanes_, :] = full.T.astype(BF16)


def lay_bias_vectors(vec, vf, bt1, bt2, cv, b1):
    vf[...] = vec[...].astype(F32)

    def put(ref, row, first, n, src):
        for c in range(n // LANES):
            ref[row:row + ONE, LANES * c:LANES * c + LANES] = src[first + c:first + c + ONE, :]

    ng, nt = CH // LANES, TH // LANES
    put(cv, ZERO, ZERO, CH, vf)
    put(cv, ONE, ng, CH, vf)
    for c in range(nt):
        bt1[LANES * c:LANES * c + LANES, :] = jnp.broadcast_to(vf[TWO * ng + c:TWO * ng + c + ONE, :], (LANES, LANES)).T
    at = TWO * ng + nt
    cols = [jnp.broadcast_to(vf[at + i:at + i + ONE, :], (LANES, LANES)).T for i in range(TWO)]
    cut = TOK - LANES
    for i in range(GROUP):
        bt2[i] = jnp.zeros((WIN, LANES), F32)
        bt2[i, FOUR * i:FOUR * i + LANES, :] = cols[ZERO]
        bt2[i, FOUR * i + LANES:FOUR * i + TOK, :] = cols[ONE][ZERO:cut, :]
    n = vf.shape[ZERO] - at - TWO
    lane = lax.broadcasted_iota(jnp.int32, (n, LANES), ONE)
    rest = pltpu.roll(jnp.where(lane >= cut, vf[at + ONE:at + ONE + n, :], vf[at + TWO:at + TWO + n, :]), LANES - cut, axis=ONE)
    vf[ZERO:n, :] = rest
    put(cv, TWO, ZERO, CH, vf)
    put(cv, THREE, ng, CH, vf)
    put(b1, ZERO, TWO * ng, HID, vf)
    put(cv, FOUR, TWO * ng + HID // LANES, CH, vf)


def gather_kernel(p_ref, head_ref, small_ref, w1, w2, nw1, nw2, headf, *rest):
    (tw0, tw1, (fv, hb)), rest = (rest[ZERO:EIGHT], rest[EIGHT:SIXTEEN], rest[SIXTEEN:18]), rest[18:]
    (e1, e2, ne1, ne2, xs, s1, s2, stok, svec, shead, ssmall, tok, vec, smallf, flat, nat, vf, m1, m2, ed_sem, ld_sem, stage_sem, own_sem), rest = rest[:23], rest[23:]
    me = lax.axis_index("fsdp")
    loads = [pltpu.make_async_copy(p_ref.at[:, l, :], xs.at[l, pl.ds(MARG, SH)], ld_sem.at[l]) for l in range(TWO)]
    for copy in loads:
        copy.start()
    shead[...] = head_ref[...].astype(BF16)
    ssmall[...] = small_ref[...].astype(BF16).astype(F32)

    def early(d):
        out = [(ssmall, smallf.at[d])]
        if d == ZERO:
            out += [(stok.at[l], tok.at[l]) for l in range(TWO)]
        if d == NDEV - ONE:
            out += [(svec.at[l], vec.at[l]) for l in range(TWO)]
        return out

    def matrices(d):
        return matrix_moves(d, s1.at[ZERO], s2.at[ZERO], w1, w2, e1, e2)

    def classes(d):
        return [(shead, headf.at[pl.ds(HROWS * d, HROWS)])]

    jobs = [Spread(f, *rest[FOUR * i:FOUR * i + FOUR]) for i, f in enumerate((early, matrices, classes))]

    def keep_own(d, _):
        return [pltpu.make_async_copy(a, b, own_sem.at[i]) for i, (a, b) in enumerate(matrices(d) + classes(d))]

    for copy in loads:
        copy.wait()

    @pl.when(me == ZERO)
    def _():
        stok[...] = xs[:, MARG:MARG + T1, :].astype(BF16)
        tok[...] = stok[...]

    @pl.when(me == NDEV - ONE)
    def _():
        svec[...] = xs[:, MARG + VEC0:MARG + SH, :].astype(BF16)
        vec[...] = svec[...]

    entry_barrier(me)
    jobs[ZERO].start()

    def tile(l):
        def body(d, _):
            for span_of, per, s, skip in ((c1_span, C1, s1, T1 if d == ZERO else ZERO), (c2_span, C2, s2, max(ZERO, c1_span(d)[ONE] - c1_span(d)[ZERO]))):
                lo, hi = tiles_of(span_of(d), SIXTEEN * per)
                base0 = SIXTEEN * per * lo - span_of(d)[ZERO] + MARG + skip

                def one(i, carry, per=per, s=s, base0=base0):
                    row = pl.multiple_of(i * SIXTEEN, SIXTEEN)
                    for c in range(per):
                        s[l, pl.ds(row, SIXTEEN), LANES * c:LANES * c + LANES] = xs[l, pl.ds(base0 + c + i * (SIXTEEN * per), SIXTEEN, stride=per), :].astype(BF16)
                    return carry

                if lo < hi:
                    lax.fori_loop(ZERO, hi - lo, one, ZERO)
        jobs[ZERO].each((ZERO,), body)

    tile(ZERO)
    jobs[ONE].start()
    jobs[TWO].start()
    for d in range(NDEV):
        @pl.when(me == d)
        def _():
            smallf[d] = ssmall[...]
            for copy in keep_own(d, ZERO):
                copy.start()
    tile(ONE)

    def keep_next(d):
        return [pltpu.make_async_copy(a, b, stage_sem.at[i]) for i, (a, b) in enumerate(matrix_moves(d, s1.at[ONE], s2.at[ONE], nw1, nw2, ne1, ne2))]

    for d in range(NDEV):
        @pl.when(me == d)
        def _():
            for copy in keep_next(d):
                copy.start()
    jobs[ZERO].hand_on(ORDER[:TWO])
    jobs[ZERO].hand_on(RELS[TWO:])
    jobs[ZERO].arrive()
    for l, (wt1s, wt2s, wt1t, wt2t, bt1, bt2, cv, b1) in enumerate((tw0, tw1)):
        lay_token_weights(tok.at[l], flat, nat, wt1s, wt2s, wt1t, wt2t)
        lay_bias_vectors(vec.at[l], vf, bt1, bt2, cv, b1)
    for d in range(NDEV):
        flat[THREE * d:THREE * d + THREE, :] = smallf[d, ZERO:THREE, :]
    for i in range(TWO):
        for c in range(CH // LANES):
            fv[i:i + ONE, LANES * c:LANES * c + LANES] = flat[C2 * i + c:C2 * i + c + ONE, :]
    for c in range(NCP // LANES):
        hb[ZERO:ONE, LANES * c:LANES * c + LANES] = flat[TWO * C2 + c:TWO * C2 + c + ONE, :]
    for rels in (ORDER[:TWO], RELS[TWO:]):
        jobs[ONE].hand_on(rels)
        jobs[TWO].hand_on(rels)
    jobs[ONE].arrive()
    jobs[TWO].arrive()
    for job in jobs:
        job.sent()
    for d in range(NDEV):
        @pl.when(me == d)
        def _():
            for copy in keep_own(d, ZERO) + keep_next(d):
                copy.wait()
    merge_edges(w1, w2, e1, e2, m1, m2, ed_sem)


STAGE1 = max(SIXTEEN * (b - a) for a, b in (tiles_of(c1_span(d), SIXTEEN * C1) for d in range(NDEV)))
STAGE2 = max(SIXTEEN * (b - a) for a, b in (tiles_of(c2_span(d), SIXTEEN * C2) for d in range(NDEV)))


def gather_all(p_view, head_w, small8):
    sds = jax.ShapeDtypeStruct
    per_layer = [sds((GROUP, WIN, TH), BF16), sds((GROUP, TH, WIN), BF16), sds((GROUP, TH, WIN), BF16), sds((GROUP, WIN, TH), BF16),
                 sds((TH, LANES), F32), sds((GROUP, WIN, LANES), F32), sds((EIGHT, CH), F32), sds((EIGHT, HID), F32)]
    far = [sds((CH, HID), BF16), sds((HID, CH), BF16)] * TWO + [sds((CH, NCLS), BF16)]
    near = per_layer * TWO + [sds((EIGHT, CH), F32), sds((EIGHT, NCP), F32)]
    edge = [sds((len(EDGE1), SIXTEEN, HID), BF16), sds((len(EDGE2), SIXTEEN, CH), BF16)] * TWO
    dma = pltpu.SemaphoreType.DMA
    nv = SH - VEC0
    outs = pl.pallas_call(
        gather_kernel,
        in_specs=[ANY, VMEM, VMEM],
        out_specs=[ANY] * len(far) + [VMEM] * len(near) + [ANY] * len(edge),
        out_shape=far + near + edge,
        scratch_shapes=[pltpu.VMEM((TWO, SH + TWO * MARG + FIVE, LANES), F32), pltpu.VMEM((TWO, STAGE1, HID), BF16), pltpu.VMEM((TWO, STAGE2, CH), BF16),
                        pltpu.VMEM((TWO, T1, LANES), BF16), pltpu.VMEM((TWO, nv, LANES), BF16), pltpu.VMEM((HROWS, NCLS), BF16), pltpu.VMEM((EIGHT, LANES), F32),
                        pltpu.VMEM((TWO, T1, LANES), BF16), pltpu.VMEM((TWO, nv, LANES), BF16), pltpu.VMEM((NDEV, EIGHT, LANES), F32),
                        pltpu.VMEM((T1 + WIN + EIGHT, LANES), F32), pltpu.VMEM((TWO, TH, LANES), F32), pltpu.VMEM((nv, LANES), F32)] + edge_scratch()
        + [dma((TWO,)), dma((FOUR,)), dma((SIX,))] + spread_sems(THREE) + spread_sems(FOUR) + spread_sems(ONE),
        compiler_params=pltpu.CompilerParams(collective_id=ZERO, has_side_effects=True, vmem_limit_bytes=60000000),
        name="gather_weights",
    )(p_view, head_w, small8)
    n = len(far)
    return outs[:n], outs[-TWO:], outs[n:n + EIGHT], outs[n + EIGHT:n + SIXTEEN], outs[n + SIXTEEN:n + 18]


def g1_rows(d):
    lo, hi = tiles_of(c1_span(d), EIGHT * C1)
    return EIGHT * lo, EIGHT * hi


def g2_rows(d):
    lo, hi = tiles_of(c2_span(d), EIGHT * C2)
    return EIGHT * lo, EIGHT * hi


QUART = HID // CH
HALF = CH // TWO
BLK = max(QUART * (g1_rows(d)[ONE] - g1_rows(d)[ZERO]) + g2_rows(d)[ONE] - g2_rows(d)[ZERO] for d in range(NDEV))


def core_rows(s):
    lo, hi = g1_rows(s)
    return QUART * (hi - lo) + g2_rows(s)[ONE] - g2_rows(s)[ZERO]


def chunk_pieces(chunk, core, ds1, ds2, blocks):
    out = []
    for k in range(NDEV // TWO):
        s = TWO * k + core
        lo, hi = g1_rows(s)
        n1 = hi - lo
        q, third = divmod(chunk, CH // NJ)
        if n1:
            out.append((ds1.at[pl.ds(lo, n1)], blocks.at[k, pl.ds(q * n1, n1), pl.ds(NJ * third, NJ)]))
        lo, hi = g2_rows(s)
        first, last = max(lo, NJ * chunk), min(hi, NJ * chunk + NJ)
        if first < last:
            out.append((ds2.at[pl.ds(first - NJ * chunk, last - first)], blocks.at[k, pl.ds(QUART * n1 + first - lo, last - first)]))
    return list(enumerate(out))


def extra_pieces(core, tok, vec, blocks):
    if core == ZERO:
        return [(tok, blocks.at[ZERO, pl.ds(core_rows(ZERO), TROWS)])]
    return [(vec, blocks.at[NDEV // TWO - ONE, pl.ds(core_rows(NDEV - ONE), VROWS)])]


NJ = TWO_TILES
NCP = 1024
HROWS = CH // NDEV
TROWS, VROWS = 200, SIXTEEN


def add_into(dst, src, n):
    def one(i, carry):
        at = pl.ds(pl.multiple_of(i * ADD, ADD), ADD)
        dst[at, :] = dst[at, :] + src[at, :]
        return carry
    lax.fori_loop(ZERO, n // ADD, one, ZERO)


ADD = 32


class Reduction:
    def __init__(self, mine, theirs, red, sums, own, ld, hs, hr, out_sem, free):
        self.mine, self.theirs, self.red, self.sums, self.own, self.free = mine, theirs, red, sums, own, free
        self.n = red.shape[ONE]
        self.ld, self.hs, self.hr, self.out_sem = ld, hs, hr, out_sem
        self.me = lax.axis_index("fsdp")
        chip = self.me // TWO
        px, py = lax.rem(chip, TWO), chip // TWO
        self.k, self.kx, self.ky = chip, chip + ONE - TWO * px, chip + TWO - FOUR * py
        self.kd = self.kx + TWO - FOUR * py

    def load(self, k):
        return pltpu.make_async_copy(self.mine.at[k], self.own.at[k % TWO], self.ld.at[ZERO, k])

    def load_theirs(self, k):
        return pltpu.make_async_copy(self.theirs.at[k], self.sums.at[k], self.ld.at[ONE, k])

    def hop(self, i, src, dst, rel):
        return pltpu.make_async_remote_copy(src_ref=src, dst_ref=dst, send_sem=self.hs.at[i], recv_sem=self.hr.at[i], device_id=(peer(self.me, rel),), device_id_type=MESH)

    def left(self, ref, k):
        return ref.at[k, :, pl.ds(ZERO, HALF)]

    def right(self, ref, k):
        return ref.at[k, :, pl.ds(HALF, HALF)]

    def ready(self, i):
        for rel in (TWO, FOUR):
            pl.semaphore_signal(self.free.at[i], inc=ONE, device_id=(peer(self.me, rel),), device_id_type=MESH)
        pl.semaphore_wait(self.free.at[i], TWO)

    def first_hops(self):
        return [self.hop(ZERO, self.left(self.sums, self.kx), self.left(self.own, ZERO), TWO), self.hop(ONE, self.left(self.sums, self.kd), self.left(self.own, ONE), TWO),
                self.hop(TWO, self.right(self.sums, self.ky), self.right(self.own, ZERO), FOUR), self.hop(THREE, self.right(self.sums, self.kd), self.right(self.own, ONE), FOUR)]

    def begin(self):
        for k in range(NDEV // TWO):
            self.load_theirs(k).start()
        for k in range(TWO):
            self.load(k).start()
        barrier = pltpu.get_barrier_semaphore()
        for rel in (TWO, FOUR):
            pl.semaphore_signal(barrier, inc=ONE, device_id=(peer(self.me, rel),), device_id_type=MESH)
        pl.semaphore_wait(barrier, TWO)
    def combine(self):
        for k in range(NDEV // TWO):
            self.load(k).wait()
            self.load_theirs(k).wait()
            add_into(self.sums.at[k], self.own.at[k % TWO], self.n)
            if k < TWO:
                self.load(k + TWO).start()
        self.ready(ZERO)
        for copy in self.first_hops():
            copy.start()

    def take(self):
        add_into(self.sums.at[self.k], self.own.at[ZERO], self.n)
        add_into(self.left(self.sums, self.ky), self.left(self.own, ONE), self.n)
        add_into(self.right(self.sums, self.kx), self.right(self.own, ONE), self.n)

    def first_done(self):
        for copy in self.first_hops():
            copy.wait_recv()
        self.take()
        self.ready(ONE)
        for copy in self.second_hops():
            copy.start()

    def second_hops(self):
        return [self.hop(FOUR, self.left(self.sums, self.ky), self.left(self.own, ZERO), FOUR), self.hop(FIVE, self.right(self.sums, self.kx), self.right(self.own, ZERO), TWO)]

    def finish(self):
        for copy in self.second_hops():
            copy.wait_recv()
        add_into(self.sums.at[self.k], self.own.at[ZERO], self.n)
        out = pltpu.make_async_copy(self.sums.at[self.k], self.red.at[ZERO], self.out_sem.at[ZERO])
        out.start()
        for copy in self.first_hops() + self.second_hops():
            copy.wait_send()
        out.wait()

    def hand_over(self):
        own, left, right = self.red.at[ZERO], self.red.at[ONE, :, pl.ds(ZERO, HALF)], self.red.at[ONE, :, pl.ds(HALF, HALF)]
        outs = [pltpu.make_async_copy(a, b, self.out_sem.at[i]) for i, (a, b) in enumerate(((self.sums.at[self.k], own), (self.left(self.sums, self.ky), left), (self.right(self.sums, self.kx), right)))]
        for copy in self.first_hops():
            copy.wait_recv()
        self.take()
        for copy in outs:
            copy.start()
        for copy in self.first_hops():
            copy.wait_send()
        for copy in outs:
            copy.wait()


def last_hops(red, late, send, recv, me):
    out = []
    for i, rel in enumerate((FOUR, TWO)):
        part = pl.ds(HALF * i, HALF)
        out.append(pltpu.make_async_remote_copy(src_ref=red.at[ONE, :, part], dst_ref=late.at[:, part], send_sem=send.at[i], recv_sem=recv.at[i], device_id=(peer(me, rel),), device_id_type=MESH))
    return out


def reduction_scratch(n):
    dma = pltpu.SemaphoreType.DMA
    return [pltpu.VMEM((FOUR, n, CH), F32), pltpu.VMEM((TWO, n, CH), F32), dma((TWO, FOUR)), dma((SIX,)), dma((SIX,)), dma((THREE,)), pltpu.SemaphoreType.REGULAR((TWO,))]


def untile(block, flat, d):
    lo, hi = g1_rows(d)
    n1 = hi - lo
    jobs = [(q * n1, n1, C1, C1 * lo - c1_span(d)[ZERO] + (T1 if d == ZERO else ZERO) + C2 * q) for q in range(QUART) if n1]
    lo, hi = g2_rows(d)
    if lo < hi:
        jobs.append((QUART * n1, hi - lo, C2, C2 * lo - c2_span(d)[ZERO] + max(ZERO, c1_span(d)[ONE] - c1_span(d)[ZERO])))
    for at, n, stride, base in jobs:
        def one(i, carry, at=at, stride=stride, base=base):
            rows = pl.ds(pl.multiple_of(at + EIGHT * i, EIGHT), EIGHT)
            for c in range(C2):
                flat[pl.ds(MARG + base + c + i * (EIGHT * stride), EIGHT, stride=stride), :] = block[rows, LANES * c:LANES * c + LANES]
            return carry
        lax.fori_loop(ZERO, n // EIGHT, one, ZERO)


def adam_math(p, g, m, v, decay):
    m_new = BETA_ONE * m + (1.0 - BETA_ONE) * g
    v_new = BETA_TWO * v + (1.0 - BETA_TWO) * g * g
    m_hat = m_new / (1.0 - BETA_ONE ** ADAM_STEP)
    v_hat = v_new / (1.0 - BETA_TWO ** ADAM_STEP)
    p_new = p - LEARN_RATE * (m_hat / (jnp.sqrt(v_hat) + ADAM_EPS) + decay * p)
    return p_new, m_new, v_new


NVIEW = 40
CHUNK = 1200
NCHUNK = FOUR
GROWS = CHUNK * NCHUNK
EXR = 32
LOSS_ROW = 24


def chunk_rows(k):
    return k * CHUNK, min(SH, (k + ONE) * CHUNK) - k * CHUNK


def lay_tokens(blk, r0, flat, flip, ta, tb):
    for c in range(TH // LANES):
        flat[pl.ds(MARG + c, TOK, stride=TH // LANES), :] = blk[r0:r0 + TOK, LANES * c:LANES * c + LANES]
    flip[:, ZERO:TROWS] = blk[r0:r0 + TROWS, TH:TWO * TH].T
    ta[ZERO:TH, :] = flip[:, ZERO:LANES]
    tb[ZERO:TH, :] = flip[:, LANES:TWO_TILES]
    period = LANES * TOK // math.gcd(LANES, TOK)
    nrow, npos = period // LANES, period // TOK
    reps = TH // npos
    lane = lax.broadcasted_iota(jnp.int32, (reps, LANES), ONE)
    for m in range(nrow):
        j, o = divmod(LANES * m, TOK)
        first = ta[pl.ds(j, reps, stride=npos), :]
        second = tb[pl.ds(j, reps, stride=npos), :]
        if o < LANES:
            row = pltpu.roll(jnp.where(lane >= o, first, second), (LANES - o) % LANES, axis=ONE) if o else first
        else:
            row = pltpu.roll(second, (TWO_TILES - o) % LANES, axis=ONE) if o > LANES else second
        if TOK - o < LANES:
            following = ta[pl.ds(j + ONE, reps, stride=npos), :]
            row = jnp.where(lane < TOK - o, row, pltpu.roll(following, TOK - o, axis=ONE))
        flat[pl.ds(MARG + T1 // TWO + m, reps, stride=nrow), :] = row


def lay_vectors(blk, r0, flat, va, vb):
    at = MARG + VEC0

    def pieces(row, n):
        return [blk[r0 + row:r0 + row + ONE, LANES * c:LANES * c + LANES] for c in range(n // LANES)]

    b_t2 = pieces(VROWS - SIX, TWO_TILES)
    plain = pieces(ZERO, CH) + pieces(ONE, CH) + pieces(9, TH) + b_t2[:ONE]
    for i, v in enumerate(plain):
        flat[at + i:at + i + ONE, :] = v
    moved = pieces(TWO, CH) + pieces(THREE, CH) + sum([pieces(FIVE + q, CH) for q in range(QUART)], []) + pieces(FOUR, CH)
    va[...] = jnp.zeros(va.shape, F32)
    for i, v in enumerate(moved):
        va[i:i + ONE, :] = v
    cut = TOK - LANES
    vb[ZERO:EIGHT, :] = jnp.broadcast_to(b_t2[ONE], (EIGHT, LANES))
    vb[EIGHT:EIGHT + va.shape[ZERO], :] = pltpu.roll(va[...], cut, axis=ONE)
    n = SH - VEC0 - len(plain)
    lane = lax.broadcasted_iota(jnp.int32, (n, LANES), ONE)
    flat[at + len(plain):MARG + SH, :] = jnp.where(lane < cut, vb[SEVEN:SEVEN + n, :], vb[EIGHT:EIGHT + n, :])


def finish_kernel(red0, red1, late1, heads, tok_ref, vec_ref, ex_ref, g_out, gh_out, gsm_out, loss_ref,
                  gs, r0, r1, l1, tsum, tgot, vsum, vgot, ex, nrm, flip, ta, tb, va, vb, hparts,
                  g_sem, head_sem, red_sem, pair_s, pair_r, own_s, own_r, ex_s, ex_r, nm_s, nm_r):
    me = lax.axis_index("fsdp")
    core = lax.rem(me, TWO)
    others = [lax.rem(me + i, NDEV) for i in range(ONE, NDEV)]
    reds = [pltpu.make_async_copy(a, b, red_sem.at[i]) for i, (a, b) in enumerate(((red1.at[ZERO], r1), (late1, l1), (red0.at[ZERO], r0)))]
    heads_in = pltpu.make_async_copy(heads, hparts, head_sem)
    for copy in reds + [heads_in]:
        copy.start()
    ex[ZERO] = ex_ref[...]
    barrier = pltpu.get_barrier_semaphore()
    for dev in others:
        pl.semaphore_signal(barrier, inc=ONE, device_id=(dev,), device_id_type=MESH)
    pl.semaphore_wait(barrier, NDEV - ONE)

    def remote(src, dst, ss, rs, dev):
        return pltpu.make_async_remote_copy(src_ref=src, dst_ref=dst, send_sem=ss, recv_sem=rs, device_id=(dev,), device_id_type=MESH)

    give_tok = remote(tok_ref, tgot.at[THREE], pair_s, pair_r, peer(me, ONE))
    give_vec = remote(vec_ref, vgot.at[THREE], pair_s, pair_r, peer(me, ONE))
    pl.when(core == ONE)(give_tok.start)
    pl.when(core == ZERO)(give_vec.start)
    small = [remote(ex.at[ZERO], ex.at[i], ex_s.at[i], ex_r.at[i], others[i - ONE]) for i in range(ONE, NDEV)]
    for copy in small:
        copy.start()

    def to_owner(src, dst, rel, owner):
        slot = rel // TWO - ONE
        return remote(src, dst.at[slot], own_s.at[slot], own_r.at[slot], owner)

    sides = ((ZERO, ZERO, give_tok, tok_ref, tsum, tgot), (ONE, NDEV - ONE, give_vec, vec_ref, vsum, vgot))
    for c, owner, give, mine, total, got in sides:
        @pl.when(core == c)
        def _():
            give.wait_recv()
            total[...] = mine[...] + got[THREE]
            for rel in RELS:
                @pl.when(me == owner ^ rel)
                def _():
                    to_owner(total, got, rel, owner).start()
    for copy in reds:
        copy.wait()
    add_into(r1, l1, r1.shape[ZERO])

    def per_device(body):
        for d in range(NDEV):
            @pl.when(me == d)
            def _():
                body(d)

    per_device(lambda d: untile(r1, gs.at[ONE], d))
    heads_in.wait()
    g_head = hparts[ZERO]
    for d in range(ONE, NDEV):
        g_head = g_head + hparts[d]
    gh_out[...] = g_head[:, ZERO:NCLS]
    acc = fold_rows(fold_lanes(g_head * g_head))
    for copy in small:
        copy.wait_recv()
    first = lax.rem(NDEV - me, NDEV)
    tot = ex[first]
    for d in range(ONE, NDEV):
        tot = tot + ex[lax.rem(first + d, NDEV)]
    ta[ZERO:EXR, :] = tot
    loss_ref[...] = tot[LOSS_ROW:LOSS_ROW + EIGHT, :]
    g_small = ta[pl.ds(THREE * me, THREE), :]
    gsm_out[...] = g_small
    acc = acc + jnp.sum(g_small * g_small, axis=ZERO, keepdims=True) / EIGHT
    def rest_of(d):
        untile(r0, gs.at[ZERO], d)
        if d == ZERO:
            lay_tokens(r0, core_rows(ZERO), gs.at[ONE], flip, ta, tb)
        if d == NDEV - ONE:
            lay_vectors(r0, core_rows(NDEV - ONE), gs.at[ONE], va, vb)

    per_device(rest_of)

    for c, owner, give, mine, total, got in sides:
        @pl.when(me == owner)
        def _():
            for rel in RELS:
                to_owner(total, got, rel, owner).wait_recv()
            total[...] = total[...] + got[ZERO] + (got[ONE] + got[TWO])
            if c == ZERO:
                lay_tokens(total, ZERO, gs.at[ZERO], flip, ta, tb)
            else:
                lay_vectors(total, ZERO, gs.at[ZERO], va, vb)
    flats = [pltpu.make_async_copy(gs.at[l, pl.ds(MARG, SH)], g_out.at[l], g_sem.at[l]) for l in range(TWO)]
    for copy in flats:
        copy.start()

    def square(i, carry):
        for l in range(TWO):
            part = gs[l, pl.ds(pl.multiple_of(MARG + i * NVIEW, EIGHT), NVIEW), :]
            carry = carry + fold_rows(part * part)
        return carry

    whole = SH // NVIEW
    acc = lax.fori_loop(ZERO, whole, square, acc)
    rest = SH - whole * NVIEW
    for l in range(TWO):
        part = gs[l, MARG + SH - rest:MARG + SH, :]
        acc = acc + jnp.sum(part * part, axis=ZERO, keepdims=True) / EIGHT
    nrm[ZERO] = acc
    norms = [remote(nrm.at[ZERO], nrm.at[i], nm_s.at[i], nm_r.at[i], others[i - ONE]) for i in range(ONE, NDEV)]
    for copy in norms:
        copy.start()
    for copy in norms:
        copy.wait_recv()
    tot = nrm[first]
    for d in range(ONE, NDEV):
        tot = tot + nrm[lax.rem(first + d, NDEV)]
    norm = jnp.sqrt(jnp.sum(jnp.sum(tot, axis=ZERO, keepdims=True), axis=ONE, keepdims=True))
    loss_ref[FOUR:EIGHT, :] = jnp.broadcast_to(1.0 / jnp.maximum(1.0, norm), (FOUR, LANES))
    for copy in small + norms:
        copy.wait_send()
    for c, owner, give, mine, total, got in sides:
        pl.when(core != c)(give.wait_send)
        for rel in RELS:
            pl.when(me == owner ^ rel)(to_owner(total, got, rel, owner).wait_send)
    for copy in flats:
        copy.wait()


def finish(red0, red1, late1, heads, tok, vec, ex):
    sds = jax.ShapeDtypeStruct
    dma = pltpu.SemaphoreType.DMA
    blk0, blk1 = pltpu.VMEM(red0.shape[ONE:], F32), pltpu.VMEM(red1.shape[ONE:], F32)
    return pl.pallas_call(
        finish_kernel,
        in_specs=[ANY] * FOUR + [VMEM] * THREE,
        out_specs=[ANY] + [VMEM] * THREE,
        out_shape=[sds((TWO, SH, LANES), F32), sds((HROWS, NCLS), F32), sds((THREE, LANES), F32), sds((EIGHT, LANES), F32)],
        scratch_shapes=[pltpu.VMEM((TWO, GROWS + TWO * MARG, LANES), F32), blk0, blk1, blk1,
                        pltpu.VMEM((TROWS, CH), F32), pltpu.VMEM((FOUR, TROWS, CH), F32), pltpu.VMEM((VROWS, CH), F32), pltpu.VMEM((FOUR, VROWS, CH), F32),
                        pltpu.VMEM((NDEV, EXR, LANES), F32), pltpu.VMEM((NDEV, EIGHT, LANES), F32), pltpu.VMEM((TH, TWO_TILES), F32),
                        pltpu.VMEM((TH + EIGHT, LANES), F32), pltpu.VMEM((TH + EIGHT, LANES), F32), pltpu.VMEM((48, LANES), F32), pltpu.VMEM((56, LANES), F32), pltpu.VMEM((NDEV, HROWS, NCP), F32),
                        dma((TWO,)), dma, dma((THREE,)), dma, dma, dma((THREE,)), dma((THREE,)), dma((NDEV,)), dma((NDEV,)), dma((NDEV,)), dma((NDEV,))],
        compiler_params=pltpu.CompilerParams(collective_id=THREE, has_side_effects=True, vmem_limit_bytes=67000000),
        name="finish",
    )(red0, red1, late1, heads, tok, vec, ex)


def update_kernel(p_ref, m_ref, v_ref, g_ref, hg_ref, sg_ref, scale_ref, hp_ref, hm_ref, hv_ref, sp_ref, sm_ref, sv_ref,
                  po, mo, vo, hpo, hmo, hvo, spo, smo, svo, ps, ms, vs, gs, in_sem, out_sem):
    me = lax.axis_index("fsdp")
    ins = ((p_ref, ps), (m_ref, ms), (v_ref, vs))
    outs = ((ps, po), (ms, mo), (vs, vo))

    def loads(k):
        a, n = chunk_rows(k)
        rows = pl.ds(a, n)
        return [pltpu.make_async_copy(src.at[rows, l, :], dst.at[l, rows], in_sem.at[k, j, l]) for j, (src, dst) in enumerate(ins) for l in range(TWO)] + [
            pltpu.make_async_copy(g_ref.at[l, rows], gs.at[l, rows], in_sem.at[k, THREE, l]) for l in range(TWO)]

    def stores(k):
        a, n = chunk_rows(k)
        return [pltpu.make_async_copy(src.at[l, pl.ds(a, n)], dst.at[pl.ds(a, n), l, :], out_sem.at[k, j, l]) for j, (src, dst) in enumerate(outs) for l in range(TWO)]

    for k in range(NCHUNK):
        for copy in loads(k):
            copy.start()
    scale = scale_ref[FOUR:FIVE, ZERO:ONE]
    hpo[...], hmo[...], hvo[...] = adam_math(hp_ref[...], hg_ref[...] * scale, hm_ref[...], hv_ref[...], WEIGHT_DECAY)
    spo[...], smo[...], svo[...] = adam_math(sp_ref[...], sg_ref[...] * scale, sm_ref[...], sv_ref[...], 0.0)
    mat_rows = T1 + TWO * RW - me * SH
    for k in range(NCHUNK):
        for copy in loads(k):
            copy.wait()
        a, n = chunk_rows(k)
        for l in range(TWO):
            def one(i, carry, l=l, a=a):
                o = pl.multiple_of(a + i * NVIEW, EIGHT)
                row = o + lax.broadcasted_iota(jnp.int32, (NVIEW, LANES), ZERO)
                decay = jnp.where(row < mat_rows, WEIGHT_DECAY, 0.0)
                at = pl.ds(o, NVIEW)
                ps[l, at, :], ms[l, at, :], vs[l, at, :] = adam_math(ps[l, at, :], gs[l, at, :] * scale, ms[l, at, :], vs[l, at, :], decay)
                return carry
            lax.fori_loop(ZERO, -(-n // NVIEW), one, ZERO)
        for copy in stores(k):
            copy.start()
    for k in range(NCHUNK):
        for copy in stores(k):
            copy.wait()


def update(pv, mv, vv, g, head_g, small_g, scale, heads, smalls):
    sds = jax.ShapeDtypeStruct
    dma = pltpu.SemaphoreType.DMA
    big, hd, sm = sds((SH, TWO, LANES), F32), sds((HROWS, NCLS), F32), sds((THREE, LANES), F32)
    return pl.pallas_call(
        update_kernel,
        in_specs=[ANY] * FOUR + [VMEM] * 9,
        out_specs=[ANY] * THREE + [VMEM] * SIX,
        out_shape=[big] * THREE + [hd] * THREE + [sm] * THREE,
        scratch_shapes=[pltpu.VMEM((TWO, GROWS, LANES), F32)] * FOUR + [dma((NCHUNK, FOUR, TWO)), dma((NCHUNK, THREE, TWO))],
        compiler_params=pltpu.CompilerParams(vmem_limit_bytes=67000000),
        name="update",
    )(pv, mv, vv, g, head_g, small_g, scale, *heads, *smalls)

CG = math.sqrt(2.0 / math.pi)
CA = CG * 0.044715


def mm(a, b):
    return jnp.dot(a, b, preferred_element_type=F32)


def mm_t(a, b):
    return lax.dot_general(a, b, (((ONE,), (ONE,)), ((), ())), preferred_element_type=F32)


def cat6(col):
    return jnp.concatenate([col] * (CH // LANES), axis=ONE)


def norm_stats(x):
    mean = jnp.mean(x, axis=-ONE, keepdims=True)
    cent = x - mean
    rstd = lax.rsqrt(jnp.mean(cent * cent, axis=-ONE, keepdims=True) + LN_EPS)
    return cent * rstd, rstd


def gelu_of(x):
    t = jnp.tanh(x * (CG + CA * (x * x)))
    half = 0.5 * x
    return half + half * t


def gelu_and_grad(x, d):
    u = CA * (x * x)
    q = CG + u
    t = jnp.tanh(x * q)
    s = 1.0 + t
    act = 0.5 * x * s
    return act, d * (0.5 * s + act * (1.0 - t) * (q + (u + u)))


def load_group(x_ref, xf):
    if len(x_ref.shape) == THREE:
        for i in range(GROUP):
            xf[TOK * i:TOK * i + TOK, :] = x_ref[i].astype(F32)
    else:
        xf[...] = x_ref[...].astype(F32)


def forward_kernel(first, x_ref, wt1_ref, wt2_ref, bt1_ref, bt2_ref, w1_ref, w2_ref, cv_ref, b1_ref, *rest):
    if first:
        rest = rest[FOUR:]
    (x1_ref, ut_ref, hid_ref, h2_ref, x2_ref), rest = rest[:FIVE], rest[FIVE:]
    if first:
        (flat_ref, nw1, nw2, e1, e2), rest = rest[:FIVE], rest[FIVE:]
    (xf, hs, acts), rest = rest[:THREE], rest[THREE:]
    step = pl.program_id(ZERO)
    if first:
        m1, m2, ed_sem, *sems = rest

        job = Spread(lambda d: [(there, there) for _, there in matrix_moves(d, nw1, nw2, nw1, nw2, e1, e2)], *sems)

        @pl.when(step == ZERO)
        def _():
            entry_barrier(job.me)
            job.start()

        pl.when(step == ROWS // GR // TWO)(functools.partial(job.hand_on, ORDER[:TWO]))
        pl.when(step == ROWS // GR - ONE)(functools.partial(job.hand_on, RELS[TWO:]))
    load_group(x_ref, xf)
    if first:
        flat_ref[...] = xf[...].astype(BF16)
    nrm, _ = norm_stats(xf[...])
    hs[...] = (nrm * cv_ref[ZERO:ONE, :] + cv_ref[ONE:TWO, :]).astype(BF16)
    for i in range(GROUP):
        lo = 192 * i
        ut = mm(wt1_ref[i], hs[lo:lo + WIN, :]) + cat6(bt1_ref[...])
        ut_ref[i] = ut
        out = mm(wt2_ref[i], gelu_of(ut).astype(BF16)) + cat6(bt2_ref[i])
        xf[lo:lo + WIN, :] = xf[lo:lo + WIN, :] + out
    x1b = xf[...].astype(BF16)
    x1_ref[...] = x1b
    x1 = x1b.astype(F32)
    nrm2, _ = norm_stats(x1)
    h2_ref[...] = (nrm2 * cv_ref[TWO:THREE, :] + cv_ref[THREE:FOUR, :]).astype(BF16)
    for j in range(ZERO, HID, 512):
        hid = mm(h2_ref[...], w1_ref[:, j:j + 512]) + b1_ref[ZERO:ONE, j:j + 512]
        hid_ref[:, j:j + 512] = hid
        acts[:, j:j + 512] = gelu_of(hid).astype(BF16)
    x2_ref[...] = (x1_ref[...].astype(F32) + (mm(acts[...], w2_ref[...]) + cv_ref[FOUR:FIVE, :])).astype(BF16)

    if first:
        @pl.when(step == ROWS // GR - ONE)
        def _():
            job.arrive()
            job.sent()
            merge_edges(nw1, nw2, e1, e2, m1, m2, ed_sem)


def once(shape):
    return pl.BlockSpec(shape, lambda g: (ZERO,) * len(shape), pipeline_mode=pl.Buffered(ONE))


def by_group(shape):
    return pl.BlockSpec(shape, lambda g: (g,) + (ZERO,) * (len(shape) - ONE))


def forward_layer(x, wt1t, wt2t, bt1, bt2, w1, w2, cv, b1, after=()):
    sds = jax.ShapeDtypeStruct
    first = x.ndim == THREE
    act = by_group((GR, CH))
    act_s = sds((ROWS, CH), BF16)
    outs = [act, by_group((GROUP, TH, CH)), by_group((GR, HID)), act, act]
    shapes = [act_s, sds((24, TH, CH), F32), sds((ROWS, HID), F32), act_s, act_s]
    scratch = [pltpu.VMEM((GR, CH), F32), pltpu.VMEM((GR, CH), BF16), pltpu.VMEM((GR, HID), BF16)]
    params, alias = {}, {}
    if first:
        outs += [act] + [ANY] * FOUR
        shapes += [act_s, sds((CH, HID), BF16), sds((HID, CH), BF16), sds((len(EDGE1), SIXTEEN, HID), BF16), sds((len(EDGE2), SIXTEEN, CH), BF16)]
        scratch += edge_scratch() + spread_sems(FOUR)
        params = {"collective_id": FOUR, "has_side_effects": True}
        alias = {9 + i: SIX + i for i in range(FOUR)}
    return pl.pallas_call(
        functools.partial(forward_kernel, first),
        grid=(ROWS // GR,),
        in_specs=[by_group((GROUP, TOK, CH)) if first else act, once((GROUP, TH, WIN)), once((GROUP, WIN, TH)), once((TH, LANES)), once((GROUP, WIN, LANES)),
                  once((CH, HID)), once((HID, CH)), once((EIGHT, CH)), once((EIGHT, HID))] + [ANY] * len(after),
        out_specs=outs,
        out_shape=shapes,
        scratch_shapes=scratch,
        input_output_aliases=alias,
        compiler_params=pltpu.CompilerParams(vmem_limit_bytes=67000000, **params),
        name="forward_layer",
    )(x, wt1t, wt2t, bt1, bt2, w1, w2, cv, b1, *after)

def fold_rows(a):
    return jnp.sum(a.reshape(a.shape[ZERO] // EIGHT, EIGHT, a.shape[ONE]), axis=ZERO)


def fold_lanes(a):
    tot = a[:, ZERO:LANES]
    for k in range(ONE, a.shape[ONE] // LANES):
        tot = tot + a[:, LANES * k:LANES * k + LANES]
    return tot


def norm_back(nrm, rstd, gain, d):
    dg = d * gain
    m1 = jnp.mean(dg, axis=-ONE, keepdims=True)
    m2 = jnp.mean(dg * nrm, axis=-ONE, keepdims=True)
    return rstd * (dg - m1 - nrm * m2)


SUB = 112


def backward_kernel(first, dh_ref, d2_ref, x1_ref, x_ref, ut_ref, w1_ref, wt1_ref, wt2_ref, cv_ref, gb1_ref, mine, theirs, *rest):
    if not first:
        dx_ref, *rest = rest
    tok_ref, vec_ref, red, gt1_ref, gt2_ref, gbt1_ref, gbt2_ref, gcv_ref, d1b, hs, dhf, acts0, dus0, acts1, dus1, da0, da1, *comm = rest
    pair = (acts0, dus0), (acts1, dus1)
    das = da0, da1
    step = pl.program_id(ZERO)
    job = Reduction(mine, theirs, red, *comm)
    pl.when(step == ZERO)(job.begin)
    if not first:
        pl.when(step == ONE)(job.combine)

    @pl.when(step == ZERO)
    def _():
        for r in (gt1_ref, gt2_ref, gbt1_ref, gbt2_ref, gcv_ref):
            r[...] = jnp.zeros(r.shape, F32)

    half = SUB * GROUP
    for rows in (slice(ZERO, half), slice(half, GR)):
        dhf[rows, :] = mm_t(dh_ref[rows, :], w1_ref[...])

    for i in range(GR // SUB):
        rows = slice(SUB * i, SUB * i + SUB)
        d_n2 = dhf[rows, :].astype(BF16).astype(F32)
        nrm2, rstd2 = norm_stats(x1_ref[rows, :].astype(F32))
        d2 = d2_ref[rows, :].astype(F32)
        for k, part in ((TWO, d_n2 * nrm2), (THREE, d_n2), (FOUR, d2)):
            gcv_ref[k] += fold_rows(part)
        d1 = (norm_back(nrm2, rstd2, cv_ref[TWO:THREE, :], d_n2) + d2).astype(BF16)
        d1b[rows, :] = d1
        gbt2_ref[rows, :] += fold_lanes(d1.astype(F32))
        nrm1, _ = norm_stats(x_ref[rows, :].astype(F32))
        hs[rows, :] = (nrm1 * cv_ref[ZERO:ONE, :] + cv_ref[ONE:TWO, :]).astype(BF16)
        dhf[rows, :] = jnp.zeros((SUB, CH), F32)

    def window(i):
        return slice(192 * i, 192 * i + WIN)

    def through_wt2(i):
        das[i % TWO][...] = mm(wt2_ref[i], d1b[window(i), :]).astype(BF16)

    def through_gelu(i):
        acts, dus = pair[i % TWO]
        for j in range(ZERO, TH, LANES):
            part = slice(j, j + LANES)
            act, d_u = gelu_and_grad(ut_ref[i, part, :], das[i % TWO][part, :].astype(F32))
            gbt1_ref[part, :] += fold_lanes(d_u)
            acts[part, :] = act.astype(BF16)
            dus[part, :] = d_u.astype(BF16)

    def products(i):
        acts, dus = pair[i % TWO]
        gt2_ref[i] += mm_t(d1b[window(i), :], acts[...])
        gt1_ref[i] += mm_t(hs[window(i), :], dus[...])
        dhf[window(i), :] += mm(wt1_ref[i], dus[...])

    if first:
        pl.when(step == ZERO)(job.combine)
        pl.when(step == ROWS // GR - TWO)(job.first_done)
    for i in range(GROUP + ONE):
        if i < GROUP:
            through_wt2(i)
        if i > ZERO:
            products(i - ONE)
        if i < GROUP:
            through_gelu(i)

    def norm_one(i, carry):
        rows = pl.ds(pl.multiple_of(i * SUB, SUB), SUB)
        d_n1 = dhf[rows, :].astype(BF16).astype(F32)
        nrm1, rstd1 = norm_stats(x_ref[rows, :].astype(F32))
        for k, part in ((ZERO, d_n1 * nrm1), (ONE, d_n1)):
            gcv_ref[k] += fold_rows(part)
        if not first:
            dx_ref[rows, :] = (norm_back(nrm1, rstd1, cv_ref[ZERO:ONE, :], d_n1) + d1b[rows, :].astype(F32)).astype(BF16)
        return carry

    lax.fori_loop(ZERO, GR // SUB, norm_one, ZERO)

    @pl.when(step == ROWS // GR - ONE)
    def _():
        for g, at in ((gt1_ref, ZERO), (gt2_ref, TH)):
            tok_ref[ZERO:TOK, at:at + TH] = sum(g[i, FOUR * i:FOUR * i + TOK, :] for i in range(ONE, GROUP)) + g[ZERO, ZERO:TOK, :]
        tok_ref[TOK:TROWS, :] = jnp.zeros((TROWS - TOK, CH), F32)
        vec_ref[...] = jnp.zeros(vec_ref.shape, F32)
        for i in range(FIVE):
            vec_ref[i:i + ONE, :] = jnp.sum(gcv_ref[i], axis=ZERO, keepdims=True)
        for q in range(QUART):
            vec_ref[FIVE + q:SIX + q, :] = jnp.sum(gb1_ref[:, CH * q:CH * q + CH], axis=ZERO, keepdims=True)
        vec_ref[9:10, ZERO:TH] = jnp.sum(gbt1_ref[...].T, axis=ZERO, keepdims=True)
        per_tok = sum(gbt2_ref[TOK * i:TOK * i + TOK, :] for i in range(ONE, GROUP)) + gbt2_ref[ZERO:TOK, :]
        vec_ref[10:11, ZERO:TOK] = jnp.sum(per_tok.T, axis=ZERO, keepdims=True)
        if first:
            job.finish()
        else:
            job.hand_over()


def backward_layer(dh, d2, x1, x, ut, w1, wt1s, wt2s, cv, gb1, mine, theirs, first):
    sds = jax.ShapeDtypeStruct
    act = by_group((GR, CH))
    keep = lambda shape: pl.BlockSpec(shape, lambda g: (ZERO,) * len(shape))
    n = BLK
    outs, shapes = [keep((TROWS, CH)), keep((VROWS, CH)), ANY], [sds((TROWS, CH), F32), sds((VROWS, CH), F32), sds((ONE if first else TWO, n, CH), F32)]
    if not first:
        outs, shapes = [act] + outs, [sds((ROWS, CH), BF16)] + shapes
    return pl.pallas_call(
        functools.partial(backward_kernel, first),
        grid=(ROWS // GR,),
        in_specs=[by_group((GR, HID)), act, act, act, by_group((GROUP, TH, CH)), once((CH, HID)), once((GROUP, WIN, TH)), once((GROUP, TH, WIN)), once((EIGHT, CH)), once((EIGHT, HID))] + [ANY] * TWO,
        out_specs=outs,
        out_shape=shapes,
        scratch_shapes=[pltpu.VMEM((GROUP, WIN, TH), F32), pltpu.VMEM((GROUP, WIN, TH), F32), pltpu.VMEM((TH, LANES), F32), pltpu.VMEM((GR, LANES), F32), pltpu.VMEM((FIVE, EIGHT, CH), F32),
                        pltpu.VMEM((GR, CH), BF16), pltpu.VMEM((GR, CH), BF16), pltpu.VMEM((GR, CH), F32)] + [pltpu.VMEM((TH, CH), BF16)] * SIX + reduction_scratch(n),
        compiler_params=pltpu.CompilerParams(collective_id=ONE if first else TWO, has_side_effects=True, vmem_limit_bytes=67000000),
        name="backward_layer",
    )(dh, d2, x1, x, ut, w1, wt1s, wt2s, cv, gb1, mine, theirs)

KP = 4864
NSUB = THREE
STEPS = HID // NJ


def channel_back_kernel(late, d2_ref, h2_ref, w2_ref, hid_ref, *rest):
    if late:
        tok, vec, red, dh_ref, mine, theirs, db1_ref, take, st, even, odd, dbs, dwst, ds1, ds2, ls, ss, rs, own_sem, send, recv = rest
    else:
        head, dh_ref, mine, theirs, db1_ref, heads, st, even, odd, dbs, dwst, ds1, ds2, ls, ss, rs, own_sem, send, recv = rest
    j = pl.program_id(ZERO)
    sub, part = ROWS // NSUB, CH // NSUB
    me = lax.axis_index("fsdp")
    core, partner = lax.rem(me, TWO), peer(me, ONE)

    def remote(src, dst, s, r, dev):
        return pltpu.make_async_remote_copy(src_ref=src, dst_ref=dst, send_sem=s, recv_sem=r, device_id=(dev,), device_id_type=MESH)

    def per_core(body):
        for c in range(TWO):
            pl.when(core == c)(functools.partial(body, c))

    def kept(chunk, c):
        p = chunk % TWO
        return [pltpu.make_async_copy(a, b, ls.at[p, i]) for i, (a, b) in chunk_pieces(chunk, c, ds1.at[p], ds2.at[p], mine)]

    def given(chunk, c):
        p = chunk % TWO
        return [remote(a, b, ss.at[p, i], rs.at[chunk, i], partner) for i, (a, b) in chunk_pieces(chunk, c, ds1.at[p], ds2.at[p], theirs)]

    def drain(old, c):
        for copy in kept(old, c):
            copy.wait()
        for copy in given(old, ONE - c):
            copy.wait_send()

    def leave():
        for chunk in range(TWO, STEPS):
            pl.when(j == chunk + ONE)(functools.partial(per_core, functools.partial(drain, chunk - TWO)))
        slot = lax.rem(j + ONE, TWO)
        ds1[slot] = dwst[ZERO:CH, :]
        ds2[slot] = dwst[CH:TWO * CH, :].T

        def start(chunk, c):
            for copy in given(chunk, ONE - c) + kept(chunk, c):
                copy.start()

        for chunk in range(STEPS):
            pl.when(j == chunk + ONE)(functools.partial(per_core, functools.partial(start, chunk)))

        def settle(c):
            drain(STEPS - TWO, c)
            drain(STEPS - ONE, c)
            for old in range(STEPS):
                for copy in given(old, c):
                    copy.wait_recv()

        pl.when(j == STEPS)(functools.partial(per_core, settle))

    def side(c, act):
        if late:
            (a, b), = extra_pieces(c, tok, vec, mine)
            (a2, b2), = extra_pieces(ONE - c, tok, vec, theirs)
            local, sent = pltpu.make_async_copy(a, b, own_sem), remote(a2, b2, send.at[TWO], recv.at[TWO], partner)
            if act:
                local.start()
                sent.start()
            else:
                local.wait()
                sent.wait_send()
                remote(*extra_pieces(c, tok, vec, theirs)[ZERO], send.at[TWO], recv.at[TWO], partner).wait_recv()

    others = [lax.rem(me + i, NDEV) for i in range(ONE, NDEV)]
    if late:
        others = [peer(me, rel) for rel in (ONE, TWO, FOUR)]
        hops = last_hops(red, take, send, recv, me)
    else:
        rows_for = lambda d: head.at[pl.ds(pl.multiple_of(HROWS * d, HROWS), HROWS)]
        hops = [remote(rows_for(d), heads.at[me], send.at[i], recv.at[i], d) for i, d in enumerate(others)]
        own = pltpu.make_async_copy(rows_for(me), heads.at[me], own_sem)

    @pl.when(j == ZERO)
    def _():
        barrier = pltpu.get_barrier_semaphore()
        for dev in others:
            pl.semaphore_signal(barrier, inc=ONE, device_id=(dev,), device_id_type=MESH)
        pl.semaphore_wait(barrier, len(others))
        for copy in hops:
            copy.start()
        if late:
            per_core(lambda c: side(c, True))
        else:
            own.start()

    @pl.when(j == ZERO)
    def _():
        st[ZERO:CH, ZERO:ROWS] = h2_ref[...].T
        st[CH:TWO * CH, ZERO:ROWS] = d2_ref[...].T
        st[:, ROWS:KP] = jnp.zeros((TWO * CH, KP - ROWS), BF16)
        for rhs in (even, odd):
            rhs[:, ROWS:KP, :] = jnp.zeros((TWO, KP - ROWS, NJ), BF16)

    def through_w2(r):
        rows = pl.ds(pl.multiple_of(r * sub, sub), sub)
        return mm_t(d2_ref[rows, :], w2_ref[...])

    def through_gelu(r, d_act, sums, rhs):
        rows = pl.ds(pl.multiple_of(r * sub, sub), sub)
        act, dh = gelu_and_grad(hid_ref[rows, :], d_act.astype(BF16).astype(F32))
        rhs[ONE, rows, :] = act.astype(BF16)
        dhb = dh.astype(BF16)
        rhs[ZERO, rows, :] = dhb
        dh_ref[rows, :] = dhb
        return sums + fold_rows(dh)

    def weight_part(r, rhs):
        for kind in range(TWO):
            rows = pl.ds(pl.multiple_of(CH * kind + r * part, part), part)
            dwst[rows, :] = mm(st[rows, :], rhs[kind])

    zero = jnp.zeros((EIGHT, NJ), F32)

    @pl.when(j == ZERO)
    def _():
        dbs[...] = lax.fori_loop(ZERO, NSUB, lambda r, sums: through_gelu(r, through_w2(r), sums, even), zero)

    for parity, (new, old) in enumerate(((even, odd), (odd, even))):
        @pl.when((j > ZERO) & (j < STEPS) & (lax.rem(j, TWO) == parity))
        def _():
            def both(r, sums):
                d_act = through_w2(r)
                weight_part(r, old)
                return through_gelu(r, d_act, sums, new)

            sums = lax.fori_loop(ZERO, NSUB, both, zero)
            db1_ref[...] = dbs[...]
            dbs[...] = sums

    @pl.when(j == STEPS)
    def _():
        def only(r, carry):
            weight_part(r, odd)
            return carry

        lax.fori_loop(ZERO, NSUB, only, ZERO)
        db1_ref[...] = dbs[...]

    pl.when(j > ZERO)(leave)

    @pl.when(j == STEPS)
    def _():
        for copy in hops:
            copy.wait()
        if late:
            per_core(lambda c: side(c, False))
        else:
            own.wait()


def channel_back(d2, h2, w2, hid, give):
    sds = jax.ShapeDtypeStruct
    dma = pltpu.SemaphoreType.DMA
    late = len(give) > ONE
    cur = lambda j: jnp.minimum(j, STEPS - ONE)
    prev = lambda j: jnp.maximum(j - ONE, ZERO)
    blocks = sds((NDEV // TWO, BLK, CH), F32)
    outs = [pl.BlockSpec((ROWS, NJ), lambda j: (ZERO, cur(j))), ANY, ANY, pl.BlockSpec((EIGHT, NJ), lambda j: (ZERO, prev(j)))]
    shapes = [sds((ROWS, HID), BF16), blocks, blocks, sds((EIGHT, HID), F32)]
    outs.append(ANY)
    shapes.append(sds(give[TWO].shape[ONE:] if late else (NDEV, HROWS, NCP), F32))
    return pl.pallas_call(
        functools.partial(channel_back_kernel, late),
        grid=(STEPS + ONE,),
        in_specs=[once((ROWS, CH)), once((ROWS, CH)), pl.BlockSpec((NJ, CH), lambda j: (cur(j), ZERO)), pl.BlockSpec((ROWS, NJ), lambda j: (ZERO, cur(j)))] + [ANY] * len(give),
        out_specs=outs,
        out_shape=shapes,
        scratch_shapes=[pltpu.VMEM((TWO * CH, KP), BF16), pltpu.VMEM((TWO, KP, NJ), BF16), pltpu.VMEM((TWO, KP, NJ), BF16), pltpu.VMEM((EIGHT, NJ), F32), pltpu.VMEM((TWO * CH, NJ), F32),
                        pltpu.VMEM((TWO, CH, NJ), F32), pltpu.VMEM((TWO, NJ, CH), F32), dma((TWO, EIGHT)), dma((TWO, EIGHT)), dma((STEPS, EIGHT)), dma, dma((NDEV,)), dma((NDEV,))],
        compiler_params=pltpu.CompilerParams(collective_id=FIVE + late, has_side_effects=True, vmem_limit_bytes=67000000),
        name="channel_back",
    )(d2, h2, w2, hid, *give)

IMG_PAD = 32


def head_kernel(x_ref, lab_ref, hw_ref, fv_ref, hb_ref, d2_ref, ghw_ref, ex_ref, pool, gfv_ref, dl, nrms, rstds):
    ngroup = ROWS // GR

    def image_of_row(shape, dim, g):
        row = lax.broadcasted_iota(jnp.int32, shape, dim)
        return GROUP * g + sum((row >= TOK * i).astype(jnp.int32) for i in range(ONE, GROUP))

    def rows_of(g):
        return pl.ds(pl.multiple_of(g * GR, GR), GR)

    pool[...] = jnp.zeros(pool.shape, F32)

    def pool_one(g, carry):
        nrm, rstd = norm_stats(x_ref[rows_of(g), :].astype(F32))
        nrms[rows_of(g), :] = nrm
        rstds[rows_of(g), :] = rstd
        pick = image_of_row((IMG_PAD, GR), ONE, g) == lax.broadcasted_iota(jnp.int32, (IMG_PAD, GR), ZERO)
        pool[...] += mm(pick.astype(F32).astype(BF16), (nrm * fv_ref[ZERO:ONE, :] + fv_ref[ONE:TWO, :]).astype(BF16))
        return carry

    lax.fori_loop(ZERO, ngroup, pool_one, ZERO)
    real = lax.broadcasted_iota(jnp.int32, (IMG_PAD, NCLS), ZERO) < 24
    pooled = (pool[...] / TOK).astype(BF16)
    logits = mm(pooled, hw_ref[...]) + hb_ref[ZERO:ONE, ZERO:NCLS]
    top = jnp.max(logits, axis=-ONE, keepdims=True)
    log_norm = top + jnp.log(jnp.sum(jnp.exp(logits - top), axis=-ONE, keepdims=True))
    is_label = lax.broadcasted_iota(jnp.int32, (IMG_PAD, NCLS), ONE) == lab_ref[:, ZERO:ONE]
    picked = jnp.sum(jnp.where(is_label, logits, 0.0), axis=-ONE, keepdims=True)
    per_image = jnp.where(lax.broadcasted_iota(jnp.int32, (IMG_PAD, ONE), ZERO) < 24, log_norm - picked, 0.0)
    d_logits = jnp.where(real, (jnp.exp(logits - log_norm) - is_label.astype(F32)) / (24 * NDEV), 0.0)
    d_log_b = d_logits.astype(BF16)
    dl[...] = jnp.zeros(dl.shape, F32)
    dl[:, ZERO:NCLS] = d_logits
    ghw_ref[...] = lax.dot_general(pooled, dl[...].astype(BF16), (((ZERO,), (ZERO,)), ((), ())), preferred_element_type=F32)
    d_pool = mm_t(d_log_b, hw_ref[...])
    pool[...] = d_pool / TOK
    gfv_ref[...] = jnp.zeros(gfv_ref.shape, F32)

    def back_one(g, carry):
        nrm, rstd = nrms[rows_of(g), :], rstds[rows_of(g), :]
        pick = image_of_row((GR, IMG_PAD), ZERO, g) == lax.broadcasted_iota(jnp.int32, (GR, IMG_PAD), ONE)
        d_n = mm(pick.astype(F32).astype(BF16), pool[...].astype(BF16))
        gfv_ref[ZERO] += fold_rows(d_n * nrm)
        gfv_ref[ONE] += fold_rows(d_n)
        d2_ref[rows_of(g), :] = norm_back(nrm, rstd, fv_ref[ZERO:ONE, :], d_n).astype(BF16)
        return carry

    lax.fori_loop(ZERO, ngroup, back_one, ZERO)
    nrow = CH // LANES
    parts = [jnp.sum(gfv_ref[i], axis=ZERO, keepdims=True) for i in range(TWO)] + [jnp.sum(dl[...], axis=ZERO, keepdims=True)]
    ex_ref[...] = jnp.zeros(ex_ref.shape, F32)
    for i, part in enumerate(parts):
        for c in range(part.shape[ONE] // LANES):
            ex_ref[nrow * i + c:nrow * i + c + ONE, :] = part[:, LANES * c:LANES * c + LANES]
    ex_ref[LOSS_ROW:EXR, :] = jnp.broadcast_to(jnp.sum(per_image, axis=ZERO, keepdims=True), (EXR - LOSS_ROW, LANES))


def head_layer(x2, labels, head_full, fv, head_b):
    sds = jax.ShapeDtypeStruct
    lab = jnp.broadcast_to(jnp.pad(labels, (ZERO, IMG_PAD - 24))[:, None], (IMG_PAD, LANES))
    return pl.pallas_call(
        head_kernel,
        in_specs=[VMEM] * FIVE,
        out_specs=[VMEM] * THREE,
        out_shape=[sds((ROWS, CH), BF16), sds((CH, NCP), F32), sds((EXR, LANES), F32)],
        scratch_shapes=[pltpu.VMEM((IMG_PAD, CH), F32), pltpu.VMEM((TWO, EIGHT, CH), F32), pltpu.VMEM((IMG_PAD, NCP), F32), pltpu.VMEM((ROWS, CH), F32), pltpu.VMEM((ROWS, ONE), F32)],
        compiler_params=pltpu.CompilerParams(vmem_limit_bytes=60000000),
        name="head_loss",
    )(x2, lab, head_full, fv, head_b)


def view(a):
    return a.reshape(TWO, SH, LANES).transpose(ONE, ZERO, TWO)


def unview(a):
    return a.transpose(ONE, ZERO, TWO).reshape(TWO, SH * LANES)


def solution(mesh):
    row_spec = P('fsdp')
    layer_spec = P(None, 'fsdp')
    in_specs = (row_spec, row_spec) + (layer_spec, row_spec, row_spec) * THREE
    out_specs = (P(),) + in_specs[TWO:]

    def device_step(act_in, labels, layer_p, head_w, small_p, layer_m, head_m, small_m, layer_v, head_v, small_v):
        small8 = jnp.pad(small_p.reshape(THREE, LANES), ((ZERO, FIVE), (ZERO, ZERO)))
        (w1, w2, nw1, nw2, head_full), edges_, *vectors, (fv, hb) = gather_all(view(layer_p), head_w, small8)
        x, after, saved = act_in, (nw1, nw2, *edges_), []
        for wt1s, wt2s, wt1t, wt2t, bt1, bt2, cv, b1 in vectors:
            x1, ut, hid, h2, x2, *more = forward_layer(x, wt1t, wt2t, bt1, bt2, w1, w2, cv, b1, after)
            saved.append((more[ZERO] if more else x, x1, ut, hid, h2, w1, w2, wt1s, wt2s, cv))
            if more:
                w1, w2 = more[ONE:THREE]
            x, after = x2, ()
        d2, g_head, ex = head_layer(x, labels, head_full, fv, hb)
        give, arrived = (g_head,), []
        for l, (x, x1, ut, hid, h2, w1, w2, wt1s, wt2s, cv) in reversed(list(enumerate(saved))):
            dh, mine, theirs, gb1, got = channel_back(d2, h2, w2, hid, give)
            *d_in, g_tok, g_vec, red = backward_layer(dh, d2, x1, x, ut, w1, wt1s, wt2s, cv, gb1, mine, theirs, l == ZERO)
            give = g_tok, g_vec, red
            arrived += [got, red]
            d2 = d_in[ZERO] if d_in else None
        heads, red1, late, red0 = arrived
        g, g_head, g_small, scalars = finish(red0, red1, late, heads, g_tok, g_vec, ex)
        smalls = [a.reshape(THREE, LANES) for a in (small_p, small_m, small_v)]
        outs = update(view(layer_p), view(layer_m), view(layer_v), g, g_head, g_small, scalars, (head_w, head_m, head_v), smalls)
        new_lp, new_lm, new_lv = [unview(a) for a in outs[:THREE]]
        new_hw, new_hm, new_hv = outs[THREE:SIX]
        new_sp, new_sm, new_sv = [a.reshape(-ONE) for a in outs[SIX:]]
        return (scalars[ZERO, ZERO] / (act_in.shape[ZERO] * NDEV), new_lp, new_hw, new_sp, new_lm, new_hm, new_sm, new_lv, new_hv, new_sv)

    return jax.shard_map(device_step, mesh=mesh, in_specs=in_specs, out_specs=out_specs, check_vma=False)
```

```python
import functools
import math

import jax
import jax.numpy as jnp
from jax import lax
from jax.experimental import pallas as pl
from jax.experimental.pallas import tpu as pltpu
from jax.sharding import PartitionSpec as P

F32, BF16 = jnp.float32, jnp.bfloat16
ZERO = 0
ONE = 1
TWO = 2
THREE = 3
FOUR = 4
FIVE = 5
SIX = 6
EIGHT = 8
SIXTEEN = 16
LANES = 128
TWO_TILES = 256
SEVEN = 7
LN_EPS = 1e-6
LEARN_RATE = 0.003
BETA_ONE = 0.9
BETA_TWO = 0.999
ADAM_EPS = 1e-8
WEIGHT_DECAY = 0.03
ADAM_STEP = 10

NDEV = EIGHT
TOK, CH, TH, HID, NCLS = 196, 768, 384, 3072, 1000
SH = 4763
T1 = TWO * TOK * TH // LANES
RW = CH * HID // LANES
C1, C2 = HID // LANES, CH // LANES
VEC0 = T1 + TWO * RW - SEVEN * SH
MARG = 384
GROUP = FOUR
GR = GROUP * TOK
ROWS = 24 * TOK
WIN = 208
MESH = pl.DeviceIdType.MESH
ANY = pl.BlockSpec(memory_space=pl.ANY)
VMEM = pl.BlockSpec(memory_space=pltpu.VMEM)


def c1_span(d):
    return max(ZERO, SH * d - T1), min(RW, SH * (d + ONE) - T1)


def c2_span(d):
    return max(ZERO, SH * d - T1 - RW), min(RW, SH * (d + ONE) - T1 - RW)


def tiles_of(span, per):
    lo, hi = span
    if lo >= hi:
        return ZERO, ZERO
    return lo // per, -(-hi // per)


def edges(span_of, per):
    out = []
    for d in range(NDEV):
        lo, hi = span_of(d)
        if lo < hi and lo > ZERO and lo % per:
            out.append((d, lo // per, lo % per))
    return out


EDGE1 = edges(c1_span, SIXTEEN * C1)
EDGE2 = edges(c2_span, SIXTEEN * C2)


def matrix_moves(d, s1, s2, w1, w2, e1, e2):
    out = []
    for span_of, per, s, w, e, eds in ((c1_span, SIXTEEN * C1, s1, w1, e1, EDGE1), (c2_span, SIXTEEN * C2, s2, w2, e2, EDGE2)):
        lo, hi = tiles_of(span_of(d), per)
        if lo == hi:
            continue
        first = lo
        for k, (owner, row, _) in enumerate(eds):
            if owner == d:
                out.append((s.at[pl.ds(ZERO, SIXTEEN)], e.at[k]))
                first = lo + ONE
        n = hi - first
        out.append((s.at[pl.ds(SIXTEEN * (first - lo), SIXTEEN * n)], w.at[pl.ds(SIXTEEN * first, SIXTEEN * n)]))
    return out


def entry_barrier(me):
    barrier = pltpu.get_barrier_semaphore()
    for rel in (ONE, TWO, FOUR, SIX):
        pl.semaphore_signal(barrier, inc=ONE, device_id=(peer(me, rel),), device_id_type=MESH)
    pl.semaphore_wait(barrier, FOUR)


def peer(me, rel):
    t = me
    if rel & ONE:
        t = t + ONE - TWO * lax.rem(me, TWO)
    if rel & TWO:
        t = t + TWO - FOUR * lax.rem(me // TWO, TWO)
    if rel & FOUR:
        t = t + FOUR - EIGHT * (me // FOUR)
    return t


RELS = (TWO, FOUR, SIX)


class Spread:
    def __init__(self, pieces, send_sem, recv_sem, fwd_sem, far_sem):
        self.pieces, self.send_sem, self.recv_sem, self.fwd_sem, self.far_sem = pieces, send_sem, recv_sem, fwd_sem, far_sem
        self.me = lax.axis_index("fsdp")

    def copies(self, d, k, rel):
        return [pltpu.make_async_remote_copy(src_ref=a, dst_ref=b, send_sem=self.send_sem.at[k, i], recv_sem=self.recv_sem.at[d, i], device_id=(d ^ rel,), device_id_type=MESH)
                for i, (a, b) in enumerate(self.pieces(d))]

    def handed(self, s, to):
        return [pltpu.make_async_remote_copy(src_ref=b, dst_ref=b, send_sem=self.fwd_sem.at[s, i], recv_sem=self.recv_sem.at[s, i], device_id=(to,), device_id_type=MESH)
                for i, (_, b) in enumerate(self.pieces(s))]

    def each(self, rels, body):
        for rel in rels:
            for s in range(NDEV):
                if self.pieces(s):
                    pl.when(self.me == s ^ rel)(functools.partial(body, s, rel))

    def start(self):
        def body(d, _):
            for k, rel in enumerate(ORDER):
                for copy in self.copies(d, k, rel):
                    copy.start()
        self.each((ZERO,), body)

    def across(self, s, rel):
        if rel != (FOUR if s % TWO else TWO):
            return []
        return [pltpu.make_async_remote_copy(src_ref=b, dst_ref=b, send_sem=self.far_sem.at[i], recv_sem=self.recv_sem.at[s, i], device_id=(s ^ SIX,), device_id_type=MESH)
                for i, (_, b) in enumerate(self.pieces(s))]

    def hand_on(self, rels):
        def body(s, rel):
            for copy in self.handed(s, s ^ rel ^ ONE):
                copy.wait_recv()
            for copy in self.across(s, rel) + self.handed(s, s ^ rel ^ ONE):
                copy.start()
        self.each(rels, body)

    def arrive(self):
        def body(s, rel):
            for copy in self.handed(s, s):
                copy.wait_recv()
        self.each((ONE, THREE, FIVE, SEVEN), body)

    def sent(self):
        def own(d, _):
            for k, rel in enumerate(ORDER):
                for copy in self.copies(d, k, rel):
                    copy.wait_send()
        self.each((ZERO,), own)

        def other(s, rel):
            for copy in self.across(s, rel) + self.handed(s, s ^ rel ^ ONE):
                copy.wait_send()
        self.each(RELS, other)


ORDER = (FOUR, TWO, ONE)


def merge_edges(w1, w2, e1, e2, m1, m2, sem):
    jobs = [(k, per, w.at[pl.ds(SIXTEEN * row, SIXTEEN)], e.at[k], m, below)
            for per, w, e, m, eds in ((C1, w1, e1, m1, EDGE1), (C2, w2, e2, m2, EDGE2)) for k, (_, row, below) in enumerate(eds)]
    loads = [pltpu.make_async_copy(src, m.at[i, k], sem.at[i, n]) for n, (k, _, w, e, m, _) in enumerate(jobs) for i, src in enumerate((w, e))]
    stores = [pltpu.make_async_copy(m.at[ZERO, k], w, sem.at[ZERO, n]) for n, (k, _, w, e, m, _) in enumerate(jobs)]
    for copy in loads:
        copy.start()
    for copy in loads:
        copy.wait()
    for k, per, _, _, m, below in jobs:
        shape = (SIXTEEN, LANES * per)
        pos = lax.broadcasted_iota(jnp.int32, shape, ZERO) * per + lax.broadcasted_iota(jnp.int32, shape, ONE) // LANES
        m[ZERO, k] = jnp.where(pos < below, m[ZERO, k].astype(F32), m[ONE, k].astype(F32)).astype(BF16)
    for copy in stores:
        copy.start()
    for copy in stores:
        copy.wait()


def edge_scratch():
    return [pltpu.VMEM((TWO, len(EDGE1), SIXTEEN, HID), BF16), pltpu.VMEM((TWO, len(EDGE2), SIXTEEN, CH), BF16), pltpu.SemaphoreType.DMA((TWO, len(EDGE1) + len(EDGE2)))]


def spread_sems(n):
    dma = pltpu.SemaphoreType.DMA
    return [dma((len(ORDER), n)), dma((NDEV, n)), dma((NDEV, n)), dma((n,))]


def lay_token_weights(tok, flat, nat, wt1s, wt2s, wt1t, wt2t):
    flat[ZERO:T1, :] = tok[...].astype(F32)
    period = LANES * TOK // math.gcd(LANES, TOK)
    nrow, npos = period // LANES, period // TOK
    reps = TH // npos
    lane = lax.broadcasted_iota(jnp.int32, (reps, LANES), ONE)
    for j in range(npos):
        f, o = divmod(TOK * j, LANES)
        rows = [flat[pl.ds(T1 // TWO + f + i, reps, stride=nrow), :] for i in range(THREE)]
        for i in range(TWO):
            part = jnp.where(lane >= o, rows[i], rows[i + ONE])
            nat[i, pl.ds(j, reps, stride=npos), :] = pltpu.roll(part, (LANES - o) % LANES, axis=ONE) if o else part
    two_t = jnp.concatenate([nat[ZERO].T, nat[ONE].T], axis=ZERO)
    for i in range(GROUP):
        for s, t, ref_n in ((wt2t, wt2s, two_t), (wt1s, wt1t, None)):
            flat[T1:T1 + WIN, :] = jnp.zeros((WIN, LANES), F32)
            for c in range(TH // LANES):
                lanes_ = slice(LANES * c, LANES * c + LANES)
                part = flat[pl.ds(c, TOK, stride=TH // LANES), :] if ref_n is None else ref_n[ZERO:TOK, lanes_]
                flat[T1 + FOUR * i:T1 + FOUR * i + TOK, :] = part
                full = flat[T1:T1 + WIN, :]
                s[i, :, lanes_] = full.astype(BF16)
                t[i, lanes_, :] = full.T.astype(BF16)


def lay_bias_vectors(vec, vf, bt1, bt2, cv, b1):
    vf[...] = vec[...].astype(F32)

    def put(ref, row, first, n, src):
        for c in range(n // LANES):
            ref[row:row + ONE, LANES * c:LANES * c + LANES] = src[first + c:first + c + ONE, :]

    ng, nt = CH // LANES, TH // LANES
    put(cv, ZERO, ZERO, CH, vf)
    put(cv, ONE, ng, CH, vf)
    for c in range(nt):
        bt1[LANES * c:LANES * c + LANES, :] = jnp.broadcast_to(vf[TWO * ng + c:TWO * ng + c + ONE, :], (LANES, LANES)).T
    at = TWO * ng + nt
    cols = [jnp.broadcast_to(vf[at + i:at + i + ONE, :], (LANES, LANES)).T for i in range(TWO)]
    cut = TOK - LANES
    for i in range(GROUP):
        bt2[i] = jnp.zeros((WIN, LANES), F32)
        bt2[i, FOUR * i:FOUR * i + LANES, :] = cols[ZERO]
        bt2[i, FOUR * i + LANES:FOUR * i + TOK, :] = cols[ONE][ZERO:cut, :]
    n = vf.shape[ZERO] - at - TWO
    lane = lax.broadcasted_iota(jnp.int32, (n, LANES), ONE)
    rest = pltpu.roll(jnp.where(lane >= cut, vf[at + ONE:at + ONE + n, :], vf[at + TWO:at + TWO + n, :]), LANES - cut, axis=ONE)
    vf[ZERO:n, :] = rest
    put(cv, TWO, ZERO, CH, vf)
    put(cv, THREE, ng, CH, vf)
    put(b1, ZERO, TWO * ng, HID, vf)
    put(cv, FOUR, TWO * ng + HID // LANES, CH, vf)


def gather_kernel(p_ref, head_ref, small_ref, w1, w2, nw1, nw2, headf, *rest):
    (tw0, tw1, (fv, hb)), rest = (rest[ZERO:EIGHT], rest[EIGHT:SIXTEEN], rest[SIXTEEN:18]), rest[18:]
    (e1, e2, ne1, ne2, xs, s1, s2, stok, svec, shead, ssmall, tok, vec, smallf, flat, nat, vf, m1, m2, ed_sem, ld_sem, stage_sem, own_sem), rest = rest[:23], rest[23:]
    me = lax.axis_index("fsdp")
    loads = [pltpu.make_async_copy(p_ref.at[:, l, :], xs.at[l, pl.ds(MARG, SH)], ld_sem.at[l]) for l in range(TWO)]
    for copy in loads:
        copy.start()
    shead[...] = head_ref[...].astype(BF16)
    ssmall[...] = small_ref[...].astype(BF16).astype(F32)

    def early(d):
        out = [(ssmall, smallf.at[d])]
        if d == ZERO:
            out += [(stok.at[l], tok.at[l]) for l in range(TWO)]
        if d == NDEV - ONE:
            out += [(svec.at[l], vec.at[l]) for l in range(TWO)]
        return out

    def matrices(d):
        return matrix_moves(d, s1.at[ZERO], s2.at[ZERO], w1, w2, e1, e2)

    def classes(d):
        return [(shead, headf.at[pl.ds(HROWS * d, HROWS)])]

    jobs = [Spread(f, *rest[FOUR * i:FOUR * i + FOUR]) for i, f in enumerate((early, matrices, classes))]

    def keep_own(d, _):
        return [pltpu.make_async_copy(a, b, own_sem.at[i]) for i, (a, b) in enumerate(matrices(d) + classes(d))]

    for copy in loads:
        copy.wait()

    @pl.when(me == ZERO)
    def _():
        stok[...] = xs[:, MARG:MARG + T1, :].astype(BF16)
        tok[...] = stok[...]

    @pl.when(me == NDEV - ONE)
    def _():
        svec[...] = xs[:, MARG + VEC0:MARG + SH, :].astype(BF16)
        vec[...] = svec[...]

    entry_barrier(me)
    jobs[ZERO].start()

    def tile(l):
        def body(d, _):
            for span_of, per, s, skip in ((c1_span, C1, s1, T1 if d == ZERO else ZERO), (c2_span, C2, s2, max(ZERO, c1_span(d)[ONE] - c1_span(d)[ZERO]))):
                lo, hi = tiles_of(span_of(d), SIXTEEN * per)
                base0 = SIXTEEN * per * lo - span_of(d)[ZERO] + MARG + skip

                def one(i, carry, per=per, s=s, base0=base0):
                    row = pl.multiple_of(i * SIXTEEN, SIXTEEN)
                    for c in range(per):
                        s[l, pl.ds(row, SIXTEEN), LANES * c:LANES * c + LANES] = xs[l, pl.ds(base0 + c + i * (SIXTEEN * per), SIXTEEN, stride=per), :].astype(BF16)
                    return carry

                if lo < hi:
                    lax.fori_loop(ZERO, hi - lo, one, ZERO)
        jobs[ZERO].each((ZERO,), body)

    tile(ZERO)
    jobs[ONE].start()
    jobs[TWO].start()
    for d in range(NDEV):
        @pl.when(me == d)
        def _():
            smallf[d] = ssmall[...]
            for copy in keep_own(d, ZERO):
                copy.start()
    tile(ONE)

    def keep_next(d):
        return [pltpu.make_async_copy(a, b, stage_sem.at[i]) for i, (a, b) in enumerate(matrix_moves(d, s1.at[ONE], s2.at[ONE], nw1, nw2, ne1, ne2))]

    for d in range(NDEV):
        @pl.when(me == d)
        def _():
            for copy in keep_next(d):
                copy.start()
    jobs[ZERO].hand_on(ORDER[:TWO])
    jobs[ZERO].hand_on(RELS[TWO:])
    jobs[ZERO].arrive()
    for l, (wt1s, wt2s, wt1t, wt2t, bt1, bt2, cv, b1) in enumerate((tw0, tw1)):
        lay_token_weights(tok.at[l], flat, nat, wt1s, wt2s, wt1t, wt2t)
        lay_bias_vectors(vec.at[l], vf, bt1, bt2, cv, b1)
    for d in range(NDEV):
        flat[THREE * d:THREE * d + THREE, :] = smallf[d, ZERO:THREE, :]
    for i in range(TWO):
        for c in range(CH // LANES):
            fv[i:i + ONE, LANES * c:LANES * c + LANES] = flat[C2 * i + c:C2 * i + c + ONE, :]
    for c in range(NCP // LANES):
        hb[ZERO:ONE, LANES * c:LANES * c + LANES] = flat[TWO * C2 + c:TWO * C2 + c + ONE, :]
    for rels in (ORDER[:TWO], RELS[TWO:]):
        jobs[ONE].hand_on(rels)
        jobs[TWO].hand_on(rels)
    jobs[ONE].arrive()
    jobs[TWO].arrive()
    for job in jobs:
        job.sent()
    for d in range(NDEV):
        @pl.when(me == d)
        def _():
            for copy in keep_own(d, ZERO) + keep_next(d):
                copy.wait()
    merge_edges(w1, w2, e1, e2, m1, m2, ed_sem)


STAGE1 = max(SIXTEEN * (b - a) for a, b in (tiles_of(c1_span(d), SIXTEEN * C1) for d in range(NDEV)))
STAGE2 = max(SIXTEEN * (b - a) for a, b in (tiles_of(c2_span(d), SIXTEEN * C2) for d in range(NDEV)))


def gather_all(p_view, head_w, small8):
    sds = jax.ShapeDtypeStruct
    per_layer = [sds((GROUP, WIN, TH), BF16), sds((GROUP, TH, WIN), BF16), sds((GROUP, TH, WIN), BF16), sds((GROUP, WIN, TH), BF16),
                 sds((TH, LANES), F32), sds((GROUP, WIN, LANES), F32), sds((EIGHT, CH), F32), sds((EIGHT, HID), F32)]
    far = [sds((CH, HID), BF16), sds((HID, CH), BF16)] * TWO + [sds((CH, NCLS), BF16)]
    near = per_layer * TWO + [sds((EIGHT, CH), F32), sds((EIGHT, NCP), F32)]
    edge = [sds((len(EDGE1), SIXTEEN, HID), BF16), sds((len(EDGE2), SIXTEEN, CH), BF16)] * TWO
    dma = pltpu.SemaphoreType.DMA
    nv = SH - VEC0
    outs = pl.pallas_call(
        gather_kernel,
        in_specs=[ANY, VMEM, VMEM],
        out_specs=[ANY] * len(far) + [VMEM] * len(near) + [ANY] * len(edge),
        out_shape=far + near + edge,
        scratch_shapes=[pltpu.VMEM((TWO, SH + TWO * MARG + FIVE, LANES), F32), pltpu.VMEM((TWO, STAGE1, HID), BF16), pltpu.VMEM((TWO, STAGE2, CH), BF16),
                        pltpu.VMEM((TWO, T1, LANES), BF16), pltpu.VMEM((TWO, nv, LANES), BF16), pltpu.VMEM((HROWS, NCLS), BF16), pltpu.VMEM((EIGHT, LANES), F32),
                        pltpu.VMEM((TWO, T1, LANES), BF16), pltpu.VMEM((TWO, nv, LANES), BF16), pltpu.VMEM((NDEV, EIGHT, LANES), F32),
                        pltpu.VMEM((T1 + WIN + EIGHT, LANES), F32), pltpu.VMEM((TWO, TH, LANES), F32), pltpu.VMEM((nv, LANES), F32)] + edge_scratch()
        + [dma((TWO,)), dma((FOUR,)), dma((SIX,))] + spread_sems(THREE) + spread_sems(FOUR) + spread_sems(ONE),
        compiler_params=pltpu.CompilerParams(collective_id=ZERO, has_side_effects=True, vmem_limit_bytes=60000000),
        name="gather_weights",
    )(p_view, head_w, small8)
    n = len(far)
    return outs[:n], outs[-TWO:], outs[n:n + EIGHT], outs[n + EIGHT:n + SIXTEEN], outs[n + SIXTEEN:n + 18]


def g1_rows(d):
    lo, hi = tiles_of(c1_span(d), EIGHT * C1)
    return EIGHT * lo, EIGHT * hi


def g2_rows(d):
    lo, hi = tiles_of(c2_span(d), EIGHT * C2)
    return EIGHT * lo, EIGHT * hi


QUART = HID // CH
HALF = CH // TWO
BLK = max(QUART * (g1_rows(d)[ONE] - g1_rows(d)[ZERO]) + g2_rows(d)[ONE] - g2_rows(d)[ZERO] for d in range(NDEV))


def core_rows(s):
    lo, hi = g1_rows(s)
    return QUART * (hi - lo) + g2_rows(s)[ONE] - g2_rows(s)[ZERO]


def chunk_pieces(chunk, core, ds1, ds2, blocks):
    out = []
    for k in range(NDEV // TWO):
        s = TWO * k + core
        lo, hi = g1_rows(s)
        n1 = hi - lo
        q, third = divmod(chunk, CH // NJ)
        if n1:
            out.append((ds1.at[pl.ds(lo, n1)], blocks.at[k, pl.ds(q * n1, n1), pl.ds(NJ * third, NJ)]))
        lo, hi = g2_rows(s)
        first, last = max(lo, NJ * chunk), min(hi, NJ * chunk + NJ)
        if first < last:
            out.append((ds2.at[pl.ds(first - NJ * chunk, last - first)], blocks.at[k, pl.ds(QUART * n1 + first - lo, last - first)]))
    return list(enumerate(out))


def extra_pieces(core, tok, vec, blocks):
    if core == ZERO:
        return [(tok, blocks.at[ZERO, pl.ds(core_rows(ZERO), TROWS)])]
    return [(vec, blocks.at[NDEV // TWO - ONE, pl.ds(core_rows(NDEV - ONE), VROWS)])]


NJ = TWO_TILES
NCP = 1024
HROWS = CH // NDEV
TROWS, VROWS = 200, SIXTEEN


def add_into(dst, src, n):
    def one(i, carry):
        at = pl.ds(pl.multiple_of(i * ADD, ADD), ADD)
        dst[at, :] = dst[at, :] + src[at, :]
        return carry
    lax.fori_loop(ZERO, n // ADD, one, ZERO)


ADD = 32


class Reduction:
    def __init__(self, mine, theirs, red, sums, own, ld, hs, hr, out_sem, free):
        self.mine, self.theirs, self.red, self.sums, self.own, self.free = mine, theirs, red, sums, own, free
        self.n = red.shape[ONE]
        self.ld, self.hs, self.hr, self.out_sem = ld, hs, hr, out_sem
        self.me = lax.axis_index("fsdp")
        chip = self.me // TWO
        px, py = lax.rem(chip, TWO), chip // TWO
        self.k, self.kx, self.ky = chip, chip + ONE - TWO * px, chip + TWO - FOUR * py
        self.kd = self.kx + TWO - FOUR * py

    def load(self, k):
        return pltpu.make_async_copy(self.mine.at[k], self.own.at[k % TWO], self.ld.at[ZERO, k])

    def load_theirs(self, k):
        return pltpu.make_async_copy(self.theirs.at[k], self.sums.at[k], self.ld.at[ONE, k])

    def hop(self, i, src, dst, rel):
        return pltpu.make_async_remote_copy(src_ref=src, dst_ref=dst, send_sem=self.hs.at[i], recv_sem=self.hr.at[i], device_id=(peer(self.me, rel),), device_id_type=MESH)

    def left(self, ref, k):
        return ref.at[k, :, pl.ds(ZERO, HALF)]

    def right(self, ref, k):
        return ref.at[k, :, pl.ds(HALF, HALF)]

    def ready(self, i):
        for rel in (TWO, FOUR):
            pl.semaphore_signal(self.free.at[i], inc=ONE, device_id=(peer(self.me, rel),), device_id_type=MESH)
        pl.semaphore_wait(self.free.at[i], TWO)

    def first_hops(self):
        return [self.hop(ZERO, self.left(self.sums, self.kx), self.left(self.own, ZERO), TWO), self.hop(ONE, self.left(self.sums, self.kd), self.left(self.own, ONE), TWO),
                self.hop(TWO, self.right(self.sums, self.ky), self.right(self.own, ZERO), FOUR), self.hop(THREE, self.right(self.sums, self.kd), self.right(self.own, ONE), FOUR)]

    def begin(self):
        for k in range(NDEV // TWO):
            self.load_theirs(k).start()
        for k in range(TWO):
            self.load(k).start()
        barrier = pltpu.get_barrier_semaphore()
        for rel in (TWO, FOUR):
            pl.semaphore_signal(barrier, inc=ONE, device_id=(peer(self.me, rel),), device_id_type=MESH)
        pl.semaphore_wait(barrier, TWO)
    def combine(self):
        for k in range(NDEV // TWO):
            self.load(k).wait()
            self.load_theirs(k).wait()
            add_into(self.sums.at[k], self.own.at[k % TWO], self.n)
            if k < TWO:
                self.load(k + TWO).start()
        self.ready(ZERO)
        for copy in self.first_hops():
            copy.start()

    def take(self):
        add_into(self.sums.at[self.k], self.own.at[ZERO], self.n)
        add_into(self.left(self.sums, self.ky), self.left(self.own, ONE), self.n)
        add_into(self.right(self.sums, self.kx), self.right(self.own, ONE), self.n)

    def first_done(self):
        for copy in self.first_hops():
            copy.wait_recv()
        self.take()
        self.ready(ONE)
        for copy in self.second_hops():
            copy.start()

    def second_hops(self):
        return [self.hop(FOUR, self.left(self.sums, self.ky), self.left(self.own, ZERO), FOUR), self.hop(FIVE, self.right(self.sums, self.kx), self.right(self.own, ZERO), TWO)]

    def finish(self):
        for copy in self.second_hops():
            copy.wait_recv()
        add_into(self.sums.at[self.k], self.own.at[ZERO], self.n)
        out = pltpu.make_async_copy(self.sums.at[self.k], self.red.at[ZERO], self.out_sem.at[ZERO])
        out.start()
        for copy in self.first_hops() + self.second_hops():
            copy.wait_send()
        out.wait()

    def hand_over(self):
        own, left, right = self.red.at[ZERO], self.red.at[ONE, :, pl.ds(ZERO, HALF)], self.red.at[ONE, :, pl.ds(HALF, HALF)]
        outs = [pltpu.make_async_copy(a, b, self.out_sem.at[i]) for i, (a, b) in enumerate(((self.sums.at[self.k], own), (self.left(self.sums, self.ky), left), (self.right(self.sums, self.kx), right)))]
        for copy in self.first_hops():
            copy.wait_recv()
        self.take()
        for copy in outs:
            copy.start()
        for copy in self.first_hops():
            copy.wait_send()
        for copy in outs:
            copy.wait()


def last_hops(red, late, send, recv, me):
    out = []
    for i, rel in enumerate((FOUR, TWO)):
        part = pl.ds(HALF * i, HALF)
        out.append(pltpu.make_async_remote_copy(src_ref=red.at[ONE, :, part], dst_ref=late.at[:, part], send_sem=send.at[i], recv_sem=recv.at[i], device_id=(peer(me, rel),), device_id_type=MESH))
    return out


def reduction_scratch(n):
    dma = pltpu.SemaphoreType.DMA
    return [pltpu.VMEM((FOUR, n, CH), F32), pltpu.VMEM((TWO, n, CH), F32), dma((TWO, FOUR)), dma((SIX,)), dma((SIX,)), dma((THREE,)), pltpu.SemaphoreType.REGULAR((TWO,))]


def untile(block, flat, d):
    lo, hi = g1_rows(d)
    n1 = hi - lo
    jobs = [(q * n1, n1, C1, C1 * lo - c1_span(d)[ZERO] + (T1 if d == ZERO else ZERO) + C2 * q) for q in range(QUART) if n1]
    lo, hi = g2_rows(d)
    if lo < hi:
        jobs.append((QUART * n1, hi - lo, C2, C2 * lo - c2_span(d)[ZERO] + max(ZERO, c1_span(d)[ONE] - c1_span(d)[ZERO])))
    for at, n, stride, base in jobs:
        def one(i, carry, at=at, stride=stride, base=base):
            rows = pl.ds(pl.multiple_of(at + EIGHT * i, EIGHT), EIGHT)
            for c in range(C2):
                flat[pl.ds(MARG + base + c + i * (EIGHT * stride), EIGHT, stride=stride), :] = block[rows, LANES * c:LANES * c + LANES]
            return carry
        lax.fori_loop(ZERO, n // EIGHT, one, ZERO)


def adam_math(p, g, m, v, decay):
    m_new = BETA_ONE * m + (1.0 - BETA_ONE) * g
    v_new = BETA_TWO * v + (1.0 - BETA_TWO) * g * g
    m_hat = m_new / (1.0 - BETA_ONE ** ADAM_STEP)
    v_hat = v_new / (1.0 - BETA_TWO ** ADAM_STEP)
    p_new = p - LEARN_RATE * (m_hat / (jnp.sqrt(v_hat) + ADAM_EPS) + decay * p)
    return p_new, m_new, v_new


NVIEW = 40
CHUNK = 600
NCHUNK = EIGHT
GROWS = CHUNK * NCHUNK
EXR = 32
LOSS_ROW = 24


def chunk_rows(k):
    return k * CHUNK, min(SH, (k + ONE) * CHUNK) - k * CHUNK


def lay_tokens(blk, r0, flat, flip, ta, tb):
    for c in range(TH // LANES):
        flat[pl.ds(MARG + c, TOK, stride=TH // LANES), :] = blk[r0:r0 + TOK, LANES * c:LANES * c + LANES]
    flip[:, ZERO:TROWS] = blk[r0:r0 + TROWS, TH:TWO * TH].T
    ta[ZERO:TH, :] = flip[:, ZERO:LANES]
    tb[ZERO:TH, :] = flip[:, LANES:TWO_TILES]
    period = LANES * TOK // math.gcd(LANES, TOK)
    nrow, npos = period // LANES, period // TOK
    reps = TH // npos
    lane = lax.broadcasted_iota(jnp.int32, (reps, LANES), ONE)
    for m in range(nrow):
        j, o = divmod(LANES * m, TOK)
        first = ta[pl.ds(j, reps, stride=npos), :]
        second = tb[pl.ds(j, reps, stride=npos), :]
        if o < LANES:
            row = pltpu.roll(jnp.where(lane >= o, first, second), (LANES - o) % LANES, axis=ONE) if o else first
        else:
            row = pltpu.roll(second, (TWO_TILES - o) % LANES, axis=ONE) if o > LANES else second
        if TOK - o < LANES:
            following = ta[pl.ds(j + ONE, reps, stride=npos), :]
            row = jnp.where(lane < TOK - o, row, pltpu.roll(following, TOK - o, axis=ONE))
        flat[pl.ds(MARG + T1 // TWO + m, reps, stride=nrow), :] = row


def lay_vectors(blk, r0, flat, va, vb):
    at = MARG + VEC0

    def pieces(row, n):
        return [blk[r0 + row:r0 + row + ONE, LANES * c:LANES * c + LANES] for c in range(n // LANES)]

    b_t2 = pieces(VROWS - SIX, TWO_TILES)
    plain = pieces(ZERO, CH) + pieces(ONE, CH) + pieces(9, TH) + b_t2[:ONE]
    for i, v in enumerate(plain):
        flat[at + i:at + i + ONE, :] = v
    moved = pieces(TWO, CH) + pieces(THREE, CH) + sum([pieces(FIVE + q, CH) for q in range(QUART)], []) + pieces(FOUR, CH)
    va[...] = jnp.zeros(va.shape, F32)
    for i, v in enumerate(moved):
        va[i:i + ONE, :] = v
    cut = TOK - LANES
    vb[ZERO:EIGHT, :] = jnp.broadcast_to(b_t2[ONE], (EIGHT, LANES))
    vb[EIGHT:EIGHT + va.shape[ZERO], :] = pltpu.roll(va[...], cut, axis=ONE)
    n = SH - VEC0 - len(plain)
    lane = lax.broadcasted_iota(jnp.int32, (n, LANES), ONE)
    flat[at + len(plain):MARG + SH, :] = jnp.where(lane < cut, vb[SEVEN:SEVEN + n, :], vb[EIGHT:EIGHT + n, :])


def finish_kernel(red0, red1, late1, heads, tok_ref, vec_ref, ex_ref, g_out, gh_out, gsm_out, loss_ref,
                  gs, r0, r1, l1, tsum, tgot, vsum, vgot, ex, nrm, flip, ta, tb, va, vb, hparts,
                  g_sem, head_sem, red_sem, pair_s, pair_r, own_s, own_r, ex_s, ex_r, nm_s, nm_r):
    me = lax.axis_index("fsdp")
    core = lax.rem(me, TWO)
    others = [lax.rem(me + i, NDEV) for i in range(ONE, NDEV)]
    reds = [pltpu.make_async_copy(a, b, red_sem.at[i]) for i, (a, b) in enumerate(((red1.at[ZERO], r1), (late1, l1), (red0.at[ZERO], r0)))]
    heads_in = pltpu.make_async_copy(heads, hparts, head_sem)
    for copy in reds + [heads_in]:
        copy.start()
    ex[ZERO] = ex_ref[...]
    barrier = pltpu.get_barrier_semaphore()
    for dev in others:
        pl.semaphore_signal(barrier, inc=ONE, device_id=(dev,), device_id_type=MESH)
    pl.semaphore_wait(barrier, NDEV - ONE)

    def remote(src, dst, ss, rs, dev):
        return pltpu.make_async_remote_copy(src_ref=src, dst_ref=dst, send_sem=ss, recv_sem=rs, device_id=(dev,), device_id_type=MESH)

    give_tok = remote(tok_ref, tgot.at[THREE], pair_s, pair_r, peer(me, ONE))
    give_vec = remote(vec_ref, vgot.at[THREE], pair_s, pair_r, peer(me, ONE))
    pl.when(core == ONE)(give_tok.start)
    pl.when(core == ZERO)(give_vec.start)
    small = [remote(ex.at[ZERO], ex.at[i], ex_s.at[i], ex_r.at[i], others[i - ONE]) for i in range(ONE, NDEV)]
    for copy in small:
        copy.start()

    def to_owner(src, dst, rel, owner):
        slot = rel // TWO - ONE
        return remote(src, dst.at[slot], own_s.at[slot], own_r.at[slot], owner)

    sides = ((ZERO, ZERO, give_tok, tok_ref, tsum, tgot), (ONE, NDEV - ONE, give_vec, vec_ref, vsum, vgot))
    for c, owner, give, mine, total, got in sides:
        @pl.when(core == c)
        def _():
            give.wait_recv()
            total[...] = mine[...] + got[THREE]
            for rel in RELS:
                @pl.when(me == owner ^ rel)
                def _():
                    to_owner(total, got, rel, owner).start()
    for copy in reds:
        copy.wait()
    add_into(r1, l1, r1.shape[ZERO])

    def per_device(body):
        for d in range(NDEV):
            @pl.when(me == d)
            def _():
                body(d)

    per_device(lambda d: untile(r1, gs.at[ONE], d))
    heads_in.wait()
    g_head = hparts[ZERO]
    for d in range(ONE, NDEV):
        g_head = g_head + hparts[d]
    gh_out[...] = g_head[:, ZERO:NCLS]
    acc = fold_rows(fold_lanes(g_head * g_head))
    for copy in small:
        copy.wait_recv()
    first = lax.rem(NDEV - me, NDEV)
    tot = ex[first]
    for d in range(ONE, NDEV):
        tot = tot + ex[lax.rem(first + d, NDEV)]
    ta[ZERO:EXR, :] = tot
    loss_ref[...] = tot[LOSS_ROW:LOSS_ROW + EIGHT, :]
    g_small = ta[pl.ds(THREE * me, THREE), :]
    gsm_out[...] = g_small
    acc = acc + jnp.sum(g_small * g_small, axis=ZERO, keepdims=True) / EIGHT
    def rest_of(d):
        untile(r0, gs.at[ZERO], d)
        if d == ZERO:
            lay_tokens(r0, core_rows(ZERO), gs.at[ONE], flip, ta, tb)
        if d == NDEV - ONE:
            lay_vectors(r0, core_rows(NDEV - ONE), gs.at[ONE], va, vb)

    per_device(rest_of)

    for c, owner, give, mine, total, got in sides:
        @pl.when(me == owner)
        def _():
            for rel in RELS:
                to_owner(total, got, rel, owner).wait_recv()
            total[...] = total[...] + got[ZERO] + (got[ONE] + got[TWO])
            if c == ZERO:
                lay_tokens(total, ZERO, gs.at[ZERO], flip, ta, tb)
            else:
                lay_vectors(total, ZERO, gs.at[ZERO], va, vb)
    flats = [pltpu.make_async_copy(gs.at[l, pl.ds(MARG, SH)], g_out.at[l], g_sem.at[l]) for l in range(TWO)]
    for copy in flats:
        copy.start()

    def square(i, carry):
        for l in range(TWO):
            part = gs[l, pl.ds(pl.multiple_of(MARG + i * NVIEW, EIGHT), NVIEW), :]
            carry = carry + fold_rows(part * part)
        return carry

    whole = SH // NVIEW
    acc = lax.fori_loop(ZERO, whole, square, acc)
    rest = SH - whole * NVIEW
    for l in range(TWO):
        part = gs[l, MARG + SH - rest:MARG + SH, :]
        acc = acc + jnp.sum(part * part, axis=ZERO, keepdims=True) / EIGHT
    nrm[ZERO] = acc
    norms = [remote(nrm.at[ZERO], nrm.at[i], nm_s.at[i], nm_r.at[i], others[i - ONE]) for i in range(ONE, NDEV)]
    for copy in norms:
        copy.start()
    for copy in norms:
        copy.wait_recv()
    tot = nrm[first]
    for d in range(ONE, NDEV):
        tot = tot + nrm[lax.rem(first + d, NDEV)]
    norm = jnp.sqrt(jnp.sum(jnp.sum(tot, axis=ZERO, keepdims=True), axis=ONE, keepdims=True))
    loss_ref[FOUR:EIGHT, :] = jnp.broadcast_to(1.0 / jnp.maximum(1.0, norm), (FOUR, LANES))
    for copy in small + norms:
        copy.wait_send()
    for c, owner, give, mine, total, got in sides:
        pl.when(core != c)(give.wait_send)
        for rel in RELS:
            pl.when(me == owner ^ rel)(to_owner(total, got, rel, owner).wait_send)
    for copy in flats:
        copy.wait()


def finish(red0, red1, late1, heads, tok, vec, ex):
    sds = jax.ShapeDtypeStruct
    dma = pltpu.SemaphoreType.DMA
    blk0, blk1 = pltpu.VMEM(red0.shape[ONE:], F32), pltpu.VMEM(red1.shape[ONE:], F32)
    return pl.pallas_call(
        finish_kernel,
        in_specs=[ANY] * FOUR + [VMEM] * THREE,
        out_specs=[ANY] + [VMEM] * THREE,
        out_shape=[sds((TWO, SH, LANES), F32), sds((HROWS, NCLS), F32), sds((THREE, LANES), F32), sds((EIGHT, LANES), F32)],
        scratch_shapes=[pltpu.VMEM((TWO, GROWS + TWO * MARG, LANES), F32), blk0, blk1, blk1,
                        pltpu.VMEM((TROWS, CH), F32), pltpu.VMEM((FOUR, TROWS, CH), F32), pltpu.VMEM((VROWS, CH), F32), pltpu.VMEM((FOUR, VROWS, CH), F32),
                        pltpu.VMEM((NDEV, EXR, LANES), F32), pltpu.VMEM((NDEV, EIGHT, LANES), F32), pltpu.VMEM((TH, TWO_TILES), F32),
                        pltpu.VMEM((TH + EIGHT, LANES), F32), pltpu.VMEM((TH + EIGHT, LANES), F32), pltpu.VMEM((48, LANES), F32), pltpu.VMEM((56, LANES), F32), pltpu.VMEM((NDEV, HROWS, NCP), F32),
                        dma((TWO,)), dma, dma((THREE,)), dma, dma, dma((THREE,)), dma((THREE,)), dma((NDEV,)), dma((NDEV,)), dma((NDEV,)), dma((NDEV,))],
        compiler_params=pltpu.CompilerParams(collective_id=THREE, has_side_effects=True, vmem_limit_bytes=67000000),
        name="finish",
    )(red0, red1, late1, heads, tok, vec, ex)


def update_kernel(p_ref, m_ref, v_ref, g_ref, hg_ref, sg_ref, scale_ref, hp_ref, hm_ref, hv_ref, sp_ref, sm_ref, sv_ref,
                  po, mo, vo, hpo, hmo, hvo, spo, smo, svo, ps, ms, vs, gs, in_sem, out_sem):
    me = lax.axis_index("fsdp")
    ins = ((p_ref, ps), (m_ref, ms), (v_ref, vs))
    outs = ((ps, po), (ms, mo), (vs, vo))

    def loads(k):
        a, n = chunk_rows(k)
        rows = pl.ds(a, n)
        return [pltpu.make_async_copy(src.at[rows, l, :], dst.at[l, rows], in_sem.at[k, j, l]) for j, (src, dst) in enumerate(ins) for l in range(TWO)] + [
            pltpu.make_async_copy(g_ref.at[l, rows], gs.at[l, rows], in_sem.at[k, THREE, l]) for l in range(TWO)]

    def stores(k):
        a, n = chunk_rows(k)
        return [pltpu.make_async_copy(src.at[l, pl.ds(a, n)], dst.at[pl.ds(a, n), l, :], out_sem.at[k, j, l]) for j, (src, dst) in enumerate(outs) for l in range(TWO)]

    for k in range(NCHUNK):
        for copy in loads(k):
            copy.start()
    scale = scale_ref[FOUR:FIVE, ZERO:ONE]
    hpo[...], hmo[...], hvo[...] = adam_math(hp_ref[...], hg_ref[...] * scale, hm_ref[...], hv_ref[...], WEIGHT_DECAY)
    spo[...], smo[...], svo[...] = adam_math(sp_ref[...], sg_ref[...] * scale, sm_ref[...], sv_ref[...], 0.0)
    mat_rows = T1 + TWO * RW - me * SH
    for k in range(NCHUNK):
        for copy in loads(k):
            copy.wait()
        a, n = chunk_rows(k)
        for l in range(TWO):
            def one(i, carry, l=l, a=a):
                o = pl.multiple_of(a + i * NVIEW, EIGHT)
                row = o + lax.broadcasted_iota(jnp.int32, (NVIEW, LANES), ZERO)
                decay = jnp.where(row < mat_rows, WEIGHT_DECAY, 0.0)
                at = pl.ds(o, NVIEW)
                ps[l, at, :], ms[l, at, :], vs[l, at, :] = adam_math(ps[l, at, :], gs[l, at, :] * scale, ms[l, at, :], vs[l, at, :], decay)
                return carry
            lax.fori_loop(ZERO, -(-n // NVIEW), one, ZERO)
        for copy in stores(k):
            copy.start()
    for k in range(NCHUNK):
        for copy in stores(k):
            copy.wait()


def update(pv, mv, vv, g, head_g, small_g, scale, heads, smalls):
    sds = jax.ShapeDtypeStruct
    dma = pltpu.SemaphoreType.DMA
    big, hd, sm = sds((SH, TWO, LANES), F32), sds((HROWS, NCLS), F32), sds((THREE, LANES), F32)
    return pl.pallas_call(
        update_kernel,
        in_specs=[ANY] * FOUR + [VMEM] * 9,
        out_specs=[ANY] * THREE + [VMEM] * SIX,
        out_shape=[big] * THREE + [hd] * THREE + [sm] * THREE,
        scratch_shapes=[pltpu.VMEM((TWO, GROWS, LANES), F32)] * FOUR + [dma((NCHUNK, FOUR, TWO)), dma((NCHUNK, THREE, TWO))],
        compiler_params=pltpu.CompilerParams(vmem_limit_bytes=67000000),
        name="update",
    )(pv, mv, vv, g, head_g, small_g, scale, *heads, *smalls)

CG = math.sqrt(2.0 / math.pi)
CA = CG * 0.044715


def mm(a, b):
    return jnp.dot(a, b, preferred_element_type=F32)


def mm_t(a, b):
    return lax.dot_general(a, b, (((ONE,), (ONE,)), ((), ())), preferred_element_type=F32)


def cat6(col):
    return jnp.concatenate([col] * (CH // LANES), axis=ONE)


def norm_stats(x):
    mean = jnp.mean(x, axis=-ONE, keepdims=True)
    cent = x - mean
    rstd = lax.rsqrt(jnp.mean(cent * cent, axis=-ONE, keepdims=True) + LN_EPS)
    return cent * rstd, rstd


def gelu_of(x):
    t = jnp.tanh(x * (CG + CA * (x * x)))
    half = 0.5 * x
    return half + half * t


def gelu_and_grad(x, d):
    u = CA * (x * x)
    q = CG + u
    t = jnp.tanh(x * q)
    s = 1.0 + t
    act = 0.5 * x * s
    return act, d * (0.5 * s + act * (1.0 - t) * (q + (u + u)))


def load_group(x_ref, xf):
    if len(x_ref.shape) == THREE:
        for i in range(GROUP):
            xf[TOK * i:TOK * i + TOK, :] = x_ref[i].astype(F32)
    else:
        xf[...] = x_ref[...].astype(F32)


def forward_kernel(first, x_ref, wt1_ref, wt2_ref, bt1_ref, bt2_ref, w1_ref, w2_ref, cv_ref, b1_ref, *rest):
    if first:
        rest = rest[FOUR:]
    (x1_ref, ut_ref, hid_ref, h2_ref, x2_ref), rest = rest[:FIVE], rest[FIVE:]
    if first:
        (flat_ref, nw1, nw2, e1, e2), rest = rest[:FIVE], rest[FIVE:]
    (xf, hs, acts), rest = rest[:THREE], rest[THREE:]
    step = pl.program_id(ZERO)
    if first:
        m1, m2, ed_sem, *sems = rest

        job = Spread(lambda d: [(there, there) for _, there in matrix_moves(d, nw1, nw2, nw1, nw2, e1, e2)], *sems)

        @pl.when(step == ZERO)
        def _():
            entry_barrier(job.me)
            job.start()

        pl.when(step == ROWS // GR // TWO)(functools.partial(job.hand_on, ORDER[:TWO]))
        pl.when(step == ROWS // GR - ONE)(functools.partial(job.hand_on, RELS[TWO:]))
    load_group(x_ref, xf)
    if first:
        flat_ref[...] = xf[...].astype(BF16)
    nrm, _ = norm_stats(xf[...])
    hs[...] = (nrm * cv_ref[ZERO:ONE, :] + cv_ref[ONE:TWO, :]).astype(BF16)
    for i in range(GROUP):
        lo = 192 * i
        ut = mm(wt1_ref[i], hs[lo:lo + WIN, :]) + cat6(bt1_ref[...])
        ut_ref[i] = ut
        out = mm(wt2_ref[i], gelu_of(ut).astype(BF16)) + cat6(bt2_ref[i])
        xf[lo:lo + WIN, :] = xf[lo:lo + WIN, :] + out
    x1b = xf[...].astype(BF16)
    x1_ref[...] = x1b
    x1 = x1b.astype(F32)
    nrm2, _ = norm_stats(x1)
    h2_ref[...] = (nrm2 * cv_ref[TWO:THREE, :] + cv_ref[THREE:FOUR, :]).astype(BF16)
    for j in range(ZERO, HID, 512):
        hid = mm(h2_ref[...], w1_ref[:, j:j + 512]) + b1_ref[ZERO:ONE, j:j + 512]
        hid_ref[:, j:j + 512] = hid
        acts[:, j:j + 512] = gelu_of(hid).astype(BF16)
    x2_ref[...] = (x1_ref[...].astype(F32) + (mm(acts[...], w2_ref[...]) + cv_ref[FOUR:FIVE, :])).astype(BF16)

    if first:
        @pl.when(step == ROWS // GR - ONE)
        def _():
            job.arrive()
            job.sent()
            merge_edges(nw1, nw2, e1, e2, m1, m2, ed_sem)


def once(shape):
    return pl.BlockSpec(shape, lambda g: (ZERO,) * len(shape), pipeline_mode=pl.Buffered(ONE))


def by_group(shape):
    return pl.BlockSpec(shape, lambda g: (g,) + (ZERO,) * (len(shape) - ONE))


def forward_layer(x, wt1t, wt2t, bt1, bt2, w1, w2, cv, b1, after=()):
    sds = jax.ShapeDtypeStruct
    first = x.ndim == THREE
    act = by_group((GR, CH))
    act_s = sds((ROWS, CH), BF16)
    outs = [act, by_group((GROUP, TH, CH)), by_group((GR, HID)), act, act]
    shapes = [act_s, sds((24, TH, CH), F32), sds((ROWS, HID), F32), act_s, act_s]
    scratch = [pltpu.VMEM((GR, CH), F32), pltpu.VMEM((GR, CH), BF16), pltpu.VMEM((GR, HID), BF16)]
    params, alias = {}, {}
    if first:
        outs += [act] + [ANY] * FOUR
        shapes += [act_s, sds((CH, HID), BF16), sds((HID, CH), BF16), sds((len(EDGE1), SIXTEEN, HID), BF16), sds((len(EDGE2), SIXTEEN, CH), BF16)]
        scratch += edge_scratch() + spread_sems(FOUR)
        params = {"collective_id": FOUR, "has_side_effects": True}
        alias = {9 + i: SIX + i for i in range(FOUR)}
    return pl.pallas_call(
        functools.partial(forward_kernel, first),
        grid=(ROWS // GR,),
        in_specs=[by_group((GROUP, TOK, CH)) if first else act, once((GROUP, TH, WIN)), once((GROUP, WIN, TH)), once((TH, LANES)), once((GROUP, WIN, LANES)),
                  once((CH, HID)), once((HID, CH)), once((EIGHT, CH)), once((EIGHT, HID))] + [ANY] * len(after),
        out_specs=outs,
        out_shape=shapes,
        scratch_shapes=scratch,
        input_output_aliases=alias,
        compiler_params=pltpu.CompilerParams(vmem_limit_bytes=67000000, **params),
        name="forward_layer",
    )(x, wt1t, wt2t, bt1, bt2, w1, w2, cv, b1, *after)

def fold_rows(a):
    return jnp.sum(a.reshape(a.shape[ZERO] // EIGHT, EIGHT, a.shape[ONE]), axis=ZERO)


def fold_lanes(a):
    tot = a[:, ZERO:LANES]
    for k in range(ONE, a.shape[ONE] // LANES):
        tot = tot + a[:, LANES * k:LANES * k + LANES]
    return tot


def norm_back(nrm, rstd, gain, d):
    dg = d * gain
    m1 = jnp.mean(dg, axis=-ONE, keepdims=True)
    m2 = jnp.mean(dg * nrm, axis=-ONE, keepdims=True)
    return rstd * (dg - m1 - nrm * m2)


SUB = 112


def backward_kernel(first, dh_ref, d2_ref, x1_ref, x_ref, ut_ref, w1_ref, wt1_ref, wt2_ref, cv_ref, gb1_ref, mine, theirs, *rest):
    if not first:
        dx_ref, *rest = rest
    tok_ref, vec_ref, red, gt1_ref, gt2_ref, gbt1_ref, gbt2_ref, gcv_ref, d1b, hs, dhf, acts0, dus0, acts1, dus1, da0, da1, *comm = rest
    pair = (acts0, dus0), (acts1, dus1)
    das = da0, da1
    step = pl.program_id(ZERO)
    job = Reduction(mine, theirs, red, *comm)
    pl.when(step == ZERO)(job.begin)
    if not first:
        pl.when(step == ONE)(job.combine)

    @pl.when(step == ZERO)
    def _():
        for r in (gt1_ref, gt2_ref, gbt1_ref, gbt2_ref, gcv_ref):
            r[...] = jnp.zeros(r.shape, F32)

    half = SUB * GROUP
    for rows in (slice(ZERO, half), slice(half, GR)):
        dhf[rows, :] = mm_t(dh_ref[rows, :], w1_ref[...])

    for i in range(GR // SUB):
        rows = slice(SUB * i, SUB * i + SUB)
        d_n2 = dhf[rows, :].astype(BF16).astype(F32)
        nrm2, rstd2 = norm_stats(x1_ref[rows, :].astype(F32))
        d2 = d2_ref[rows, :].astype(F32)
        for k, part in ((TWO, d_n2 * nrm2), (THREE, d_n2), (FOUR, d2)):
            gcv_ref[k] += fold_rows(part)
        d1 = (norm_back(nrm2, rstd2, cv_ref[TWO:THREE, :], d_n2) + d2).astype(BF16)
        d1b[rows, :] = d1
        gbt2_ref[rows, :] += fold_lanes(d1.astype(F32))
        nrm1, _ = norm_stats(x_ref[rows, :].astype(F32))
        hs[rows, :] = (nrm1 * cv_ref[ZERO:ONE, :] + cv_ref[ONE:TWO, :]).astype(BF16)
        dhf[rows, :] = jnp.zeros((SUB, CH), F32)

    def window(i):
        return slice(192 * i, 192 * i + WIN)

    def through_wt2(i):
        das[i % TWO][...] = mm(wt2_ref[i], d1b[window(i), :]).astype(BF16)

    def through_gelu(i):
        acts, dus = pair[i % TWO]
        for j in range(ZERO, TH, LANES):
            part = slice(j, j + LANES)
            act, d_u = gelu_and_grad(ut_ref[i, part, :], das[i % TWO][part, :].astype(F32))
            gbt1_ref[part, :] += fold_lanes(d_u)
            acts[part, :] = act.astype(BF16)
            dus[part, :] = d_u.astype(BF16)

    def products(i):
        acts, dus = pair[i % TWO]
        gt2_ref[i] += mm_t(d1b[window(i), :], acts[...])
        gt1_ref[i] += mm_t(hs[window(i), :], dus[...])
        dhf[window(i), :] += mm(wt1_ref[i], dus[...])

    if first:
        pl.when(step == ZERO)(job.combine)
        pl.when(step == ROWS // GR - TWO)(job.first_done)
    for i in range(GROUP + ONE):
        if i < GROUP:
            through_wt2(i)
        if i > ZERO:
            products(i - ONE)
        if i < GROUP:
            through_gelu(i)

    def norm_one(i, carry):
        rows = pl.ds(pl.multiple_of(i * SUB, SUB), SUB)
        d_n1 = dhf[rows, :].astype(BF16).astype(F32)
        nrm1, rstd1 = norm_stats(x_ref[rows, :].astype(F32))
        for k, part in ((ZERO, d_n1 * nrm1), (ONE, d_n1)):
            gcv_ref[k] += fold_rows(part)
        if not first:
            dx_ref[rows, :] = (norm_back(nrm1, rstd1, cv_ref[ZERO:ONE, :], d_n1) + d1b[rows, :].astype(F32)).astype(BF16)
        return carry

    lax.fori_loop(ZERO, GR // SUB, norm_one, ZERO)

    @pl.when(step == ROWS // GR - ONE)
    def _():
        for g, at in ((gt1_ref, ZERO), (gt2_ref, TH)):
            tok_ref[ZERO:TOK, at:at + TH] = sum(g[i, FOUR * i:FOUR * i + TOK, :] for i in range(ONE, GROUP)) + g[ZERO, ZERO:TOK, :]
        tok_ref[TOK:TROWS, :] = jnp.zeros((TROWS - TOK, CH), F32)
        vec_ref[...] = jnp.zeros(vec_ref.shape, F32)
        for i in range(FIVE):
            vec_ref[i:i + ONE, :] = jnp.sum(gcv_ref[i], axis=ZERO, keepdims=True)
        for q in range(QUART):
            vec_ref[FIVE + q:SIX + q, :] = jnp.sum(gb1_ref[:, CH * q:CH * q + CH], axis=ZERO, keepdims=True)
        vec_ref[9:10, ZERO:TH] = jnp.sum(gbt1_ref[...].T, axis=ZERO, keepdims=True)
        per_tok = sum(gbt2_ref[TOK * i:TOK * i + TOK, :] for i in range(ONE, GROUP)) + gbt2_ref[ZERO:TOK, :]
        vec_ref[10:11, ZERO:TOK] = jnp.sum(per_tok.T, axis=ZERO, keepdims=True)
        if first:
            job.finish()
        else:
            job.hand_over()


def backward_layer(dh, d2, x1, x, ut, w1, wt1s, wt2s, cv, gb1, mine, theirs, first):
    sds = jax.ShapeDtypeStruct
    act = by_group((GR, CH))
    keep = lambda shape: pl.BlockSpec(shape, lambda g: (ZERO,) * len(shape))
    n = BLK
    outs, shapes = [keep((TROWS, CH)), keep((VROWS, CH)), ANY], [sds((TROWS, CH), F32), sds((VROWS, CH), F32), sds((ONE if first else TWO, n, CH), F32)]
    if not first:
        outs, shapes = [act] + outs, [sds((ROWS, CH), BF16)] + shapes
    return pl.pallas_call(
        functools.partial(backward_kernel, first),
        grid=(ROWS // GR,),
        in_specs=[by_group((GR, HID)), act, act, act, by_group((GROUP, TH, CH)), once((CH, HID)), once((GROUP, WIN, TH)), once((GROUP, TH, WIN)), once((EIGHT, CH)), once((EIGHT, HID))] + [ANY] * TWO,
        out_specs=outs,
        out_shape=shapes,
        scratch_shapes=[pltpu.VMEM((GROUP, WIN, TH), F32), pltpu.VMEM((GROUP, WIN, TH), F32), pltpu.VMEM((TH, LANES), F32), pltpu.VMEM((GR, LANES), F32), pltpu.VMEM((FIVE, EIGHT, CH), F32),
                        pltpu.VMEM((GR, CH), BF16), pltpu.VMEM((GR, CH), BF16), pltpu.VMEM((GR, CH), F32)] + [pltpu.VMEM((TH, CH), BF16)] * SIX + reduction_scratch(n),
        compiler_params=pltpu.CompilerParams(collective_id=ONE if first else TWO, has_side_effects=True, vmem_limit_bytes=67000000),
        name="backward_layer",
    )(dh, d2, x1, x, ut, w1, wt1s, wt2s, cv, gb1, mine, theirs)

KP = 4864
NSUB = THREE
STEPS = HID // NJ


def channel_back_kernel(late, d2_ref, h2_ref, w2_ref, hid_ref, *rest):
    if late:
        tok, vec, red, dh_ref, mine, theirs, db1_ref, take, st, even, odd, dbs, dwst, ds1, ds2, ls, ss, rs, own_sem, send, recv = rest
    else:
        head, dh_ref, mine, theirs, db1_ref, heads, st, even, odd, dbs, dwst, ds1, ds2, ls, ss, rs, own_sem, send, recv = rest
    j = pl.program_id(ZERO)
    sub, part = ROWS // NSUB, CH // NSUB
    me = lax.axis_index("fsdp")
    core, partner = lax.rem(me, TWO), peer(me, ONE)

    def remote(src, dst, s, r, dev):
        return pltpu.make_async_remote_copy(src_ref=src, dst_ref=dst, send_sem=s, recv_sem=r, device_id=(dev,), device_id_type=MESH)

    def per_core(body):
        for c in range(TWO):
            pl.when(core == c)(functools.partial(body, c))

    def kept(chunk, c):
        p = chunk % TWO
        return [pltpu.make_async_copy(a, b, ls.at[p, i]) for i, (a, b) in chunk_pieces(chunk, c, ds1.at[p], ds2.at[p], mine)]

    def given(chunk, c):
        p = chunk % TWO
        return [remote(a, b, ss.at[p, i], rs.at[chunk, i], partner) for i, (a, b) in chunk_pieces(chunk, c, ds1.at[p], ds2.at[p], theirs)]

    def drain(old, c):
        for copy in kept(old, c):
            copy.wait()
        for copy in given(old, ONE - c):
            copy.wait_send()

    def leave():
        for chunk in range(TWO, STEPS):
            pl.when(j == chunk + ONE)(functools.partial(per_core, functools.partial(drain, chunk - TWO)))
        slot = lax.rem(j + ONE, TWO)
        ds1[slot] = dwst[ZERO:CH, :]
        ds2[slot] = dwst[CH:TWO * CH, :].T

        def start(chunk, c):
            for copy in given(chunk, ONE - c) + kept(chunk, c):
                copy.start()

        for chunk in range(STEPS):
            pl.when(j == chunk + ONE)(functools.partial(per_core, functools.partial(start, chunk)))

        def settle(c):
            drain(STEPS - TWO, c)
            drain(STEPS - ONE, c)
            for old in range(STEPS):
                for copy in given(old, c):
                    copy.wait_recv()

        pl.when(j == STEPS)(functools.partial(per_core, settle))

    def side(c, act):
        if late:
            (a, b), = extra_pieces(c, tok, vec, mine)
            (a2, b2), = extra_pieces(ONE - c, tok, vec, theirs)
            local, sent = pltpu.make_async_copy(a, b, own_sem), remote(a2, b2, send.at[TWO], recv.at[TWO], partner)
            if act:
                local.start()
                sent.start()
            else:
                local.wait()
                sent.wait_send()
                remote(*extra_pieces(c, tok, vec, theirs)[ZERO], send.at[TWO], recv.at[TWO], partner).wait_recv()

    others = [lax.rem(me + i, NDEV) for i in range(ONE, NDEV)]
    if late:
        others = [peer(me, rel) for rel in (ONE, TWO, FOUR)]
        hops = last_hops(red, take, send, recv, me)
    else:
        rows_for = lambda d: head.at[pl.ds(pl.multiple_of(HROWS * d, HROWS), HROWS)]
        hops = [remote(rows_for(d), heads.at[me], send.at[i], recv.at[i], d) for i, d in enumerate(others)]
        own = pltpu.make_async_copy(rows_for(me), heads.at[me], own_sem)

    @pl.when(j == ZERO)
    def _():
        barrier = pltpu.get_barrier_semaphore()
        for dev in others:
            pl.semaphore_signal(barrier, inc=ONE, device_id=(dev,), device_id_type=MESH)
        pl.semaphore_wait(barrier, len(others))
        for copy in hops:
            copy.start()
        if late:
            per_core(lambda c: side(c, True))
        else:
            own.start()

    @pl.when(j == ZERO)
    def _():
        st[ZERO:CH, ZERO:ROWS] = h2_ref[...].T
        st[CH:TWO * CH, ZERO:ROWS] = d2_ref[...].T
        st[:, ROWS:KP] = jnp.zeros((TWO * CH, KP - ROWS), BF16)
        for rhs in (even, odd):
            rhs[:, ROWS:KP, :] = jnp.zeros((TWO, KP - ROWS, NJ), BF16)

    def through_w2(r):
        rows = pl.ds(pl.multiple_of(r * sub, sub), sub)
        return mm_t(d2_ref[rows, :], w2_ref[...])

    def through_gelu(r, d_act, sums, rhs):
        rows = pl.ds(pl.multiple_of(r * sub, sub), sub)
        act, dh = gelu_and_grad(hid_ref[rows, :], d_act.astype(BF16).astype(F32))
        rhs[ONE, rows, :] = act.astype(BF16)
        dhb = dh.astype(BF16)
        rhs[ZERO, rows, :] = dhb
        dh_ref[rows, :] = dhb
        return sums + fold_rows(dh)

    def weight_part(r, rhs):
        for kind in range(TWO):
            rows = pl.ds(pl.multiple_of(CH * kind + r * part, part), part)
            dwst[rows, :] = mm(st[rows, :], rhs[kind])

    zero = jnp.zeros((EIGHT, NJ), F32)

    @pl.when(j == ZERO)
    def _():
        dbs[...] = lax.fori_loop(ZERO, NSUB, lambda r, sums: through_gelu(r, through_w2(r), sums, even), zero)

    for parity, (new, old) in enumerate(((even, odd), (odd, even))):
        @pl.when((j > ZERO) & (j < STEPS) & (lax.rem(j, TWO) == parity))
        def _():
            def both(r, sums):
                d_act = through_w2(r)
                weight_part(r, old)
                return through_gelu(r, d_act, sums, new)

            sums = lax.fori_loop(ZERO, NSUB, both, zero)
            db1_ref[...] = dbs[...]
            dbs[...] = sums

    @pl.when(j == STEPS)
    def _():
        def only(r, carry):
            weight_part(r, odd)
            return carry

        lax.fori_loop(ZERO, NSUB, only, ZERO)
        db1_ref[...] = dbs[...]

    pl.when(j > ZERO)(leave)

    @pl.when(j == STEPS)
    def _():
        for copy in hops:
            copy.wait()
        if late:
            per_core(lambda c: side(c, False))
        else:
            own.wait()


def channel_back(d2, h2, w2, hid, give):
    sds = jax.ShapeDtypeStruct
    dma = pltpu.SemaphoreType.DMA
    late = len(give) > ONE
    cur = lambda j: jnp.minimum(j, STEPS - ONE)
    prev = lambda j: jnp.maximum(j - ONE, ZERO)
    blocks = sds((NDEV // TWO, BLK, CH), F32)
    outs = [pl.BlockSpec((ROWS, NJ), lambda j: (ZERO, cur(j))), ANY, ANY, pl.BlockSpec((EIGHT, NJ), lambda j: (ZERO, prev(j)))]
    shapes = [sds((ROWS, HID), BF16), blocks, blocks, sds((EIGHT, HID), F32)]
    outs.append(ANY)
    shapes.append(sds(give[TWO].shape[ONE:] if late else (NDEV, HROWS, NCP), F32))
    return pl.pallas_call(
        functools.partial(channel_back_kernel, late),
        grid=(STEPS + ONE,),
        in_specs=[once((ROWS, CH)), once((ROWS, CH)), pl.BlockSpec((NJ, CH), lambda j: (cur(j), ZERO)), pl.BlockSpec((ROWS, NJ), lambda j: (ZERO, cur(j)))] + [ANY] * len(give),
        out_specs=outs,
        out_shape=shapes,
        scratch_shapes=[pltpu.VMEM((TWO * CH, KP), BF16), pltpu.VMEM((TWO, KP, NJ), BF16), pltpu.VMEM((TWO, KP, NJ), BF16), pltpu.VMEM((EIGHT, NJ), F32), pltpu.VMEM((TWO * CH, NJ), F32),
                        pltpu.VMEM((TWO, CH, NJ), F32), pltpu.VMEM((TWO, NJ, CH), F32), dma((TWO, EIGHT)), dma((TWO, EIGHT)), dma((STEPS, EIGHT)), dma, dma((NDEV,)), dma((NDEV,))],
        compiler_params=pltpu.CompilerParams(collective_id=FIVE + late, has_side_effects=True, vmem_limit_bytes=67000000),
        name="channel_back",
    )(d2, h2, w2, hid, *give)

IMG_PAD = 32


def head_kernel(x_ref, lab_ref, hw_ref, fv_ref, hb_ref, d2_ref, ghw_ref, ex_ref, pool, gfv_ref, dl, nrms, rstds):
    ngroup = ROWS // GR

    def image_of_row(shape, dim, g):
        row = lax.broadcasted_iota(jnp.int32, shape, dim)
        return GROUP * g + sum((row >= TOK * i).astype(jnp.int32) for i in range(ONE, GROUP))

    def rows_of(g):
        return pl.ds(pl.multiple_of(g * GR, GR), GR)

    pool[...] = jnp.zeros(pool.shape, F32)

    def pool_one(g, carry):
        nrm, rstd = norm_stats(x_ref[rows_of(g), :].astype(F32))
        nrms[rows_of(g), :] = nrm
        rstds[rows_of(g), :] = rstd
        pick = image_of_row((IMG_PAD, GR), ONE, g) == lax.broadcasted_iota(jnp.int32, (IMG_PAD, GR), ZERO)
        pool[...] += mm(pick.astype(F32).astype(BF16), (nrm * fv_ref[ZERO:ONE, :] + fv_ref[ONE:TWO, :]).astype(BF16))
        return carry

    lax.fori_loop(ZERO, ngroup, pool_one, ZERO)
    real = lax.broadcasted_iota(jnp.int32, (IMG_PAD, NCLS), ZERO) < 24
    pooled = (pool[...] / TOK).astype(BF16)
    logits = mm(pooled, hw_ref[...]) + hb_ref[ZERO:ONE, ZERO:NCLS]
    top = jnp.max(logits, axis=-ONE, keepdims=True)
    log_norm = top + jnp.log(jnp.sum(jnp.exp(logits - top), axis=-ONE, keepdims=True))
    is_label = lax.broadcasted_iota(jnp.int32, (IMG_PAD, NCLS), ONE) == lab_ref[:, ZERO:ONE]
    picked = jnp.sum(jnp.where(is_label, logits, 0.0), axis=-ONE, keepdims=True)
    per_image = jnp.where(lax.broadcasted_iota(jnp.int32, (IMG_PAD, ONE), ZERO) < 24, log_norm - picked, 0.0)
    d_logits = jnp.where(real, (jnp.exp(logits - log_norm) - is_label.astype(F32)) / (24 * NDEV), 0.0)
    d_log_b = d_logits.astype(BF16)
    dl[...] = jnp.zeros(dl.shape, F32)
    dl[:, ZERO:NCLS] = d_logits
    ghw_ref[...] = lax.dot_general(pooled, dl[...].astype(BF16), (((ZERO,), (ZERO,)), ((), ())), preferred_element_type=F32)
    d_pool = mm_t(d_log_b, hw_ref[...])
    pool[...] = d_pool / TOK
    gfv_ref[...] = jnp.zeros(gfv_ref.shape, F32)

    def back_one(g, carry):
        nrm, rstd = nrms[rows_of(g), :], rstds[rows_of(g), :]
        pick = image_of_row((GR, IMG_PAD), ZERO, g) == lax.broadcasted_iota(jnp.int32, (GR, IMG_PAD), ONE)
        d_n = mm(pick.astype(F32).astype(BF16), pool[...].astype(BF16))
        gfv_ref[ZERO] += fold_rows(d_n * nrm)
        gfv_ref[ONE] += fold_rows(d_n)
        d2_ref[rows_of(g), :] = norm_back(nrm, rstd, fv_ref[ZERO:ONE, :], d_n).astype(BF16)
        return carry

    lax.fori_loop(ZERO, ngroup, back_one, ZERO)
    nrow = CH // LANES
    parts = [jnp.sum(gfv_ref[i], axis=ZERO, keepdims=True) for i in range(TWO)] + [jnp.sum(dl[...], axis=ZERO, keepdims=True)]
    ex_ref[...] = jnp.zeros(ex_ref.shape, F32)
    for i, part in enumerate(parts):
        for c in range(part.shape[ONE] // LANES):
            ex_ref[nrow * i + c:nrow * i + c + ONE, :] = part[:, LANES * c:LANES * c + LANES]
    ex_ref[LOSS_ROW:EXR, :] = jnp.broadcast_to(jnp.sum(per_image, axis=ZERO, keepdims=True), (EXR - LOSS_ROW, LANES))


def head_layer(x2, labels, head_full, fv, head_b):
    sds = jax.ShapeDtypeStruct
    lab = jnp.broadcast_to(jnp.pad(labels, (ZERO, IMG_PAD - 24))[:, None], (IMG_PAD, LANES))
    return pl.pallas_call(
        head_kernel,
        in_specs=[VMEM] * FIVE,
        out_specs=[VMEM] * THREE,
        out_shape=[sds((ROWS, CH), BF16), sds((CH, NCP), F32), sds((EXR, LANES), F32)],
        scratch_shapes=[pltpu.VMEM((IMG_PAD, CH), F32), pltpu.VMEM((TWO, EIGHT, CH), F32), pltpu.VMEM((IMG_PAD, NCP), F32), pltpu.VMEM((ROWS, CH), F32), pltpu.VMEM((ROWS, ONE), F32)],
        compiler_params=pltpu.CompilerParams(vmem_limit_bytes=60000000),
        name="head_loss",
    )(x2, lab, head_full, fv, head_b)


def view(a):
    return a.reshape(TWO, SH, LANES).transpose(ONE, ZERO, TWO)


def unview(a):
    return a.transpose(ONE, ZERO, TWO).reshape(TWO, SH * LANES)


def solution(mesh):
    row_spec = P('fsdp')
    layer_spec = P(None, 'fsdp')
    in_specs = (row_spec, row_spec) + (layer_spec, row_spec, row_spec) * THREE
    out_specs = (P(),) + in_specs[TWO:]

    def device_step(act_in, labels, layer_p, head_w, small_p, layer_m, head_m, small_m, layer_v, head_v, small_v):
        small8 = jnp.pad(small_p.reshape(THREE, LANES), ((ZERO, FIVE), (ZERO, ZERO)))
        (w1, w2, nw1, nw2, head_full), edges_, *vectors, (fv, hb) = gather_all(view(layer_p), head_w, small8)
        x, after, saved = act_in, (nw1, nw2, *edges_), []
        for wt1s, wt2s, wt1t, wt2t, bt1, bt2, cv, b1 in vectors:
            x1, ut, hid, h2, x2, *more = forward_layer(x, wt1t, wt2t, bt1, bt2, w1, w2, cv, b1, after)
            saved.append((more[ZERO] if more else x, x1, ut, hid, h2, w1, w2, wt1s, wt2s, cv))
            if more:
                w1, w2 = more[ONE:THREE]
            x, after = x2, ()
        d2, g_head, ex = head_layer(x, labels, head_full, fv, hb)
        give, arrived = (g_head,), []
        for l, (x, x1, ut, hid, h2, w1, w2, wt1s, wt2s, cv) in reversed(list(enumerate(saved))):
            dh, mine, theirs, gb1, got = channel_back(d2, h2, w2, hid, give)
            *d_in, g_tok, g_vec, red = backward_layer(dh, d2, x1, x, ut, w1, wt1s, wt2s, cv, gb1, mine, theirs, l == ZERO)
            give = g_tok, g_vec, red
            arrived += [got, red]
            d2 = d_in[ZERO] if d_in else None
        heads, red1, late, red0 = arrived
        g, g_head, g_small, scalars = finish(red0, red1, late, heads, g_tok, g_vec, ex)
        smalls = [a.reshape(THREE, LANES) for a in (small_p, small_m, small_v)]
        outs = update(view(layer_p), view(layer_m), view(layer_v), g, g_head, g_small, scalars, (head_w, head_m, head_v), smalls)
        new_lp, new_lm, new_lv = [unview(a) for a in outs[:THREE]]
        new_hw, new_hm, new_hv = outs[THREE:SIX]
        new_sp, new_sm, new_sv = [a.reshape(-ONE) for a in outs[SIX:]]
        return (scalars[ZERO, ZERO] / (act_in.shape[ZERO] * NDEV), new_lp, new_hw, new_sp, new_lm, new_hm, new_sm, new_lv, new_hv, new_sv)

    return jax.shard_map(device_step, mesh=mesh, in_specs=in_specs, out_specs=out_specs, check_vma=False)
```
